8 devices in a mesh: dp: 2 (over z, y), tp: 4 (over x, core).
Axes of the slice: x: 2, y: 2, z: 1, core: 2. Of those that a mesh axis runs over, the one named last changes fastest.
Arguments:
- tokens: bfloat16 [4, 264, 1024], P('dp', 'tp')
- grad_y: bfloat16 [4, 264, 1024], P('dp', 'tp')
- valid_len: int32 [4], P('dp')
- norm1_gain: float32 [2, 1024], replicated
- norm1_bias: float32 [2, 1024], replicated
- w_qkv: bfloat16 [2, 3, 1024, 16, 64], P(None, None, None, 'tp')
- b_qkv: float32 [2, 3, 16, 64], P(None, None, 'tp')
- w_proj: bfloat16 [2, 16, 64, 1024], P(None, 'tp')
- b_proj: float32 [2, 1024], replicated
- layer_scale1: float32 [2, 1024], replicated
- norm2_gain: float32 [2, 1024], replicated
- norm2_bias: float32 [2, 1024], replicated
- w_up: bfloat16 [2, 2, 1024, 4096], P(None, None, None, 'tp')
- b_up: float32 [2, 2, 4096], P(None, None, 'tp')
- w_down: bfloat16 [2, 4096, 1024], P(None, 'tp')
- b_down: float32 [2, 1024], replicated
- layer_scale2: float32 [2, 1024], replicated
Outputs:
- output 1: bfloat16 [4, 264, 1024], P('dp', 'tp')
- output 2: bfloat16 [4, 264, 1024], P('dp', 'tp')
- output 3: float32 [2, 1024], replicated
- output 4: float32 [2, 1024], replicated
- output 5: float32 [2, 3, 1024, 16, 64], P(None, None, None, 'tp')
- output 6: float32 [2, 3, 16, 64], P(None, None, 'tp')
- output 7: float32 [2, 16, 64, 1024], P(None, 'tp')
- output 8: float32 [2, 1024], replicated
- output 9: float32 [2, 1024], replicated
- output 10: float32 [2, 1024], replicated
- output 11: float32 [2, 1024], replicated
- output 12: float32 [2, 2, 1024, 4096], P(None, None, None, 'tp')
- output 13: float32 [2, 2, 4096], P(None, None, 'tp')
- output 14: float32 [2, 4096, 1024], P(None, 'tp')
- output 15: float32 [2, 1024], replicated
- output 16: float32 [2, 1024], replicated
All inputs are finite; a program needn't handle non-finite values.
Results may differ from the reference program's by a relative error of at most 0.02.
Values are sent between devices in bfloat16 or wider.
A program may use at most 1 GiB of HBM per device.

```python
import jax
import jax.numpy as jnp
from jax import lax

WIDTH = 1024
NUM_HEADS = 16
HEAD_DIM = 64
HIDDEN = 4096
SEQ_LEN = 264
BATCH_ALL = 4
BLOCKS = 2
NORM_EPS = 1e-6
NEG_BIG = -1e9


def setup_inputs(seed: int = 0) -> dict:
    keys = jax.random.split(jax.random.key(seed), 20)
    low_len = SEQ_LEN - SEQ_LEN // 4
    row_scale = jax.random.uniform(keys[0], (BATCH_ALL, SEQ_LEN, 1), minval=0.5, maxval=2.0)
    tokens = (jax.random.normal(keys[1], (BATCH_ALL, SEQ_LEN, WIDTH)) * row_scale).astype(jnp.bfloat16)
    grad_y = jax.random.normal(keys[2], (BATCH_ALL, SEQ_LEN, WIDTH)).astype(jnp.bfloat16)
    valid_len = jax.random.randint(keys[3], (BATCH_ALL,), low_len, SEQ_LEN + 1).astype(jnp.int32)
    valid_len = valid_len.at[0].set(SEQ_LEN).at[BATCH_ALL - 1].set(low_len)
    width_scale = WIDTH ** -0.5
    vec_shape = (BLOCKS, WIDTH)
    return {
        'tokens': tokens,
        'grad_y': grad_y,
        'valid_len': valid_len,
        'norm1_gain': 1.0 + 0.25 * jax.random.normal(keys[4], vec_shape),
        'norm1_bias': 0.2 * jax.random.normal(keys[5], vec_shape),
        'w_qkv': (jax.random.normal(keys[6], (BLOCKS, 3, WIDTH, NUM_HEADS, HEAD_DIM)) * width_scale).astype(jnp.bfloat16),
        'b_qkv': 0.3 * jax.random.normal(keys[7], (BLOCKS, 3, NUM_HEADS, HEAD_DIM)),
        'w_proj': (jax.random.normal(keys[8], (BLOCKS, NUM_HEADS, HEAD_DIM, WIDTH)) * width_scale).astype(jnp.bfloat16),
        'b_proj': 0.2 * jax.random.normal(keys[9], vec_shape),
        'layer_scale1': jax.random.uniform(keys[10], vec_shape, minval=0.2, maxval=0.8),
        'norm2_gain': 1.0 + 0.25 * jax.random.normal(keys[11], vec_shape),
        'norm2_bias': 0.2 * jax.random.normal(keys[12], vec_shape),
        'w_up': (jax.random.normal(keys[13], (BLOCKS, 2, WIDTH, HIDDEN)) * width_scale).astype(jnp.bfloat16),
        'b_up': 0.3 * jax.random.normal(keys[14], (BLOCKS, 2, HIDDEN)),
        'w_down': (jax.random.normal(keys[15], (BLOCKS, HIDDEN, WIDTH)) * HIDDEN ** -0.5).astype(jnp.bfloat16),
        'b_down': 0.2 * jax.random.normal(keys[16], vec_shape),
        'layer_scale2': jax.random.uniform(keys[17], vec_shape, minval=0.2, maxval=0.8),
    }


def layer_norm(x_tok, norm_gain, norm_shift):
    x_f32 = x_tok.astype(jnp.float32)
    centered = x_f32 - jnp.mean(x_f32, axis=-1, keepdims=True)
    var_val = jnp.mean(centered * centered, axis=-1, keepdims=True)
    return centered * lax.rsqrt(var_val + NORM_EPS) * norm_gain + norm_shift


def one_block(x_seq, key_mask, layer_prm):
    (norm1_gain, norm1_bias, w_qkv, b_qkv, w_proj, b_proj, layer_scale1,
     norm2_gain, norm2_bias, w_up, b_up, w_down, b_down, layer_scale2) = layer_prm
    normed = layer_norm(x_seq, norm1_gain, norm1_bias).astype(jnp.bfloat16).astype(jnp.float32)
    qkv_heads = (jnp.einsum('nd,cdhe->cnhe', normed, w_qkv) + b_qkv[:, None]).astype(jnp.bfloat16).astype(jnp.float32)
    scores = jnp.einsum('qhe,khe->hqk', qkv_heads[0], qkv_heads[1]) * (HEAD_DIM ** -0.5)
    attn_probs = jax.nn.softmax(jnp.where(key_mask, scores, NEG_BIG), axis=-1).astype(jnp.bfloat16).astype(jnp.float32)
    attn_heads = jnp.einsum('hqk,khe->qhe', attn_probs, qkv_heads[2]).astype(jnp.bfloat16).astype(jnp.float32)
    attn_sum = jnp.einsum('qhe,hed->qd', attn_heads, w_proj) + b_proj
    x_mid = (x_seq.astype(jnp.float32) + layer_scale1 * attn_sum).astype(jnp.bfloat16)
    normed2 = layer_norm(x_mid, norm2_gain, norm2_bias).astype(jnp.bfloat16).astype(jnp.float32)
    pre_act = jnp.einsum('nd,cdf->cnf', normed2, w_up) + b_up[:, None]
    hidden = (jax.nn.silu(pre_act[0]) * pre_act[1]).astype(jnp.bfloat16).astype(jnp.float32)
    mlp_sum = jnp.dot(hidden, w_down) + b_down
    return (x_mid.astype(jnp.float32) + layer_scale2 * mlp_sum).astype(jnp.bfloat16)


def two_blocks(x_seq, key_mask, params_f32):
    def body(x_carry, layer_prm):
        return one_block(x_carry, key_mask, layer_prm), None
    return lax.scan(body, x_seq, params_f32)[0]


def reference(tokens, grad_y, valid_len, norm1_gain, norm1_bias, w_qkv, b_qkv, w_proj, b_proj, layer_scale1,
              norm2_gain, norm2_bias, w_up, b_up, w_down, b_down, layer_scale2):
    params = (norm1_gain, norm1_bias, w_qkv, b_qkv, w_proj, b_proj, layer_scale1,
              norm2_gain, norm2_bias, w_up, b_up, w_down, b_down, layer_scale2)
    params_f32 = tuple(param_arr.astype(jnp.float32) for param_arr in params)
    positions = jnp.arange(SEQ_LEN)

    def per_seq(grad_acc, seq_row):
        x_seq, dy_seq, seq_len = seq_row
        key_mask = positions < seq_len

        def forward(x_in, params_in):
            return two_blocks(x_in, key_mask, params_in)

        y_seq, pull_back = jax.vjp(forward, x_seq, params_f32)
        dx_seq, grad_params = pull_back(dy_seq)
        grad_acc = tuple(acc_arr + grad_arr for acc_arr, grad_arr in zip(grad_acc, grad_params))
        return grad_acc, (y_seq, dx_seq)

    grad_init = tuple(jnp.zeros_like(param_arr) for param_arr in params_f32)
    grad_sums, seq_outs = lax.scan(per_seq, grad_init, (tokens, grad_y, valid_len))
    return (seq_outs[0], seq_outs[1], grad_sums[0], grad_sums[1], grad_sums[2], grad_sums[3], grad_sums[4],
            grad_sums[5], grad_sums[6], grad_sums[7], grad_sums[8], grad_sums[9], grad_sums[10], grad_sums[11],
            grad_sums[12], grad_sums[13])
```

```python
import jax
import jax.numpy as jnp
from jax import lax
from jax.sharding import PartitionSpec as P

NORM_EPS = 1e-6
NEG_BIG = -1e9
SHARED_SLOTS = (0, 1, 5, 6, 7, 8, 12, 13)
F32 = jnp.float32
BF16 = jnp.bfloat16


def dot(spec, a, b):
    return jnp.einsum(spec, a, b, preferred_element_type=F32)


def swap_dp(x):
    return lax.ppermute(x, 'dp', [(0, 1), (1, 0)])


def both(own, other, axis=0):
    return jnp.concatenate([own, other], axis=axis)


def norm_fwd(x_tok, norm_gain, norm_shift):
    x_f32 = x_tok.astype(F32)
    centered = x_f32 - jnp.mean(x_f32, axis=-1, keepdims=True)
    inv_std = lax.rsqrt(jnp.mean(centered * centered, axis=-1, keepdims=True) + NORM_EPS)
    x_hat = centered * inv_std
    return (x_hat * norm_gain + norm_shift).astype(BF16), x_hat, inv_std


def norm_bwd(grad_out, x_hat, inv_std, norm_gain):
    grad_hat = grad_out * norm_gain
    mean_one = jnp.mean(grad_hat, axis=-1, keepdims=True)
    mean_two = jnp.mean(grad_hat * x_hat, axis=-1, keepdims=True)
    grad_in = inv_std * (grad_hat - mean_one - x_hat * mean_two)
    return grad_in, jnp.sum(grad_out * x_hat, axis=(0, 1)), jnp.sum(grad_out, axis=(0, 1))


def gather_tp(x):
    return lax.all_gather(x, 'tp', axis=1, tiled=True)


def scatter_tp(x):
    return lax.psum_scatter(x, 'tp', scatter_dimension=1, tiled=True).astype(F32)


def attn_fwd(normed, key_mask, w_qkv, b_qkv):
    qkv = (dot('bnd,cdhe->cbnhe', normed, w_qkv) + b_qkv[:, None, None]).astype(BF16)
    scores = dot('bqhe,bkhe->bhqk', qkv[0], qkv[1]) * (qkv.shape[-1] ** -0.5)
    probs = jax.nn.softmax(jnp.where(key_mask, scores, NEG_BIG), axis=-1)
    probs_bf = probs.astype(BF16)
    heads = dot('bhqk,bkhe->bqhe', probs_bf, qkv[2]).astype(BF16)
    return heads, (qkv, probs, probs_bf)


def attn_bwd(grad_out_full, saved, w_proj):
    qkv, probs, probs_bf = saved
    grad_attn = dot('cre,ife->crif', grad_out_full, w_proj).astype(BF16)
    grad_probs = dot('bqhe,bkhe->bhqk', grad_attn, qkv[2])
    grad_val = dot('bhqk,bqhe->bkhe', probs_bf, grad_attn)
    grad_scores = (probs * (grad_probs - jnp.sum(grad_probs * probs, axis=-1, keepdims=True))
                   * (qkv.shape[-1] ** -0.5)).astype(BF16)
    grad_query = dot('bhqk,bkhe->bqhe', grad_scores, qkv[1])
    grad_key = dot('bhqk,bqhe->bkhe', grad_scores, qkv[0])
    grad_qkv = jnp.stack([grad_query, grad_key, grad_val])
    return grad_qkv.astype(BF16), jnp.sum(grad_qkv, axis=(1, 2))


def mlp_up(normed, w_up, b_up):
    pre = dot('bnd,cdf->cbnf', normed, w_up) + b_up[:, None, None]
    return pre, (jax.nn.silu(pre[0]) * pre[1]).astype(BF16)


def mlp_bwd(grad_mlp_full, pre, w_down):
    grad_hidden = dot('bnd,fd->bnf', grad_mlp_full, w_down)
    gate_sig = jax.nn.sigmoid(pre[0])
    grad_gate = grad_hidden * pre[1] * gate_sig * (1.0 + pre[0] * (1.0 - gate_sig))
    grad_lin = grad_hidden * pre[0] * gate_sig
    grad_pre = jnp.stack([grad_gate, grad_lin])
    return grad_pre.astype(BF16), jnp.sum(grad_pre, axis=(1, 2))


def block_fwd(x_loc, masks, prm):
    (norm1_gain, norm1_bias, w_qkv, b_qkv, w_proj, b_proj, layer_scale1,
     norm2_gain, norm2_bias, w_up, b_up, w_down, b_down, layer_scale2) = prm
    n1, hat_one, std_one = norm_fwd(x_loc, norm1_gain, norm1_bias)
    n1_own = gather_tp(n1)
    n1_oth = swap_dp(n1_own)
    heads_own, att_own = attn_fwd(n1_own, masks[0], w_qkv, b_qkv)
    proj_part = dot('crif,ife->cre', heads_own, w_proj).astype(BF16)
    attn_sum = scatter_tp(proj_part) + b_proj
    heads_oth, att_oth = attn_fwd(n1_oth, masks[1], w_qkv, b_qkv)
    x_mid = (x_loc.astype(F32) + layer_scale1 * attn_sum).astype(BF16)
    n2, hat_two, std_two = norm_fwd(x_mid, norm2_gain, norm2_bias)
    n2_own = gather_tp(n2)
    n2_oth = swap_dp(n2_own)
    pre_own, hid_own = mlp_up(n2_own, w_up, b_up)
    mlp_part = dot('bnf,fd->bnd', hid_own, w_down).astype(BF16)
    mlp_sum = scatter_tp(mlp_part) + b_down
    pre_oth, hid_oth = mlp_up(n2_oth, w_up, b_up)
    x_out = (x_mid.astype(F32) + layer_scale2 * mlp_sum).astype(BF16)
    saved = (hat_one, std_one, both(n1_own, n1_oth), att_own, att_oth, both(heads_own, heads_oth), attn_sum,
             hat_two, std_two, both(n2_own, n2_oth), pre_own, pre_oth, both(hid_own, hid_oth), mlp_sum)
    return x_out, saved


def block_bwd(grad_x, saved, prm):
    (norm1_gain, norm1_bias, w_qkv, b_qkv, w_proj, b_proj, layer_scale1,
     norm2_gain, norm2_bias, w_up, b_up, w_down, b_down, layer_scale2) = prm
    (hat_one, std_one, n1_all, att_own, att_oth, heads_all, attn_sum,
     hat_two, std_two, n2_all, pre_own, pre_oth, hid_all, mlp_sum) = saved
    grad_res = grad_x.astype(F32)
    grad_ls2 = jnp.sum(grad_res * mlp_sum, axis=(0, 1))
    grad_mlp = layer_scale2 * grad_res
    grad_b_down = jnp.sum(grad_mlp, axis=(0, 1))
    gm_own = gather_tp(grad_mlp.astype(BF16))
    gm_oth = swap_dp(gm_own)
    gp_own, gb_own = mlp_bwd(gm_own, pre_own, w_down)
    norm2_part = dot('cbnf,cdf->bnd', gp_own, w_up).astype(BF16)
    grad_normed2 = scatter_tp(norm2_part)
    gp_oth, gb_oth = mlp_bwd(gm_oth, pre_oth, w_down)
    grad_b_up = gb_own + gb_oth
    grad_w_down = dot('bnf,bnd->fd', hid_all, both(gm_own, gm_oth))
    grad_w_up = dot('bnd,cbnf->cdf', n2_all, both(gp_own, gp_oth, 1))
    grad_from2, grad_n2g, grad_n2b = norm_bwd(grad_normed2, hat_two, std_two, norm2_gain)
    grad_mid = grad_res + grad_from2
    grad_ls1 = jnp.sum(grad_mid * attn_sum, axis=(0, 1))
    grad_attn_out = layer_scale1 * grad_mid
    grad_b_proj = jnp.sum(grad_attn_out, axis=(0, 1))
    ga_own = gather_tp(grad_attn_out.astype(BF16))
    ga_oth = swap_dp(ga_own)
    gq_own, gbq_own = attn_bwd(ga_own, att_own, w_proj)
    norm1_part = dot('cbnhe,cdhe->bnd', gq_own, w_qkv).astype(BF16)
    grad_normed = scatter_tp(norm1_part)
    gq_oth, gbq_oth = attn_bwd(ga_oth, att_oth, w_proj)
    grad_b_qkv = gbq_own + gbq_oth
    grad_w_proj = dot('crif,cre->ife', heads_all, both(ga_own, ga_oth))
    grad_w_qkv = dot('bnd,cbnhe->cdhe', n1_all, both(gq_own, gq_oth, 1))
    grad_from1, grad_n1g, grad_n1b = norm_bwd(grad_normed, hat_one, std_one, norm1_gain)
    grad_in = (grad_mid + grad_from1).astype(BF16)
    layer_grads = (grad_n1g, grad_n1b, grad_w_qkv, grad_b_qkv, grad_w_proj, grad_b_proj, grad_ls1,
                   grad_n2g, grad_n2b, grad_w_up, grad_b_up, grad_w_down, grad_b_down, grad_ls2)
    return grad_in, layer_grads


def solution(mesh):
    tp_size = mesh.shape['tp']
    small_spec = P()
    act_spec = P('dp', 'tp', None)
    param_specs = (small_spec, small_spec, P(None, None, None, 'tp', None), P(None, None, 'tp', None),
                   P(None, 'tp', None, None), small_spec, small_spec, small_spec, small_spec,
                   P(None, None, None, 'tp'), P(None, None, 'tp'), P(None, 'tp', None), small_spec, small_spec)

    def device_fn(tokens, grad_y, valid_len, *params):
        num_blocks = params[0].shape[0]
        positions = jnp.arange(tokens.shape[1] * tp_size)
        masks = [(positions[None, :] < vl[:, None])[:, None, None, :] for vl in (valid_len, swap_dp(valid_len))]
        x_cur = tokens
        saved_all = []
        for layer_idx in range(num_blocks):
            prm = tuple(param_arr[layer_idx] for param_arr in params)
            x_cur, saved = block_fwd(x_cur, masks, prm)
            saved_all.append(saved)
        grad_cur = grad_y
        grads_rev = []
        for layer_idx in reversed(range(num_blocks)):
            prm = tuple(param_arr[layer_idx] for param_arr in params)
            grad_cur, layer_grads = block_bwd(grad_cur, saved_all[layer_idx], prm)
            grads_rev.append(layer_grads)
        grads_fwd = grads_rev[::-1]
        stacked = [jnp.stack([one_grads[slot] for one_grads in grads_fwd]) for slot in range(len(params))]
        shared_sums = lax.psum(tuple(stacked[slot] for slot in SHARED_SLOTS), ('dp', 'tp'))
        for out_pos, slot in enumerate(SHARED_SLOTS):
            stacked[slot] = shared_sums[out_pos]
        return (x_cur, grad_cur) + tuple(stacked)

    return jax.shard_map(device_fn, mesh=mesh, in_specs=(act_spec, act_spec, P('dp')) + param_specs,
                         out_specs=(act_spec, act_spec) + param_specs, check_vma=False)
```

```python
import jax
import jax.numpy as jnp
from jax import lax
from jax.experimental import pallas as pl
from jax.experimental.pallas import tpu as pltpu
from jax.sharding import PartitionSpec as P

NORM_EPS = 1e-6
NEG_BIG = -1e9
F32 = jnp.float32
BF16 = jnp.bfloat16
TOK = 66
PAD = 72
MESH_ID = pl.DeviceIdType.MESH


def stage_call(cid, rs, ag, local_fn, part, ins, out_shapes):
    n_seq, pad, width = ins[0].shape
    n_tp = 4
    n_in = len(ins)
    n_out = len(out_shapes)

    def kernel(*refs):
        pos = 0
        if rs:
            part_ref = refs[0]
            pos = 1
        in_refs = refs[pos:pos + n_in]
        pos += n_in
        out_refs = refs[pos:pos + n_out]
        pos += n_out
        if ag:
            full = refs[pos]
            pos += 1
        far_buf, mate_buf, peer_buf, send_buf, ssem, rsem = refs[pos:]
        dp = lax.axis_index('dp')
        t = lax.axis_index('tp')
        core = lax.rem(t, 2)
        mate = t + 1 - 2 * core
        peer = lax.rem(t + 2, n_tp)
        far = lax.rem(mate + 2, n_tp)

        def remote(src, dst, k, dev):
            return pltpu.make_async_remote_copy(src_ref=src, dst_ref=dst, send_sem=ssem.at[k], recv_sem=rsem.at[k],
                                                device_id=(dp, dev), device_id_type=MESH_ID)

        barrier = pltpu.get_barrier_semaphore()
        for dev in (mate, peer):
            pl.semaphore_signal(barrier, inc=1, device_id=(dp, dev), device_id_type=MESH_ID)
        pl.semaphore_wait(barrier, 2)

        started = []
        if rs:
            c_far = [remote(part_ref.at[b, far], far_buf.at[b], b, mate) for b in range(n_seq)]
            c_mate = [remote(part_ref.at[b, mate], mate_buf.at[b], n_seq + b, mate) for b in range(n_seq)]
            for cp in c_far + c_mate:
                cp.start()
            c_peer = []
            for b in range(n_seq):
                c_far[b].wait_recv()
                send_buf[b] = (part_ref[b, peer].astype(F32) + far_buf[b].astype(F32)).astype(BF16)
                cp = remote(send_buf.at[b], peer_buf.at[b], 2 * n_seq + b, peer)
                cp.start()
                c_peer.append(cp)
            started += c_far + c_mate + c_peer
        g_peer, g_mate = [], []
        for b in range(n_seq):
            acc = None
            if rs:
                c_mate[b].wait_recv()
                acc = part_ref[b, t].astype(F32) + mate_buf[b].astype(F32)
                c_peer[b].wait_recv()
                acc = acc + peer_buf[b].astype(F32)
            val = local_fn(b, acc, in_refs, out_refs)
            if ag:
                full[b, t] = val
                cp = remote(full.at[b, t], full.at[b, t], 3 * n_seq + b, peer)
                cp.start()
                g_peer.append(cp)
                cp = remote(full.at[b, t], full.at[b, t], 4 * n_seq + b, mate)
                cp.start()
                g_mate.append(cp)
        if ag:
            g_fwd = []
            for b in range(n_seq):
                g_peer[b].wait_recv()
                cp = remote(full.at[b, peer], full.at[b, peer], 5 * n_seq + b, mate)
                cp.start()
                g_fwd.append(cp)
            for b in range(n_seq):
                g_mate[b].wait_recv()
            for b in range(n_seq):
                g_fwd[b].wait_recv()
            started += g_peer + g_mate + g_fwd
        for cp in started:
            cp.wait_send()

    outs = list(out_shapes)
    if ag:
        outs.append(jax.ShapeDtypeStruct((n_seq, n_tp, pad, width), BF16))
    args = ([part] if rs else []) + list(ins)
    vm = pl.BlockSpec(memory_space=pltpu.VMEM)
    shard = (n_seq, pad, width)
    return pl.pallas_call(
        kernel,
        out_shape=outs,
        in_specs=[vm] * len(args),
        out_specs=[vm] * len(outs),
        scratch_shapes=[pltpu.VMEM(shard, BF16)] * 4 + [pltpu.SemaphoreType.DMA((6 * n_seq,))] * 2,
        compiler_params=pltpu.CompilerParams(collective_id=cid, has_side_effects=True, vmem_limit_bytes=24 * 2 ** 20),
        cost_estimate=pl.CostEstimate(flops=40_000_000, bytes_accessed=4_000_000, transcendentals=0),
        name=f'stage{cid}',
    )(*args)


def ln_stats(x):
    x_f32 = x.astype(F32)
    centered = x_f32 - jnp.mean(x_f32, axis=-1, keepdims=True)
    inv_std = lax.rsqrt(jnp.mean(centered * centered, axis=-1, keepdims=True) + NORM_EPS)
    return centered * inv_std, inv_std


def ln_bwd(grad_out, x, gain):
    x_hat, inv_std = ln_stats(x)
    grad_hat = grad_out * gain
    mean_one = jnp.mean(grad_hat, axis=-1, keepdims=True)
    mean_two = jnp.mean(grad_hat * x_hat, axis=-1, keepdims=True)
    return inv_std * (grad_hat - mean_one - x_hat * mean_two), x_hat


def add_rows(rows_ref, b, rows):
    for k, val in enumerate(rows):
        s = jnp.sum(val, axis=0, keepdims=True)
        rows_ref[k:k + 1, :] = s if b == 0 else rows_ref[k:k + 1, :] + s


def key_valid(rows, n_keys, seq_len):
    col = lax.broadcasted_iota(jnp.int32, (rows, n_keys), 1)
    shard = jnp.zeros_like(col)
    for k in range(1, n_keys // PAD):
        shard = shard + (col >= k * PAD).astype(jnp.int32)
    return jnp.logical_and(col - PAD * shard < TOK, col - (PAD - TOK) * shard < seq_len)


def mm(a, b, dims=((1,), (0,))):
    return lax.dot_general(a, b, (dims, ((), ())), preferred_element_type=F32)


def head_probs(q_half, k_pair, valid):
    scores = mm(q_half, k_pair, ((1,), (1,))) * 0.125
    scores = jnp.where(valid, scores, NEG_BIG)
    e = jnp.exp(scores - jnp.max(scores, axis=-1, keepdims=True))
    return e / jnp.sum(e, axis=-1, keepdims=True)


def attn_fwd_kernel(vl_ref, qkv_ref, o_ref):
    rows = qkv_ref.shape[1]
    valid = key_valid(rows, rows, vl_ref[pl.program_id(0)])
    half = lax.broadcasted_iota(jnp.int32, (rows, 128), 1) // 64
    for pair in range(2):
        cols = slice(128 * pair, 128 * pair + 128)
        q, k, v = qkv_ref[0, :, cols], qkv_ref[1, :, cols], qkv_ref[2, :, cols]
        outs = []
        for h in range(2):
            probs = head_probs(jnp.where(half == h, q, jnp.zeros_like(q)), k, valid)
            outs.append(mm(probs.astype(BF16), v))
        o_ref[:, cols] = jnp.where(half == 0, outs[0], outs[1]).astype(BF16)


def attn_bwd_kernel(vl_ref, qkv_ref, do_ref, dqkv_ref, db_ref):
    rows = qkv_ref.shape[1]
    valid = key_valid(rows, rows, vl_ref[pl.program_id(0)])
    half = lax.broadcasted_iota(jnp.int32, (rows, 128), 1) // 64

    @pl.when(pl.program_id(0) == 0)
    def _():
        db_ref[...] = jnp.zeros_like(db_ref)

    for pair in range(2):
        cols = slice(128 * pair, 128 * pair + 128)
        q, k, v = qkv_ref[0, :, cols], qkv_ref[1, :, cols], qkv_ref[2, :, cols]
        do = do_ref[:, cols]
        dq, dk, dv = [], [], []
        for h in range(2):
            probs = head_probs(jnp.where(half == h, q, jnp.zeros_like(q)), k, valid)
            grad_p = mm(jnp.where(half == h, do, jnp.zeros_like(do)), v, ((1,), (1,)))
            grad_s = (probs * (grad_p - jnp.sum(grad_p * probs, axis=-1, keepdims=True)) * 0.125).astype(BF16)
            dv.append(mm(probs.astype(BF16), do, ((0,), (0,))))
            dq.append(mm(grad_s, k))
            dk.append(mm(grad_s, q, ((0,), (0,))))
        for c, pieces in enumerate((dq, dk, dv)):
            val = jnp.where(half == 0, pieces[0], pieces[1])
            dqkv_ref[c, :, cols] = val.astype(BF16)
            db_ref[c:c + 1, cols] += jnp.sum(val, axis=0, keepdims=True)


def attn_fwd(qkv, seq_len):
    n_seq = seq_len.shape[0]
    rows = qkv.shape[1] // n_seq
    return pl.pallas_call(
        attn_fwd_kernel,
        grid=(n_seq,),
        in_specs=[pl.BlockSpec(memory_space=pltpu.SMEM), pl.BlockSpec((3, rows, 256), lambda b: (0, b, 0))],
        out_specs=pl.BlockSpec((rows, 256), lambda b: (b, 0)),
        out_shape=jax.ShapeDtypeStruct((n_seq * rows, 256), BF16),
        compiler_params=pltpu.CompilerParams(vmem_limit_bytes=24 * 2 ** 20),
        cost_estimate=pl.CostEstimate(flops=2_000_000_000, bytes_accessed=2_000_000, transcendentals=0),
        name='attn_fwd')(seq_len, qkv)


def attn_bwd(qkv, grad_o, seq_len):
    n_seq = seq_len.shape[0]
    rows = qkv.shape[1] // n_seq
    return pl.pallas_call(
        attn_bwd_kernel,
        grid=(n_seq,),
        in_specs=[pl.BlockSpec(memory_space=pltpu.SMEM), pl.BlockSpec((3, rows, 256), lambda b: (0, b, 0)),
                  pl.BlockSpec((rows, 256), lambda b: (b, 0))],
        out_specs=[pl.BlockSpec((3, rows, 256), lambda b: (0, b, 0)), pl.BlockSpec((3, 256), lambda b: (0, 0))],
        out_shape=[jax.ShapeDtypeStruct((3, n_seq * rows, 256), BF16), jax.ShapeDtypeStruct((3, 256), F32)],
        compiler_params=pltpu.CompilerParams(vmem_limit_bytes=24 * 2 ** 20, dimension_semantics=('arbitrary',)),
        cost_estimate=pl.CostEstimate(flops=4_000_000_000, bytes_accessed=3_000_000, transcendentals=0),
        name='attn_bwd')(seq_len, qkv, grad_o)


def wgrad_kernel(a0_ref, a1_ref, b0_ref, b1_ref, *rest):
    out_ref = rest[-1]
    out_ref[...] = mm(a0_ref[...], b0_ref[...], ((0,), (0,))) + mm(a1_ref[...], b1_ref[...], ((0,), (0,)))


def wgrad(layer, a_pair, b_pair, a_index, b_index, groups, n_blk, buf, name):
    rows, width = b_pair[0].shape[-2:]
    blk = 256
    a_block = (rows, blk) if a_pair[0].ndim == 2 else (pl.squeezed, rows, blk)
    b_block = (rows, width) if b_pair[0].ndim == 2 else (pl.squeezed, rows, width)
    a_spec = pl.BlockSpec(a_block, a_index)
    b_spec = pl.BlockSpec(b_block, b_index)
    out_spec = pl.BlockSpec((pl.squeezed, pl.squeezed, blk, width), lambda g, i: (layer, g, i, 0))
    args = [a_pair[0], a_pair[1], b_pair[0], b_pair[1]]
    in_specs = [a_spec, a_spec, b_spec, b_spec]
    alias = {}
    if buf is not None:
        args.append(buf)
        in_specs.append(pl.BlockSpec(memory_space=pl.ANY))
        alias = {4: 0}
    return pl.pallas_call(
        wgrad_kernel,
        grid=(groups, n_blk),
        in_specs=in_specs,
        out_specs=out_spec,
        out_shape=jax.ShapeDtypeStruct((2, groups, n_blk * blk, width), F32),
        input_output_aliases=alias,
        compiler_params=pltpu.CompilerParams(vmem_limit_bytes=32 * 2 ** 20),
        cost_estimate=pl.CostEstimate(flops=4 * rows * width * blk * groups * n_blk, bytes_accessed=8_000_000,
                                      transcendentals=0),
        name=name)(*args)


def dot(spec, a, b):
    return jnp.einsum(spec, a, b, preferred_element_type=F32)


def swap_dp(x):
    return lax.ppermute(x, 'dp', [(0, 1), (1, 0)])


def flat(x):
    return x.reshape(-1, x.shape[-1])


def shards(x):
    return x.reshape(2, 4, PAD, x.shape[-1])


def row(ref, layer):
    return ref[layer:layer + 1, :]


def gather_norm(cid, layer, x, gain, bias):
    def local(b, acc, ins, outs):
        x_ref, g_ref, b_ref = ins
        x_hat, _ = ln_stats(x_ref[b])
        return (x_hat * row(g_ref, layer) + row(b_ref, layer)).astype(BF16)
    return stage_call(cid, False, True, local, None, (x, gain, bias), [])[0]


def gather_scaled(cid, layer, g, scale):
    def local(b, acc, ins, outs):
        g_ref, s_ref = ins
        return (row(s_ref, layer) * g_ref[b].astype(F32)).astype(BF16)
    return stage_call(cid, False, True, local, None, (g, scale), [])[0]


def residual_norm(cid, layer, part, x, bias, scale, norm_layer, gain, shift):
    def local(b, acc, ins, outs):
        x_ref, b_ref, s_ref, g_ref, h_ref = ins
        total = acc + row(b_ref, layer)
        outs[1][b] = total
        x_new = (x_ref[b].astype(F32) + row(s_ref, layer) * total).astype(BF16)
        outs[0][b] = x_new
        x_hat, _ = ln_stats(x_new)
        return (x_hat * row(g_ref, norm_layer) + row(h_ref, norm_layer)).astype(BF16)
    shp = [jax.ShapeDtypeStruct(x.shape, BF16), jax.ShapeDtypeStruct(x.shape, F32)]
    return stage_call(cid, True, True, local, part, (x, bias, scale, gain, shift), shp)


def residual_last(cid, layer, part, x, bias, scale, grad_y):
    def local(b, acc, ins, outs):
        x_ref, b_ref, s_ref, g_ref = ins
        total = acc + row(b_ref, layer)
        outs[0][b] = (x_ref[b].astype(F32) + row(s_ref, layer) * total).astype(BF16)
        grad = g_ref[b].astype(F32)
        add_rows(outs[1], b, [grad * total, row(s_ref, layer) * grad])
    shp = [jax.ShapeDtypeStruct(x.shape, BF16), jax.ShapeDtypeStruct((2, x.shape[-1]), F32)]
    return stage_call(cid, True, False, local, part, (x, bias, scale, grad_y), shp)


def back_mid(cid, layer, part, x_mid, gain, grad_res, attn_sum, scale):
    def local(b, acc, ins, outs):
        x_ref, g_ref, r_ref, a_ref, s_ref = ins
        grad_in, x_hat = ln_bwd(acc, x_ref[b], row(g_ref, layer))
        grad_mid = r_ref[b].astype(F32) + grad_in
        outs[0][b] = grad_mid
        grad_attn = row(s_ref, layer) * grad_mid
        add_rows(outs[1], b, [acc * x_hat, acc, grad_mid * a_ref[b], grad_attn])
        return grad_attn.astype(BF16)
    shp = [jax.ShapeDtypeStruct(x_mid.shape, F32), jax.ShapeDtypeStruct((4, x_mid.shape[-1]), F32)]
    return stage_call(cid, True, True, local, part, (x_mid, gain, grad_res, attn_sum, scale), shp)


def back_in(cid, layer, part, x_in, gain, grad_mid, mlp_sum, scale):
    more = layer > 0

    def local(b, acc, ins, outs):
        x_ref, g_ref, m_ref = ins[:3]
        grad_in, x_hat = ln_bwd(acc, x_ref[b], row(g_ref, layer))
        grad = (m_ref[b] + grad_in).astype(BF16)
        outs[0][b] = grad
        sums = [acc * x_hat, acc]
        if not more:
            add_rows(outs[1], b, sums)
            return None
        grad = grad.astype(F32)
        grad_mlp = row(ins[4], layer - 1) * grad
        add_rows(outs[1], b, sums + [grad * ins[3][b], grad_mlp])
        return grad_mlp.astype(BF16)
    ins = (x_in, gain, grad_mid) + ((mlp_sum, scale) if more else ())
    shp = [jax.ShapeDtypeStruct(x_in.shape, BF16), jax.ShapeDtypeStruct((4 if more else 2, x_in.shape[-1]), F32)]
    return stage_call(cid, True, more, local, part, ins, shp)


def qkv_of(normed, w, b):
    return (dot('rd,kfd->krf', flat(normed), w) + b[:, None]).astype(BF16)


def mlp_up(normed, w_up, b_up):
    pre = dot('rd,cdf->crf', flat(normed), w_up) + b_up[:, None]
    return pre, (jax.nn.silu(pre[0]) * pre[1]).astype(BF16)


def mlp_bwd(grad_mlp, pre, w_down):
    grad_hidden = dot('rd,fd->rf', flat(grad_mlp), w_down)
    gate_sig = jax.nn.sigmoid(pre[0])
    grad_gate = grad_hidden * pre[1] * gate_sig * (1.0 + pre[0] * (1.0 - gate_sig))
    grad_lin = grad_hidden * pre[0] * gate_sig
    grad_pre = jnp.stack([grad_gate, grad_lin])
    return grad_pre.astype(BF16), jnp.sum(grad_pre, axis=1)


def device_fn(tokens, grad_y, valid_len, norm1_gain, norm1_bias, w_qkv, b_qkv, w_proj, b_proj, layer_scale1,
              norm2_gain, norm2_bias, w_up, b_up, w_down, b_down, layer_scale2):
    pad = ((0, 0), (0, PAD - TOK), (0, 0))
    x0 = jnp.pad(tokens, pad)
    g_y = jnp.pad(grad_y, pad)
    lens = (valid_len, swap_dp(valid_len))
    wq = w_qkv.transpose(0, 1, 3, 4, 2).reshape(2, 3, 256, 1024)
    bq = b_qkv.reshape(2, 3, 256)
    wp = w_proj.reshape(2, 256, 1024)

    x_in, x_mid, sum1, sum2, n1, n2, qkv, heads, pre, hid = ([None, None] for _ in range(10))
    x_in[0] = x0
    n1_own = gather_norm(0, 0, x0, norm1_gain, norm1_bias)
    gm_own = gather_scaled(1, 1, g_y, layer_scale2)
    gm = (gm_own, swap_dp(gm_own))
    for l in range(2):
        n1[l] = (n1_own, swap_dp(n1_own))
        qkv_own = qkv_of(n1[l][0], wq[l], bq[l])
        o_own = attn_fwd(qkv_own, lens[0])
        part = dot('rf,fd->rd', o_own, wp[l]).astype(BF16)
        x_mid[l], sum1[l], n2_own = residual_norm(2 + 3 * l, l, shards(part), x_in[l], b_proj, layer_scale1,
                                                  l, norm2_gain, norm2_bias)
        n2[l] = (n2_own, swap_dp(n2_own))
        qkv_oth = qkv_of(n1[l][1], wq[l], bq[l])
        o_oth = attn_fwd(qkv_oth, lens[1])
        qkv[l], heads[l] = (qkv_own, qkv_oth), (o_own, o_oth)
        pre_own, hid_own = mlp_up(n2[l][0], w_up[l], b_up[l])
        part = dot('rf,fd->rd', hid_own, w_down[l]).astype(BF16)
        if l == 0:
            x_in[1], sum2[0], n1_own = residual_norm(3, 0, shards(part), x_mid[0], b_down, layer_scale2,
                                                     1, norm1_gain, norm1_bias)
        else:
            y_out, rows_y = residual_last(4, 1, shards(part), x_mid[1], b_down, layer_scale2, g_y)
        pre_oth, hid_oth = mlp_up(n2[l][1], w_up[l], b_up[l])
        pre[l], hid[l] = (pre_own, pre_oth), (hid_own, hid_oth)

    grad_x = g_y
    rows_mlp = rows_y
    g_up = g_down = g_qkv = g_proj = None
    rows_by_layer, g_b_up, g_b_qkv = [None, None], [None, None], [None, None]
    for l in (1, 0):
        gp_own, gb_own = mlp_bwd(gm[0], pre[l][0], w_down[l])
        part = dot('crf,cdf->rd', gp_own, w_up[l]).astype(BF16)
        grad_mid, rows_mid, ga_own = back_mid(6 + 2 * (1 - l), l, shards(part), x_mid[l], norm2_gain, grad_x, sum1[l],
                                              layer_scale1)
        ga = (ga_own, swap_dp(ga_own))
        gp_oth, gb_oth = mlp_bwd(gm[1], pre[l][1], w_down[l])
        g_b_up[l] = gb_own + gb_oth
        g_down = wgrad(l, hid[l], [flat(g) for g in gm], lambda g, i: (0, i), lambda g, i: (0, 0), 1, 4, g_down, 'wg_down')
        g_up = wgrad(l, [flat(n) for n in n2[l]], (gp_own, gp_oth), lambda g, i: (0, i), lambda g, i: (g, 0, 0), 2, 4,
                     g_up, 'wg_up')
        do_own = dot('rd,fd->rf', flat(ga[0]), wp[l]).astype(BF16)
        gq_own, gbq_own = attn_bwd(qkv[l][0], do_own, lens[0])
        part = dot('krf,kfd->rd', gq_own, wq[l]).astype(BF16)
        res = back_in(7 + 2 * (1 - l), l, shards(part), x_in[l], norm1_gain, grad_mid, sum2[0], layer_scale2)
        do_oth = dot('rd,fd->rf', flat(ga[1]), wp[l]).astype(BF16)
        gq_oth, gbq_oth = attn_bwd(qkv[l][1], do_oth, lens[1])
        g_b_qkv[l] = gbq_own + gbq_oth
        g_proj = wgrad(l, heads[l], [flat(g) for g in ga], lambda g, i: (0, i), lambda g, i: (0, 0), 1, 1, g_proj, 'wg_proj')
        g_qkv = wgrad(l, (gq_own, gq_oth), [flat(n) for n in n1[l]], lambda g, i: (g, 0, 0), lambda g, i: (0, 0), 3, 1,
                      g_qkv, 'wg_qkv')
        grad_x = res[0]
        rows_by_layer[l] = [res[1][:2], rows_mid, rows_mlp]
        if l:
            rows_mlp = res[1][2:]
            gm = (res[2], swap_dp(res[2]))

    sums = lax.psum(jnp.concatenate(rows_by_layer[0] + rows_by_layer[1], axis=0), ('dp', 'tp')).reshape(2, 8, -1)
    n1g, n1b, n2g, n2b, ls1, bp, ls2, bd = (sums[:, k] for k in range(8))
    return (y_out[:, :TOK], grad_x[:, :TOK], n1g, n1b,
            g_qkv.reshape(2, 3, 4, 64, 1024).transpose(0, 1, 4, 2, 3), jnp.stack(g_b_qkv).reshape(2, 3, 4, 64),
            g_proj.reshape(2, 4, 64, 1024), bp, ls1, n2g, n2b, g_up, jnp.stack(g_b_up),
            g_down.reshape(2, 1024, 1024), bd, ls2)


def solution(mesh):
    rep = P()
    act = P('dp', 'tp', None)
    param_specs = (rep, rep, P(None, None, None, 'tp', None), P(None, None, 'tp', None), P(None, 'tp', None, None), rep,
                   rep, rep, rep, P(None, None, None, 'tp'), P(None, None, 'tp'), P(None, 'tp', None), rep, rep)
    return jax.shard_map(device_fn, mesh=mesh, in_specs=(act, act, P('dp')) + param_specs,
                         out_specs=(act, act) + param_specs, check_vma=False)
```

```python
import jax
import jax.numpy as jnp
from jax import lax
from jax.experimental import pallas as pl
from jax.experimental.pallas import tpu as pltpu
from jax.sharding import PartitionSpec as P

NORM_EPS = 1e-6
NEG_BIG = -1e9
F32 = jnp.float32
BF16 = jnp.bfloat16
TOK = 66
PAD = 72
N_TP = 4
N_SEQ = 2
MESH_ID = pl.DeviceIdType.MESH


def sds(shape, dtype):
    return jax.ShapeDtypeStruct(shape, dtype)


class Filler:
    def __init__(self, ins, outs, count, body, splits):
        self.ins, self.outs, self.count, self.body, self.splits = ins, outs, count, body, splits


def stage_call(cid, rs, ag, local_fn, part, ins, out_shapes, swap=None, extra=None, fill=None, sums=None):
    n_seq, pad, width = N_SEQ, PAD, ins[0].shape[-1]
    vm = pl.BlockSpec(memory_space=pltpu.VMEM)
    spaces = {'hbm': pl.BlockSpec(memory_space=pltpu.HBM), 'vmem': vm, 'smem': pl.BlockSpec(memory_space=pltpu.SMEM)}
    args, in_specs = [], []

    def add(arr, spec=vm):
        args.append(arr)
        in_specs.append(spec)

    for arr in ([part] if rs else []) + list(ins) + ([swap] if swap is not None else []) + list(extra[1:] if extra else ()):
        add(arr)
    for arr in sums or ():
        add(arr)
    for arr, space in (fill.ins if fill else ()):
        add(arr, spaces[space])
    full_shape = sds((n_seq, N_TP, pad, width), BF16)
    outs = list(out_shapes) + [full_shape] * (bool(ag) + (swap is not None) + bool(extra))
    if sums is not None:
        outs.append(sds((16, width), F32))
    outs += list(fill.outs if fill else ())
    shard = (n_seq, pad, width)
    staged = [arr for arr, space in (fill.ins if fill else ()) if space == 'hbm']
    n_sem = 6 * n_seq + 4 + 3 * n_seq + 3
    scratch = ([pltpu.VMEM(shard, BF16)] * 4 if rs else []) + [pltpu.SemaphoreType.DMA((n_sem,))] * 2
    if sums is not None:
        scratch += [pltpu.VMEM((3, 16, width), F32)] * 2
    if staged:
        scratch += [pltpu.VMEM(a.shape, a.dtype) for a in staged] + [pltpu.SemaphoreType.DMA((len(staged),))]

    def kernel(*refs):
        refs = list(refs)

        def take(n):
            got = refs[:n]
            del refs[:n]
            return got
        part_ref = take(1)[0] if rs else None
        in_refs = take(len(ins))
        swap_ref = take(1)[0] if swap is not None else None
        extra_refs = take(len(extra) - 1) if extra else None
        sum_refs = take(len(sums)) if sums is not None else None
        fill_ins = take(len(fill.ins)) if fill else []
        out_refs = take(len(out_shapes))
        full = take(1)[0] if ag else None
        other = take(1)[0] if swap is not None else None
        extra_full = take(1)[0] if extra else None
        sum_out = take(1)[0] if sums is not None else None
        fill_outs = take(len(fill.outs)) if fill else []
        if rs:
            far_buf, mate_buf, peer_buf, send_buf = take(4)
        ssem, rsem = take(2)
        if sums is not None:
            sum_src, sum_dst = take(2)
        loads = []
        if staged:
            bufs = take(len(staged))
            lsem = take(1)[0]
            use = []
            for (_, space), ref in zip(fill.ins, fill_ins):
                if space == 'hbm':
                    k = len(loads)
                    loads.append(pltpu.make_async_copy(ref, bufs[k], lsem.at[k]))
                    loads[k].start()
                    use.append(bufs[k])
                else:
                    use.append(ref)
            fill_ins = use
        dp = lax.axis_index('dp')
        t = lax.axis_index('tp')
        core = lax.rem(t, 2)
        mate = t + 1 - 2 * core
        peer = lax.rem(t + 2, N_TP)
        far = lax.rem(mate + 2, N_TP)
        here, there = (dp, 1 - dp)

        def remote(src, dst, k, dev, row=None):
            return pltpu.make_async_remote_copy(src_ref=src, dst_ref=dst, send_sem=ssem.at[k], recv_sem=rsem.at[k],
                                                device_id=(here if row is None else row, dev), device_id_type=MESH_ID)

        barrier = pltpu.get_barrier_semaphore()
        peers = [(here, mate), (here, peer)]
        if swap is not None or sums is not None:
            peers.append((there, t))
        for dev in peers:
            pl.semaphore_signal(barrier, inc=1, device_id=dev, device_id_type=MESH_ID)
        pl.semaphore_wait(barrier, len(peers))

        started = []
        done = [0]
        loaded = [False]

        def run(n):
            if not fill or n <= 0:
                return
            if not loaded[0]:
                for cp in loads:
                    cp.wait()
                loaded[0] = True
            lo = done[0]
            hi = min(lo + n, fill.count)
            done[0] = hi
            if hi - lo == 1:
                fill.body(lo, fill_ins, fill_outs)
            elif hi > lo:
                @pl.loop(lo, hi)
                def _(i):
                    fill.body(i, fill_ins, fill_outs)

        if rs:
            c_far = [remote(part_ref.at[b, far], far_buf.at[b], b, mate) for b in range(n_seq)]
            c_mate = [remote(part_ref.at[b, mate], mate_buf.at[b], n_seq + b, mate) for b in range(n_seq)]
            for cp in c_far + c_mate:
                cp.start()
        if swap is not None:
            k0 = 6 * n_seq
            s_y = [remote(swap_ref.at[:, core + 2 * j], other.at[:, core + 2 * j], k0 + j, t, there) for j in range(2)]
            for cp in s_y:
                cp.start()
        if extra:
            k0 = 6 * n_seq + 4
            x_peer, x_mate = [], []
            for b in range(n_seq):
                extra_full[b, t] = (row(extra_refs[1], extra[0]) * extra_refs[0][b].astype(F32)).astype(BF16)
                x_peer.append(remote(extra_full.at[b, t], extra_full.at[b, t], k0 + b, peer))
                x_mate.append(remote(extra_full.at[b, t], extra_full.at[b, t], k0 + n_seq + b, mate))
                x_peer[b].start()
                x_mate[b].start()
        if rs:
            c_peer = []
            for b in range(n_seq):
                c_far[b].wait_recv()
                send_buf[b] = (part_ref[b, peer].astype(F32) + far_buf[b].astype(F32)).astype(BF16)
                cp = remote(send_buf.at[b], peer_buf.at[b], 2 * n_seq + b, peer)
                cp.start()
                c_peer.append(cp)
            started += c_far + c_mate + c_peer
            if fill:
                run(fill.splits[0])
        g_peer, g_mate, g_fwd = [], [], []
        for b in range(n_seq):
            acc = None
            if rs:
                c_mate[b].wait_recv()
                acc = part_ref[b, t].astype(F32) + mate_buf[b].astype(F32)
                c_peer[b].wait_recv()
                acc = acc + peer_buf[b].astype(F32)
            val = local_fn(b, acc, in_refs, out_refs)
            if ag:
                full[b, t] = val
                cp = remote(full.at[b, t], full.at[b, t], 3 * n_seq + b, peer)
                cp.start()
                g_peer.append(cp)
                cp = remote(full.at[b, t], full.at[b, t], 4 * n_seq + b, mate)
                cp.start()
                g_mate.append(cp)
        if sums is not None:
            k0 = n_sem - 3
            sum_src[0, 0:2, :] = out_refs[-1][...]
            at = 2
            for ref in sum_refs:
                sum_src[0, at:at + ref.shape[0], :] = ref[...]
                at += ref.shape[0]
            steps = [(here, mate), (here, peer), (there, t)]
            for k, dev in enumerate(steps):
                cp = remote(sum_src.at[k], sum_dst.at[k], k0 + k, dev[1], dev[0])
                cp.start()
                if k == 1 and fill:
                    run(fill.splits[1])
                cp.wait_recv()
                started.append(cp)
                total = sum_src[k] + sum_dst[k]
                if k < 2:
                    sum_src[k + 1] = total
                else:
                    sum_out[...] = total
        if extra:
            x_fwd = []
            for b in range(n_seq):
                x_peer[b].wait_recv()
                x_fwd.append(remote(extra_full.at[b, peer], extra_full.at[b, peer], 6 * n_seq + 4 + 2 * n_seq + b, mate))
                x_fwd[b].start()
        if ag:
            for b in range(n_seq):
                if fill:
                    run(fill.splits[1 + b])
                g_peer[b].wait_recv()
                cp = remote(full.at[b, peer], full.at[b, peer], 5 * n_seq + b, mate)
                cp.start()
                g_fwd.append(cp)
        if swap is not None:
            f_y = []
            for j in range(2):
                s_y[j].wait_recv()
                f_y.append(remote(other.at[:, core + 2 * j], other.at[:, core + 2 * j], 6 * n_seq + 2 + j, mate))
                f_y[j].start()
        if fill:
            run(fill.count)
        if ag:
            for cp in g_mate + g_fwd:
                cp.wait_recv()
            started += g_peer + g_mate + g_fwd
        if swap is not None:
            for cp in f_y:
                cp.wait_recv()
            started += s_y + f_y
        if extra:
            for cp in x_mate + x_fwd:
                cp.wait_recv()
            started += x_peer + x_mate + x_fwd
        for cp in started:
            cp.wait_send()

    return pl.pallas_call(
        kernel,
        out_shape=outs,
        in_specs=in_specs,
        out_specs=[vm] * len(outs),
        scratch_shapes=scratch,
        compiler_params=pltpu.CompilerParams(collective_id=cid, has_side_effects=True, vmem_limit_bytes=48 * 2 ** 20),
        cost_estimate=pl.CostEstimate(flops=40_000_000, bytes_accessed=4_000_000, transcendentals=0),
        name=f'stage{cid}',
    )(*args)


def row(ref, layer):
    return ref[layer:layer + 1, :]


def ln_stats(x):
    x_f32 = x.astype(F32)
    centered = x_f32 - jnp.mean(x_f32, axis=-1, keepdims=True)
    inv_std = lax.rsqrt(jnp.mean(centered * centered, axis=-1, keepdims=True) + NORM_EPS)
    return centered * inv_std, inv_std


def ln_bwd(grad_out, x, gain):
    x_hat, inv_std = ln_stats(x)
    grad_hat = grad_out * gain
    mean_one = jnp.mean(grad_hat, axis=-1, keepdims=True)
    mean_two = jnp.mean(grad_hat * x_hat, axis=-1, keepdims=True)
    return inv_std * (grad_hat - mean_one - x_hat * mean_two), x_hat


def add_rows(rows_ref, b, rows):
    for k, val in enumerate(rows):
        s = jnp.sum(val, axis=0, keepdims=True)
        rows_ref[k:k + 1, :] = s if b == 0 else rows_ref[k:k + 1, :] + s


def key_valid(rows, n_keys, seq_len):
    col = lax.broadcasted_iota(jnp.int32, (rows, n_keys), 1)
    shard = jnp.zeros_like(col)
    for k in range(1, n_keys // PAD):
        shard = shard + (col >= k * PAD).astype(jnp.int32)
    return jnp.logical_and(col - PAD * shard < TOK, col - (PAD - TOK) * shard < seq_len)


def mm(a, b, dims=((1,), (0,))):
    return lax.dot_general(a, b, (dims, ((), ())), preferred_element_type=F32)


def head_probs(q_half, k_pair, valid):
    scores = mm(q_half, k_pair, ((1,), (1,))) * 0.125
    scores = jnp.where(valid, scores, NEG_BIG)
    e = jnp.exp(scores - jnp.max(scores, axis=-1, keepdims=True))
    return e / jnp.sum(e, axis=-1, keepdims=True)


def attn_fwd_kernel(vl_ref, qkv_ref, o_ref):
    rows = qkv_ref.shape[1]
    valid = key_valid(rows, rows, vl_ref[pl.program_id(0)])
    half = lax.broadcasted_iota(jnp.int32, (rows, 128), 1) // 64
    for pair in range(2):
        cols = slice(128 * pair, 128 * pair + 128)
        q, k, v = qkv_ref[0, :, cols], qkv_ref[1, :, cols], qkv_ref[2, :, cols]
        outs = []
        for h in range(2):
            probs = head_probs(jnp.where(half == h, q, jnp.zeros_like(q)), k, valid)
            outs.append(mm(probs.astype(BF16), v))
        o_ref[:, cols] = jnp.where(half == 0, outs[0], outs[1]).astype(BF16)


def pair_bwd(q, k, v, do, valid):
    half = lax.broadcasted_iota(jnp.int32, q.shape, 1) // 64
    dq, dk, dv = [], [], []
    for h in range(2):
        probs = head_probs(jnp.where(half == h, q, jnp.zeros_like(q)), k, valid)
        grad_p = mm(jnp.where(half == h, do, jnp.zeros_like(do)), v, ((1,), (1,)))
        grad_s = (probs * (grad_p - jnp.sum(grad_p * probs, axis=-1, keepdims=True)) * 0.125).astype(BF16)
        dv.append(mm(probs.astype(BF16), do, ((0,), (0,))))
        dq.append(mm(grad_s, k))
        dk.append(mm(grad_s, q, ((0,), (0,))))
    return [jnp.where(half == 0, pieces[0], pieces[1]) for pieces in (dq, dk, dv)]


def attn_bwd_kernel(vl_ref, qkv_ref, do_ref, dqkv_ref, db_ref):
    rows = qkv_ref.shape[1]
    valid = key_valid(rows, rows, vl_ref[pl.program_id(0)])

    @pl.when(pl.program_id(0) == 0)
    def _():
        db_ref[...] = jnp.zeros_like(db_ref)

    for pair in range(2):
        cols = slice(128 * pair, 128 * pair + 128)
        q, k, v = qkv_ref[0, :, cols], qkv_ref[1, :, cols], qkv_ref[2, :, cols]
        do = do_ref[:, cols]
        for c, val in enumerate(pair_bwd(q, k, v, do, valid)):
            dqkv_ref[c, :, cols] = val.astype(BF16)
            db_ref[c:c + 1, cols] += jnp.sum(val, axis=0, keepdims=True)


def attn_fwd(qkv, seq_len):
    n_seq = seq_len.shape[0]
    rows = qkv.shape[1] // n_seq
    return pl.pallas_call(
        attn_fwd_kernel,
        grid=(n_seq,),
        in_specs=[pl.BlockSpec(memory_space=pltpu.SMEM), pl.BlockSpec((3, rows, 256), lambda b: (0, b, 0))],
        out_specs=pl.BlockSpec((rows, 256), lambda b: (b, 0)),
        out_shape=jax.ShapeDtypeStruct((n_seq * rows, 256), BF16),
        compiler_params=pltpu.CompilerParams(vmem_limit_bytes=24 * 2 ** 20),
        cost_estimate=pl.CostEstimate(flops=2_000_000_000, bytes_accessed=2_000_000, transcendentals=0),
        name='attn_fwd')(seq_len, qkv)


def attn_bwd(qkv, grad_o, seq_len):
    n_seq = seq_len.shape[0]
    rows = qkv.shape[1] // n_seq
    return pl.pallas_call(
        attn_bwd_kernel,
        grid=(n_seq,),
        in_specs=[pl.BlockSpec(memory_space=pltpu.SMEM), pl.BlockSpec((3, rows, 256), lambda b: (0, b, 0)),
                  pl.BlockSpec((rows, 256), lambda b: (b, 0))],
        out_specs=[pl.BlockSpec((3, rows, 256), lambda b: (0, b, 0)), pl.BlockSpec((3, 256), lambda b: (0, 0))],
        out_shape=[jax.ShapeDtypeStruct((3, n_seq * rows, 256), BF16), jax.ShapeDtypeStruct((3, 256), F32)],
        compiler_params=pltpu.CompilerParams(vmem_limit_bytes=24 * 2 ** 20, dimension_semantics=('arbitrary',)),
        cost_estimate=pl.CostEstimate(flops=4_000_000_000, bytes_accessed=3_000_000, transcendentals=0),
        name='attn_bwd')(seq_len, qkv, grad_o)


def wgrad_kernel(a0_ref, a1_ref, b0_ref, b1_ref, *rest):
    out_ref = rest[-1]
    out_ref[...] = mm(a0_ref[...], b0_ref[...], ((0,), (0,))) + mm(a1_ref[...], b1_ref[...], ((0,), (0,)))


def wgrad(layer, a_pair, b_pair, a_index, b_index, groups, n_blk, buf, name):
    rows, width = b_pair[0].shape[-2:]
    blk = 256
    a_block = (rows, blk) if a_pair[0].ndim == 2 else (pl.squeezed, rows, blk)
    b_block = (rows, width) if b_pair[0].ndim == 2 else (pl.squeezed, rows, width)
    a_spec = pl.BlockSpec(a_block, a_index)
    b_spec = pl.BlockSpec(b_block, b_index)
    out_spec = pl.BlockSpec((pl.squeezed, pl.squeezed, blk, width), lambda g, i: (layer, g, i, 0))
    args = [a_pair[0], a_pair[1], b_pair[0], b_pair[1]]
    in_specs = [a_spec, a_spec, b_spec, b_spec]
    alias = {}
    if buf is not None:
        args.append(buf)
        in_specs.append(pl.BlockSpec(memory_space=pl.ANY))
        alias = {4: 0}
    return pl.pallas_call(
        wgrad_kernel,
        grid=(groups, n_blk),
        in_specs=in_specs,
        out_specs=out_spec,
        out_shape=jax.ShapeDtypeStruct((2, groups, n_blk * blk, width), F32),
        input_output_aliases=alias,
        compiler_params=pltpu.CompilerParams(vmem_limit_bytes=32 * 2 ** 20),
        cost_estimate=pl.CostEstimate(flops=4 * rows * width * blk * groups * n_blk, bytes_accessed=8_000_000,
                                      transcendentals=0),
        name=name)(*args)


def fill_attn_fwd(normed, wq, bq, lens, splits):
    def body(i, ins, outs):
        n_ref, w_ref, b_ref, vl_ref = ins
        qkv_ref, o_ref = outs
        b, pair = i // 2, i % 2
        x = n_ref[b]
        rows = x.shape[0]
        cols = pl.ds(pl.multiple_of(pair * 128, 128), 128)
        pieces = []
        for c in range(3):
            val = (mm(x, w_ref[c, cols, :], ((1,), (1,))) + b_ref[c:c + 1, cols]).astype(BF16)
            qkv_ref[c, pl.ds(pl.multiple_of(b * rows, rows), rows), cols] = val
            pieces.append(val)
        q, k, v = pieces
        valid = key_valid(rows, rows, vl_ref[b])
        half = lax.broadcasted_iota(jnp.int32, (rows, 128), 1) // 64
        res = []
        for h in range(2):
            probs = head_probs(jnp.where(half == h, q, jnp.zeros_like(q)), k, valid)
            res.append(mm(probs.astype(BF16), v))
        o_ref[pl.ds(pl.multiple_of(b * rows, rows), rows), cols] = jnp.where(half == 0, res[0], res[1]).astype(BF16)
    rows = N_SEQ * N_TP * PAD
    return Filler([(normed.reshape(N_SEQ, N_TP * PAD, -1), 'hbm'), (wq, 'hbm'), (bq, 'vmem'), (lens, 'smem')],
                  [sds((3, rows, 256), BF16), sds((rows, 256), BF16)], 4, body, splits)


def fill_mlp(normed, grad, w_up, b_up, w_down, splits):
    def body(i, ins, outs):
        n_ref, g_ref, u_ref, b_ref, d_ref = ins
        hid_ref, gp_ref, gb_ref = outs
        cols = pl.ds(pl.multiple_of(i * 256, 256), 256)
        for b in range(N_SEQ):
            x = n_ref[b]
            rows = pl.ds(b * x.shape[0], x.shape[0])
            gate = mm(x, u_ref[0, :, cols]) + b_ref[0:1, cols]
            lin = mm(x, u_ref[1, :, cols]) + b_ref[1:2, cols]
            grad_hid = mm(g_ref[b], d_ref[cols, :], ((1,), (1,)))
            sig = jax.nn.sigmoid(gate)
            hid_ref[rows, cols] = (gate * sig * lin).astype(BF16)
            grad_gate = grad_hid * lin * sig * (1.0 + gate * (1.0 - sig))
            grad_lin = grad_hid * gate * sig
            for c, val in enumerate((grad_gate, grad_lin)):
                gp_ref[c, rows, cols] = val.astype(BF16)
                s = jnp.sum(val, axis=0, keepdims=True)
                gb_ref[c:c + 1, cols] = s if b == 0 else gb_ref[c:c + 1, cols] + s
    rows = N_SEQ * N_TP * PAD
    shape = (N_SEQ, N_TP * PAD, -1)
    return Filler([(normed.reshape(shape), 'hbm'), (grad.reshape(shape), 'hbm'), (w_up, 'hbm'), (b_up, 'vmem'),
                   (w_down, 'hbm')],
                  [sds((rows, 1024), BF16), sds((2, rows, 1024), BF16), sds((2, 1024), F32)], 4, body, splits)


def fill_attn_bwd(qkv, grad, wp, lens, splits):
    def body(i, ins, outs):
        qkv_ref, g_ref, w_ref, vl_ref = ins
        dqkv_ref, db_ref = outs
        b, pair = i // 2, i % 2
        g = g_ref[b]
        n_rows = g.shape[0]
        rows = pl.ds(pl.multiple_of(b * n_rows, n_rows), n_rows)
        cols = pl.ds(pl.multiple_of(pair * 128, 128), 128)
        do = mm(g, w_ref[cols, :], ((1,), (1,))).astype(BF16)
        valid = key_valid(n_rows, n_rows, vl_ref[b])
        vals = pair_bwd(qkv_ref[0, rows, cols], qkv_ref[1, rows, cols], qkv_ref[2, rows, cols], do, valid)
        for c, val in enumerate(vals):
            dqkv_ref[c, rows, cols] = val.astype(BF16)
            db_ref[b, c:c + 1, cols] = jnp.sum(val, axis=0, keepdims=True)
    return Filler([(qkv, 'hbm'), (grad.reshape(N_SEQ, N_TP * PAD, -1), 'hbm'), (wp, 'hbm'), (lens, 'smem')],
                  [sds(qkv.shape, BF16), sds((N_SEQ, 3, 256), F32)], 4, body, splits)


def dot(spec, a, b):
    return jnp.einsum(spec, a, b, preferred_element_type=F32)


def swap_dp(x):
    return lax.ppermute(x, 'dp', [(0, 1), (1, 0)])


def flat(x):
    return x.reshape(-1, x.shape[-1])


def shards(x):
    return x.reshape(2, 4, PAD, x.shape[-1])


def gather_norm(cid, layer, x, gain, bias):
    def local(b, acc, ins, outs):
        x_ref, g_ref, b_ref = ins
        x_hat, _ = ln_stats(x_ref[b])
        return (x_hat * row(g_ref, layer) + row(b_ref, layer)).astype(BF16)
    return stage_call(cid, False, True, local, None, (x, gain, bias), [])[0]


def residual_norm(cid, layer, part, x, bias, scale, norm_layer, gain, shift, **side):
    def local(b, acc, ins, outs):
        x_ref, b_ref, s_ref, g_ref, h_ref = ins
        total = acc + row(b_ref, layer)
        outs[1][b] = total
        x_new = (x_ref[b].astype(F32) + row(s_ref, layer) * total).astype(BF16)
        outs[0][b] = x_new
        x_hat, _ = ln_stats(x_new)
        return (x_hat * row(g_ref, norm_layer) + row(h_ref, norm_layer)).astype(BF16)
    shp = [sds(x.shape, BF16), sds(x.shape, F32)]
    return stage_call(cid, True, True, local, part, (x, bias, scale, gain, shift), shp, **side)


def residual_last(cid, layer, part, x, bias, scale, grad_y, **side):
    def local(b, acc, ins, outs):
        x_ref, b_ref, s_ref, g_ref = ins
        total = acc + row(b_ref, layer)
        outs[0][b] = (x_ref[b].astype(F32) + row(s_ref, layer) * total).astype(BF16)
        grad = g_ref[b].astype(F32)
        add_rows(outs[1], b, [grad * total, row(s_ref, layer) * grad])
    shp = [sds(x.shape, BF16), sds((2, x.shape[-1]), F32)]
    return stage_call(cid, True, False, local, part, (x, bias, scale, grad_y), shp, **side)


def back_mid(cid, layer, part, x_mid, gain, grad_res, attn_sum, scale, **side):
    def local(b, acc, ins, outs):
        x_ref, g_ref, r_ref, a_ref, s_ref = ins
        grad_in, x_hat = ln_bwd(acc, x_ref[b], row(g_ref, layer))
        grad_mid = r_ref[b].astype(F32) + grad_in
        outs[0][b] = grad_mid
        grad_attn = row(s_ref, layer) * grad_mid
        add_rows(outs[1], b, [acc * x_hat, acc, grad_mid * a_ref[b], grad_attn])
        return grad_attn.astype(BF16)
    shp = [sds(x_mid.shape, F32), sds((4, x_mid.shape[-1]), F32)]
    return stage_call(cid, True, True, local, part, (x_mid, gain, grad_res, attn_sum, scale), shp, **side)


def back_in(cid, layer, part, x_in, gain, grad_mid, mlp_sum, scale, **side):
    more = layer > 0

    def local(b, acc, ins, outs):
        x_ref, g_ref, m_ref = ins[:3]
        grad_in, x_hat = ln_bwd(acc, x_ref[b], row(g_ref, layer))
        grad = (m_ref[b] + grad_in).astype(BF16)
        outs[0][b] = grad
        sums = [acc * x_hat, acc]
        if not more:
            add_rows(outs[1], b, sums)
            return None
        grad = grad.astype(F32)
        grad_mlp = row(ins[4], layer - 1) * grad
        add_rows(outs[1], b, sums + [grad * ins[3][b], grad_mlp])
        return grad_mlp.astype(BF16)
    ins = (x_in, gain, grad_mid) + ((mlp_sum, scale) if more else ())
    shp = [sds(x_in.shape, BF16), sds((4 if more else 2, x_in.shape[-1]), F32)]
    return stage_call(cid, True, more, local, part, ins, shp, **side)


def qkv_of(normed, w, b):
    return (dot('rd,kfd->krf', flat(normed), w) + b[:, None]).astype(BF16)


def mlp_up(normed, w_up, b_up):
    pre = dot('rd,cdf->crf', flat(normed), w_up) + b_up[:, None]
    return pre, (jax.nn.silu(pre[0]) * pre[1]).astype(BF16)


def mlp_bwd(grad_mlp, pre, w_down):
    grad_hidden = dot('rd,fd->rf', flat(grad_mlp), w_down)
    gate_sig = jax.nn.sigmoid(pre[0])
    grad_gate = grad_hidden * pre[1] * gate_sig * (1.0 + pre[0] * (1.0 - gate_sig))
    grad_lin = grad_hidden * pre[0] * gate_sig
    grad_pre = jnp.stack([grad_gate, grad_lin])
    return grad_pre.astype(BF16), jnp.sum(grad_pre, axis=1)


def device_fn(tokens, grad_y, valid_len, norm1_gain, norm1_bias, w_qkv, b_qkv, w_proj, b_proj, layer_scale1,
              norm2_gain, norm2_bias, w_up, b_up, w_down, b_down, layer_scale2):
    pad = ((0, 0), (0, PAD - TOK), (0, 0))
    x0 = jnp.pad(tokens, pad)
    g_y = jnp.pad(grad_y, pad)
    lens = (valid_len, swap_dp(valid_len))
    wq = w_qkv.transpose(0, 1, 3, 4, 2).reshape(2, 3, 256, 1024)
    bq = b_qkv.reshape(2, 3, 256)
    wp = w_proj.reshape(2, 256, 1024)

    n1_0 = gather_norm(0, 0, x0, norm1_gain, norm1_bias)
    qkv_0 = qkv_of(n1_0, wq[0], bq[0])
    o_0 = attn_fwd(qkv_0, lens[0])
    part = dot('rf,fd->rd', o_0, wp[0]).astype(BF16)
    mid_0, asum_0, n2_0, n1_0x, gm_1 = residual_norm(
        1, 0, shards(part), x0, b_proj, layer_scale1, 0, norm2_gain, norm2_bias, swap=n1_0, extra=(1, g_y, layer_scale2))
    pre_0, hid_0 = mlp_up(n2_0, w_up[0], b_up[0])
    part = dot('rf,fd->rd', hid_0, w_down[0]).astype(BF16)
    x1, msum_0, n1_1, n2_0x, qkv_0x, o_0x = residual_norm(
        2, 0, shards(part), mid_0, b_down, layer_scale2, 1, norm1_gain, norm1_bias, swap=n2_0,
        fill=fill_attn_fwd(n1_0x, wq[0], bq[0], lens[1], (2, 1, 1)))
    qkv_1 = qkv_of(n1_1, wq[1], bq[1])
    o_1 = attn_fwd(qkv_1, lens[0])
    part = dot('rf,fd->rd', o_1, wp[1]).astype(BF16)
    mid_1, asum_1, n2_1, n1_1x = residual_norm(
        3, 1, shards(part), x1, b_proj, layer_scale1, 1, norm2_gain, norm2_bias, swap=n1_1)
    pre_1, hid_1 = mlp_up(n2_1, w_up[1], b_up[1])
    part_y = dot('rf,fd->rd', hid_1, w_down[1]).astype(BF16)

    gp_1, gb_1 = mlp_bwd(gm_1, pre_1, w_down[1])
    part = dot('crf,cdf->rd', gp_1, w_up[1]).astype(BF16)
    gmid_1, rows_mid_1, ga_1, n2_1x, qkv_1x, o_1x = back_mid(
        4, 1, shards(part), mid_1, norm2_gain, g_y, asum_1, layer_scale1, swap=n2_1,
        fill=fill_attn_fwd(n1_1x, wq[1], bq[1], lens[1], (2, 1, 1)))
    y_out, rows_mlp_1, gm_1x = residual_last(5, 1, shards(part_y), mid_1, b_down, layer_scale2, g_y, swap=gm_1)
    do_1 = dot('rd,fd->rf', flat(ga_1), wp[1]).astype(BF16)
    gq_1, gbq_1 = attn_bwd(qkv_1, do_1, lens[0])
    part = dot('krf,kfd->rd', gq_1, wq[1]).astype(BF16)
    grad_1, rows_in_1, gm_0, ga_1x, hid_1x, gp_1x, gb_1x = back_in(
        6, 1, shards(part), x1, norm1_gain, gmid_1, msum_0, layer_scale2, swap=ga_1,
        fill=fill_mlp(n2_1x, gm_1x, w_up[1], b_up[1], w_down[1], (2, 1, 1)))

    gp_0, gb_0 = mlp_bwd(gm_0, pre_0, w_down[0])
    part = dot('crf,cdf->rd', gp_0, w_up[0]).astype(BF16)
    gmid_0, rows_mid_0, ga_0, gm_0x, gq_1x, gbq_1x = back_mid(
        7, 0, shards(part), mid_0, norm2_gain, grad_1, asum_0, layer_scale1, swap=gm_0,
        fill=fill_attn_bwd(qkv_1x, ga_1x, wp[1], lens[1], (2, 1, 1)))
    do_0 = dot('rd,fd->rf', flat(ga_0), wp[0]).astype(BF16)
    gq_0, gbq_0 = attn_bwd(qkv_0, do_0, lens[0])
    part = dot('krf,kfd->rd', gq_0, wq[0]).astype(BF16)
    grad_0, rows_in_0, ga_0x, sums, hid_0x, gp_0x, gb_0x = back_in(
        8, 0, shards(part), x0, norm1_gain, gmid_0, None, None, swap=ga_0,
        fill=fill_mlp(n2_0x, gm_0x, w_up[0], b_up[0], w_down[0], (2, 1, 1)),
        sums=(rows_mid_0, rows_in_1[2:], rows_in_1[:2], rows_mid_1, rows_mlp_1))
    do_0x = dot('rd,fd->rf', flat(ga_0x), wp[0]).astype(BF16)
    gq_0x, gbq_0x = attn_bwd(qkv_0x, do_0x, lens[1])

    g_up = g_down = g_qkv = g_proj = None
    for l, (n1, n2, gm, ga, o, hid, gp, gq) in (
            (1, ((n1_1, n1_1x), (n2_1, n2_1x), (gm_1, gm_1x), (ga_1, ga_1x), (o_1, o_1x), (hid_1, hid_1x), (gp_1, gp_1x),
                 (gq_1, gq_1x))),
            (0, ((n1_0, n1_0x), (n2_0, n2_0x), (gm_0, gm_0x), (ga_0, ga_0x), (o_0, o_0x), (hid_0, hid_0x), (gp_0, gp_0x),
                 (gq_0, gq_0x)))):
        g_down = wgrad(l, hid, [flat(g) for g in gm], lambda g, i: (0, i), lambda g, i: (0, 0), 1, 4, g_down, 'wg_down')
        g_up = wgrad(l, [flat(n) for n in n2], gp, lambda g, i: (0, i), lambda g, i: (g, 0, 0), 2, 4, g_up, 'wg_up')
        g_proj = wgrad(l, o, [flat(g) for g in ga], lambda g, i: (0, i), lambda g, i: (0, 0), 1, 1, g_proj, 'wg_proj')
        g_qkv = wgrad(l, gq, [flat(n) for n in n1], lambda g, i: (g, 0, 0), lambda g, i: (0, 0), 3, 1, g_qkv, 'wg_qkv')
    g_b_up = [gb_0 + gb_0x, gb_1 + gb_1x]
    g_b_qkv = [gbq_0 + gbq_0x, gbq_1 + gbq_1x.sum(0)]
    sums = sums.reshape(2, 8, -1)
    n1g, n1b, n2g, n2b, ls1, bp, ls2, bd = (sums[:, k] for k in range(8))
    return (y_out[:, :TOK], grad_0[:, :TOK], n1g, n1b,
            g_qkv.reshape(2, 3, 4, 64, 1024).transpose(0, 1, 4, 2, 3), jnp.stack(g_b_qkv).reshape(2, 3, 4, 64),
            g_proj.reshape(2, 4, 64, 1024), bp, ls1, n2g, n2b, g_up, jnp.stack(g_b_up),
            g_down.reshape(2, 1024, 1024), bd, ls2)


def solution(mesh):
    rep = P()
    act = P('dp', 'tp', None)
    param_specs = (rep, rep, P(None, None, None, 'tp', None), P(None, None, 'tp', None), P(None, 'tp', None, None), rep,
                   rep, rep, rep, P(None, None, None, 'tp'), P(None, None, 'tp'), P(None, 'tp', None), rep, rep)
    return jax.shard_map(device_fn, mesh=mesh, in_specs=(act, act, P('dp')) + param_specs,
                         out_specs=(act, act) + param_specs, check_vma=False)
```

```python
import jax
import jax.numpy as jnp
from jax import lax
from jax.experimental import pallas as pl
from jax.experimental.pallas import tpu as pltpu
from jax.sharding import PartitionSpec as P

NORM_EPS = 1e-6
NEG_BIG = -1e9
F32 = jnp.float32
BF16 = jnp.bfloat16
TOK = 66
PAD = 72
N_TP = 4
N_SEQ = 2
MESH_ID = pl.DeviceIdType.MESH


def sds(shape, dtype):
    return jax.ShapeDtypeStruct(shape, dtype)


class Filler:
    def __init__(self, ins, outs, count, cost, body, scratch=(), end=None):
        self.ins, self.outs, self.count, self.cost, self.body = ins, outs, count, cost, body
        self.scratch, self.end = scratch, end


def stage_call(cid, rs, ag, local_fn, part, ins, out_shapes, swap=(), extra=None, fills=(), sums=None,
               budget=(4.5, 2.0, 2.5, 3.0)):
    n_seq, pad, width = N_SEQ, PAD, ins[0].shape[-1]
    vm = pl.BlockSpec(memory_space=pltpu.VMEM)
    spaces = {'hbm': pl.BlockSpec(memory_space=pltpu.HBM), 'vmem': vm, 'smem': pl.BlockSpec(memory_space=pltpu.SMEM)}
    args, in_specs = [], []

    def add(arr, spec=vm):
        args.append(arr)
        in_specs.append(spec)

    for arr in ([part] if rs else []) + list(ins) + list(swap) + list(extra[2:] if extra else ()):
        add(arr)
    for arr in sums or ():
        add(arr)
    outs = list(out_shapes) + ([sds((n_seq, N_TP, pad, width), BF16)] if ag else []) + [sds(a.shape, BF16) for a in swap]
    if extra:
        outs.append(sds((1, N_TP, pad, width), BF16))
    if sums is not None:
        outs.append(sds((16, width), F32))
    out_specs = [vm] * len(outs)
    staged = []
    for fill in fills:
        for arr, space, index in fill.ins:
            add(arr, spaces[space])
            if space == 'hbm':
                staged.append(sds(arr.shape if index is None else arr.shape[1:], arr.dtype))
        for shape, space in fill.outs:
            outs.append(shape)
            out_specs.append(spaces[space])
    shard = (n_seq, pad, width)
    k_swap = 6 * n_seq
    k_extra = k_swap + 4 * len(swap)
    k_sum = k_extra + 3
    n_sem = k_sum + 3
    scratch = ([pltpu.VMEM(shard, BF16)] * 4 if rs else []) + [pltpu.SemaphoreType.DMA((n_sem,))] * 2
    if sums is not None:
        scratch += [pltpu.VMEM((3, 16, width), F32)] * 2
    if staged:
        scratch += [pltpu.VMEM(a.shape, a.dtype) for a in staged] + [pltpu.SemaphoreType.DMA((len(staged),))]
    for fill in fills:
        scratch += list(fill.scratch)

    def kernel(*refs):
        refs = list(refs)

        def take(n):
            got = refs[:n]
            del refs[:n]
            return got
        part_ref = take(1)[0] if rs else None
        in_refs = take(len(ins))
        swap_refs = take(len(swap))
        extra_refs = take(len(extra) - 2) if extra else None
        sum_refs = take(len(sums)) if sums is not None else None
        fill_ins = [take(len(fill.ins)) for fill in fills]
        out_refs = take(len(out_shapes))
        full = take(1)[0] if ag else None
        others = take(len(swap))
        extra_full = take(1)[0] if extra else None
        sum_out = take(1)[0] if sums is not None else None
        fill_outs = [take(len(fill.outs)) for fill in fills]
        if rs:
            far_buf, mate_buf, peer_buf, send_buf = take(4)
        ssem, rsem = take(2)
        if sums is not None:
            sum_src, sum_dst = take(2)
        loads = [[] for _ in fills]
        if staged:
            bufs = take(len(staged))
            lsem = take(1)[0]
            k = 0
            for f, fill in enumerate(fills):
                for pos, (_, space, index) in enumerate(fill.ins):
                    if space == 'hbm':
                        ref = fill_ins[f][pos]
                        cp = pltpu.make_async_copy(ref if index is None else ref.at[index], bufs[k], lsem.at[k])
                        cp.start()
                        loads[f].append(cp)
                        fill_ins[f][pos] = bufs[k]
                        k += 1
        fill_scratch = [take(len(fill.scratch)) for fill in fills]
        dp = lax.axis_index('dp')
        t = lax.axis_index('tp')
        core = lax.rem(t, 2)
        mate = t + 1 - 2 * core
        peer = lax.rem(t + 2, N_TP)
        far = lax.rem(mate + 2, N_TP)
        here, there = (dp, 1 - dp)

        def remote(src, dst, k, dev, row=None):
            return pltpu.make_async_remote_copy(src_ref=src, dst_ref=dst, send_sem=ssem.at[k], recv_sem=rsem.at[k],
                                                device_id=(here if row is None else row, dev), device_id_type=MESH_ID)

        barrier = pltpu.get_barrier_semaphore()
        peers = [(here, mate), (here, peer)]
        if swap or sums is not None:
            peers.append((there, t))
        for dev in peers:
            pl.semaphore_signal(barrier, inc=1, device_id=dev, device_id_type=MESH_ID)
        pl.semaphore_wait(barrier, len(peers))

        started = []
        done = [0] * len(fills)

        def run(time):
            for f, fill in enumerate(fills):
                left = fill.count - done[f]
                n = left if time is None else min(left, int(time / fill.cost + 0.5))
                if n <= 0:
                    continue
                if done[f] == 0:
                    for cp in loads[f]:
                        cp.wait()
                lo = done[f]
                done[f] = hi = lo + n
                if n == 1:
                    fill.body(lo, fill_ins[f], fill_outs[f], fill_scratch[f])
                else:
                    @pl.loop(lo, hi)
                    def _(i, fill=fill, f=f):
                        fill.body(i, fill_ins[f], fill_outs[f], fill_scratch[f])
                if hi == fill.count and fill.end is not None:
                    fill.end(fill_ins[f], fill_outs[f], fill_scratch[f])
                if time is not None:
                    time -= n * fill.cost

        if rs:
            c_far = [remote(part_ref.at[b, far], far_buf.at[b], b, mate) for b in range(n_seq)]
            c_mate = [remote(part_ref.at[b, mate], mate_buf.at[b], n_seq + b, mate) for b in range(n_seq)]
            for cp in c_far + c_mate:
                cp.start()
        if extra:
            extra_full[0, t] = (row(extra_refs[1], extra[0]) * extra_refs[0][extra[1]].astype(F32)).astype(BF16)
            x_peer = remote(extra_full.at[0, t], extra_full.at[0, t], k_extra, peer)
            x_mate = remote(extra_full.at[0, t], extra_full.at[0, t], k_extra + 1, mate)
            x_peer.start()
            x_mate.start()
        s_y = []
        for k, (src, dst) in enumerate(zip(swap_refs, others)):
            for j in range(2):
                s_y.append(remote(src.at[:, core + 2 * j], dst.at[:, core + 2 * j], k_swap + 4 * k + j, t, there))
                s_y[-1].start()
        if rs:
            c_peer = []
            for b in range(n_seq):
                c_far[b].wait_recv()
                send_buf[b] = (part_ref[b, peer].astype(F32) + far_buf[b].astype(F32)).astype(BF16)
                cp = remote(send_buf.at[b], peer_buf.at[b], 2 * n_seq + b, peer)
                cp.start()
                c_peer.append(cp)
            started += c_far + c_mate + c_peer
            run(budget[0])
        g_peer, g_mate, g_fwd = [], [], []
        for b in range(n_seq):
            acc = None
            if rs:
                if b:
                    run(budget[1])
                c_mate[b].wait_recv()
                acc = part_ref[b, t].astype(F32) + mate_buf[b].astype(F32)
                c_peer[b].wait_recv()
                acc = acc + peer_buf[b].astype(F32)
            val = local_fn(b, acc, in_refs, out_refs)
            if ag:
                full[b, t] = val
                cp = remote(full.at[b, t], full.at[b, t], 3 * n_seq + b, peer)
                cp.start()
                g_peer.append(cp)
                cp = remote(full.at[b, t], full.at[b, t], 4 * n_seq + b, mate)
                cp.start()
                g_mate.append(cp)
        if sums is not None:
            sum_src[0, 0:2, :] = out_refs[-1][...]
            at = 2
            for ref in sum_refs:
                sum_src[0, at:at + ref.shape[0], :] = ref[...]
                at += ref.shape[0]
            steps = [(here, mate), (here, peer), (there, t)]
            for k, dev in enumerate(steps):
                cp = remote(sum_src.at[k], sum_dst.at[k], k_sum + k, dev[1], dev[0])
                cp.start()
                if k:
                    run(budget[2])
                cp.wait_recv()
                started.append(cp)
                total = sum_src[k] + sum_dst[k]
                if k < 2:
                    sum_src[k + 1] = total
                else:
                    sum_out[...] = total
        if extra:
            x_peer.wait_recv()
            x_fwd = remote(extra_full.at[0, peer], extra_full.at[0, peer], k_extra + 2, mate)
            x_fwd.start()
        if ag:
            for b in range(n_seq):
                run(budget[2 + b])
                g_peer[b].wait_recv()
                cp = remote(full.at[b, peer], full.at[b, peer], 5 * n_seq + b, mate)
                cp.start()
                g_fwd.append(cp)
        f_y = []
        for k, dst in enumerate(others):
            for j in range(2):
                s_y[2 * k + j].wait_recv()
                f_y.append(remote(dst.at[:, core + 2 * j], dst.at[:, core + 2 * j], k_swap + 4 * k + 2 + j, mate))
                f_y[-1].start()
        run(None)
        for cp in g_mate + g_fwd + f_y + ([x_mate, x_fwd] if extra else []):
            cp.wait_recv()
        started += g_peer + g_mate + g_fwd + s_y + f_y + ([x_peer, x_mate, x_fwd] if extra else [])
        for cp in started:
            cp.wait_send()

    return pl.pallas_call(
        kernel,
        out_shape=outs,
        in_specs=in_specs,
        out_specs=out_specs,
        scratch_shapes=scratch,
        compiler_params=pltpu.CompilerParams(collective_id=cid, has_side_effects=True, vmem_limit_bytes=40 * 2 ** 20),
        cost_estimate=pl.CostEstimate(flops=40_000_000, bytes_accessed=4_000_000, transcendentals=0),
        name=f'stage{cid}',
    )(*args)


def row(ref, layer):
    return ref[layer:layer + 1, :]


def ln_stats(x):
    x_f32 = x.astype(F32)
    centered = x_f32 - jnp.mean(x_f32, axis=-1, keepdims=True)
    inv_std = lax.rsqrt(jnp.mean(centered * centered, axis=-1, keepdims=True) + NORM_EPS)
    return centered * inv_std, inv_std


def ln_bwd(grad_out, x, gain):
    x_hat, inv_std = ln_stats(x)
    grad_hat = grad_out * gain
    mean_one = jnp.mean(grad_hat, axis=-1, keepdims=True)
    mean_two = jnp.mean(grad_hat * x_hat, axis=-1, keepdims=True)
    return inv_std * (grad_hat - mean_one - x_hat * mean_two), x_hat


def add_rows(rows_ref, b, rows):
    for k, val in enumerate(rows):
        s = jnp.sum(val, axis=0, keepdims=True)
        rows_ref[k:k + 1, :] = s if b == 0 else rows_ref[k:k + 1, :] + s


def key_valid(rows, n_keys, seq_len):
    col = lax.broadcasted_iota(jnp.int32, (rows, n_keys), 1)
    shard = jnp.zeros_like(col)
    for k in range(1, n_keys // PAD):
        shard = shard + (col >= k * PAD).astype(jnp.int32)
    return jnp.logical_and(col - PAD * shard < TOK, col - (PAD - TOK) * shard < seq_len)


def mm(a, b, dims=((1,), (0,))):
    return lax.dot_general(a, b, (dims, ((), ())), preferred_element_type=F32)


def head_probs(q_half, k_pair, valid):
    scores = mm(q_half, k_pair, ((1,), (1,))) * 0.125
    scores = jnp.where(valid, scores, NEG_BIG)
    e = jnp.exp(scores - jnp.max(scores, axis=-1, keepdims=True))
    return e / jnp.sum(e, axis=-1, keepdims=True)


def attn_fwd_kernel(vl_ref, qkv_ref, o_ref):
    rows = qkv_ref.shape[1]
    valid = key_valid(rows, rows, vl_ref[pl.program_id(0)])
    half = lax.broadcasted_iota(jnp.int32, (rows, 128), 1) // 64
    for pair in range(2):
        cols = slice(128 * pair, 128 * pair + 128)
        q, k, v = qkv_ref[0, :, cols], qkv_ref[1, :, cols], qkv_ref[2, :, cols]
        outs = []
        for h in range(2):
            probs = head_probs(jnp.where(half == h, q, jnp.zeros_like(q)), k, valid)
            outs.append(mm(probs.astype(BF16), v))
        o_ref[:, cols] = jnp.where(half == 0, outs[0], outs[1]).astype(BF16)


def pair_bwd(q, k, v, do, valid):
    half = lax.broadcasted_iota(jnp.int32, q.shape, 1) // 64
    dq, dk, dv = [], [], []
    for h in range(2):
        probs = head_probs(jnp.where(half == h, q, jnp.zeros_like(q)), k, valid)
        grad_p = mm(jnp.where(half == h, do, jnp.zeros_like(do)), v, ((1,), (1,)))
        grad_s = (probs * (grad_p - jnp.sum(grad_p * probs, axis=-1, keepdims=True)) * 0.125).astype(BF16)
        dv.append(mm(probs.astype(BF16), do, ((0,), (0,))))
        dq.append(mm(grad_s, k))
        dk.append(mm(grad_s, q, ((0,), (0,))))
    return [jnp.where(half == 0, pieces[0], pieces[1]) for pieces in (dq, dk, dv)]


def attn_bwd_kernel(vl_ref, qkv_ref, do_ref, dqkv_ref, db_ref):
    rows = qkv_ref.shape[1]
    valid = key_valid(rows, rows, vl_ref[pl.program_id(0)])

    @pl.when(pl.program_id(0) == 0)
    def _():
        db_ref[...] = jnp.zeros_like(db_ref)

    for pair in range(2):
        cols = slice(128 * pair, 128 * pair + 128)
        q, k, v = qkv_ref[0, :, cols], qkv_ref[1, :, cols], qkv_ref[2, :, cols]
        do = do_ref[:, cols]
        for c, val in enumerate(pair_bwd(q, k, v, do, valid)):
            dqkv_ref[c, :, cols] = val.astype(BF16)
            db_ref[c:c + 1, cols] += jnp.sum(val, axis=0, keepdims=True)


def attn_fwd(qkv, seq_len):
    n_seq = seq_len.shape[0]
    rows = qkv.shape[1] // n_seq
    return pl.pallas_call(
        attn_fwd_kernel,
        grid=(n_seq,),
        in_specs=[pl.BlockSpec(memory_space=pltpu.SMEM), pl.BlockSpec((3, rows, 256), lambda b: (0, b, 0))],
        out_specs=pl.BlockSpec((rows, 256), lambda b: (b, 0)),
        out_shape=jax.ShapeDtypeStruct((n_seq * rows, 256), BF16),
        compiler_params=pltpu.CompilerParams(vmem_limit_bytes=24 * 2 ** 20),
        cost_estimate=pl.CostEstimate(flops=2_000_000_000, bytes_accessed=2_000_000, transcendentals=0),
        name='attn_fwd')(seq_len, qkv)


def attn_bwd(qkv, grad_o, seq_len):
    n_seq = seq_len.shape[0]
    rows = qkv.shape[1] // n_seq
    return pl.pallas_call(
        attn_bwd_kernel,
        grid=(n_seq,),
        in_specs=[pl.BlockSpec(memory_space=pltpu.SMEM), pl.BlockSpec((3, rows, 256), lambda b: (0, b, 0)),
                  pl.BlockSpec((rows, 256), lambda b: (b, 0))],
        out_specs=[pl.BlockSpec((3, rows, 256), lambda b: (0, b, 0)), pl.BlockSpec((3, 256), lambda b: (0, 0))],
        out_shape=[jax.ShapeDtypeStruct((3, n_seq * rows, 256), BF16), jax.ShapeDtypeStruct((3, 256), F32)],
        compiler_params=pltpu.CompilerParams(vmem_limit_bytes=24 * 2 ** 20, dimension_semantics=('arbitrary',)),
        cost_estimate=pl.CostEstimate(flops=4_000_000_000, bytes_accessed=3_000_000, transcendentals=0),
        name='attn_bwd')(seq_len, qkv, grad_o)


def wgrad_kernel(a0_ref, a1_ref, b0_ref, b1_ref, last_ref, out_ref):
    @pl.when(pl.program_id(2) == 0)
    def _():
        out_ref[...] = mm(a0_ref[...], b0_ref[...], ((0,), (0,))) + mm(a1_ref[...], b1_ref[...], ((0,), (0,)))

    @pl.when(pl.program_id(2) == 1)
    def _():
        out_ref[...] = last_ref[...]


def wgrad(a_pair, b_pair, a_index, b_index, last, name):
    rows, width = b_pair[0].shape[-2:]
    groups, total, _ = last.shape
    blk = 256
    a_block = (rows, blk) if a_pair[0].ndim == 2 else (pl.squeezed, rows, blk)
    b_block = (rows, width) if b_pair[0].ndim == 2 else (pl.squeezed, rows, width)
    a_spec = pl.BlockSpec(a_block, lambda g, i, l: a_index(g, i))
    b_spec = pl.BlockSpec(b_block, lambda g, i, l: b_index(g, i))
    last_spec = pl.BlockSpec((pl.squeezed, blk, width), lambda g, i, l: (g, i, 0))
    return pl.pallas_call(
        wgrad_kernel,
        grid=(groups, total // blk, 2),
        in_specs=[a_spec, a_spec, b_spec, b_spec, last_spec],
        out_specs=pl.BlockSpec((pl.squeezed, pl.squeezed, blk, width), lambda g, i, l: (l, g, i, 0)),
        out_shape=jax.ShapeDtypeStruct((2, groups, total, width), F32),
        compiler_params=pltpu.CompilerParams(vmem_limit_bytes=32 * 2 ** 20),
        cost_estimate=pl.CostEstimate(flops=4 * rows * width * total * groups, bytes_accessed=8_000_000,
                                      transcendentals=0),
        name=name)(*a_pair, *b_pair, last)


ROWS = N_SEQ * N_TP * PAD


def by_seq(x):
    return x.reshape(-1, N_TP * PAD, x.shape[-1])


def fill_attn_fwd(layer, normed, wq, bq, lens):
    def body(i, ins, outs, _):
        n_ref, w_ref, b_ref, vl_ref = ins
        qkv_ref, o_ref = outs
        b, pair = i // 2, i % 2
        x = n_ref[b]
        n_rows = x.shape[0]
        rows = pl.ds(pl.multiple_of(b * n_rows, n_rows), n_rows)
        cols = pl.ds(pl.multiple_of(pair * 128, 128), 128)
        pieces = []
        for c in range(3):
            val = (mm(x, w_ref[c, cols, :], ((1,), (1,))) + b_ref[layer, c:c + 1, cols]).astype(BF16)
            qkv_ref[c, rows, cols] = val
            pieces.append(val)
        q, k, v = pieces
        valid = key_valid(n_rows, n_rows, vl_ref[b])
        half = lax.broadcasted_iota(jnp.int32, (n_rows, 128), 1) // 64
        res = []
        for h in range(2):
            probs = head_probs(jnp.where(half == h, q, jnp.zeros_like(q)), k, valid)
            res.append(mm(probs.astype(BF16), v))
        o_ref[rows, cols] = jnp.where(half == 0, res[0], res[1]).astype(BF16)
    return Filler([(by_seq(normed), 'hbm', None), (wq, 'hbm', layer), (bq, 'vmem', None), (lens, 'smem', None)],
                  [(sds((3, ROWS, 256), BF16), 'vmem'), (sds((ROWS, 256), BF16), 'vmem')], 4, 1.7, body)


def fill_mlp(layer, normed, grads, w_up, b_up, w_down):
    grads = [by_seq(g) for g in grads]

    def body(i, ins, outs, _):
        n_ref, u_ref, b_ref, d_ref = ins[:4]
        seqs = [ref.at[k] for ref in ins[4:] for k in range(ref.shape[0])]
        hid_ref, gp_ref, gb_ref = outs
        cols = pl.ds(pl.multiple_of(i * 256, 256), 256)
        for b in range(N_SEQ):
            x = n_ref[b]
            rows = pl.ds(b * x.shape[0], x.shape[0])
            gate = mm(x, u_ref[0, :, cols]) + b_ref[layer, 0:1, cols]
            lin = mm(x, u_ref[1, :, cols]) + b_ref[layer, 1:2, cols]
            grad_hid = mm(seqs[b][...], d_ref[cols, :], ((1,), (1,)))
            sig = jax.nn.sigmoid(gate)
            hid_ref[rows, cols] = (gate * sig * lin).astype(BF16)
            grad_gate = grad_hid * lin * sig * (1.0 + gate * (1.0 - sig))
            grad_lin = grad_hid * gate * sig
            for c, val in enumerate((grad_gate, grad_lin)):
                gp_ref[c, rows, cols] = val.astype(BF16)
                s = jnp.sum(val, axis=0, keepdims=True)
                gb_ref[c:c + 1, cols] = s if b == 0 else gb_ref[c:c + 1, cols] + s
    return Filler([(by_seq(normed), 'hbm', None), (w_up, 'hbm', layer), (b_up, 'vmem', None), (w_down, 'hbm', layer)]
                  + [(g, 'hbm', None) for g in grads],
                  [(sds((ROWS, 1024), BF16), 'vmem'), (sds((2, ROWS, 1024), BF16), 'vmem'), (sds((2, 1024), F32), 'vmem')],
                  4, 1.8, body)


def fill_attn_bwd(layer, qkv, grad, wp, lens):
    def body(i, ins, outs, _):
        qkv_ref, g_ref, w_ref, vl_ref = ins
        dqkv_ref, db_ref = outs
        b, pair = i // 2, i % 2
        g = g_ref[b]
        n_rows = g.shape[0]
        rows = pl.ds(pl.multiple_of(b * n_rows, n_rows), n_rows)
        cols = pl.ds(pl.multiple_of(pair * 128, 128), 128)
        do = mm(g, w_ref[cols, :], ((1,), (1,))).astype(BF16)
        valid = key_valid(n_rows, n_rows, vl_ref[b])
        vals = pair_bwd(qkv_ref[0, rows, cols], qkv_ref[1, rows, cols], qkv_ref[2, rows, cols], do, valid)
        for c, val in enumerate(vals):
            dqkv_ref[c, rows, cols] = val.astype(BF16)
            db_ref[b, c:c + 1, cols] = jnp.sum(val, axis=0, keepdims=True)
    return Filler([(qkv, 'hbm', None), (by_seq(grad), 'hbm', None), (wp, 'hbm', layer), (lens, 'smem', None)],
                  [(sds(qkv.shape, BF16), 'vmem'), (sds((N_SEQ, 3, 256), F32), 'vmem')], 4, 2.0, body)


def fill_wgrad(a_pair, b_pair, groups, n_blk, cost):
    blk, width = 256, b_pair[0].shape[-1]
    count = groups * n_blk

    def out_copy(i, outs, scratch):
        stage, sem = scratch
        at = pl.ds(pl.multiple_of((i % n_blk) * blk, blk), blk)
        return pltpu.make_async_copy(stage.at[i % 2], outs[0].at[i // n_blk, at], sem.at[i % 2])

    def body(i, ins, outs, scratch):
        g = i // n_blk
        cols = pl.ds(pl.multiple_of((i % n_blk) * blk, blk), blk)
        total = None
        for a_ref, b_ref in ((ins[0], ins[2]), (ins[1], ins[3])):
            a = a_ref[g, :, cols] if len(a_ref.shape) == 3 else a_ref[:, cols]
            b = b_ref[g] if len(b_ref.shape) == 3 else b_ref[...]
            term = mm(a, b, ((0,), (0,)))
            total = term if total is None else total + term
        if isinstance(i, int):
            if i >= 2:
                out_copy(i - 2, outs, scratch).wait()
        else:
            @pl.when(i >= 2)
            def _():
                out_copy(i - 2, outs, scratch).wait()
        scratch[0][i % 2] = total
        out_copy(i, outs, scratch).start()

    def end(ins, outs, scratch):
        for i in range(max(count - 2, 0), count):
            out_copy(i, outs, scratch).wait()
    return Filler([(x, 'hbm', None) for x in (*a_pair, *b_pair)], [(sds((groups, n_blk * blk, width), F32), 'hbm')],
                  count, cost, body, [pltpu.VMEM((2, blk, width), F32), pltpu.SemaphoreType.DMA((2,))], end)


def dot(spec, a, b):
    return jnp.einsum(spec, a, b, preferred_element_type=F32)


def swap_dp(x):
    return lax.ppermute(x, 'dp', [(0, 1), (1, 0)])


def flat(x):
    return x.reshape(-1, x.shape[-1])


def shards(x):
    return x.reshape(2, 4, PAD, x.shape[-1])


def gather_norm(cid, layer, x, gain, bias):
    def local(b, acc, ins, outs):
        x_ref, g_ref, b_ref = ins
        x_hat, _ = ln_stats(x_ref[b])
        return (x_hat * row(g_ref, layer) + row(b_ref, layer)).astype(BF16)
    return stage_call(cid, False, True, local, None, (x, gain, bias), [])[0]


def residual_norm(cid, layer, part, x, bias, scale, norm_layer, gain, shift, **side):
    def local(b, acc, ins, outs):
        x_ref, b_ref, s_ref, g_ref, h_ref = ins
        total = acc + row(b_ref, layer)
        outs[1][b] = total
        x_new = (x_ref[b].astype(F32) + row(s_ref, layer) * total).astype(BF16)
        outs[0][b] = x_new
        x_hat, _ = ln_stats(x_new)
        return (x_hat * row(g_ref, norm_layer) + row(h_ref, norm_layer)).astype(BF16)
    shp = [sds(x.shape, BF16), sds(x.shape, F32)]
    return stage_call(cid, True, True, local, part, (x, bias, scale, gain, shift), shp, **side)


def residual_last(cid, layer, part, x, bias, scale, grad_y, **side):
    def local(b, acc, ins, outs):
        x_ref, b_ref, s_ref, g_ref = ins
        total = acc + row(b_ref, layer)
        outs[0][b] = (x_ref[b].astype(F32) + row(s_ref, layer) * total).astype(BF16)
        grad = g_ref[b].astype(F32)
        add_rows(outs[1], b, [grad * total, row(s_ref, layer) * grad])
    shp = [sds(x.shape, BF16), sds((2, x.shape[-1]), F32)]
    return stage_call(cid, True, False, local, part, (x, bias, scale, grad_y), shp, **side)


def back_mid(cid, layer, part, x_mid, gain, grad_res, attn_sum, scale, **side):
    def local(b, acc, ins, outs):
        x_ref, g_ref, r_ref, a_ref, s_ref = ins
        grad_in, x_hat = ln_bwd(acc, x_ref[b], row(g_ref, layer))
        grad_mid = r_ref[b].astype(F32) + grad_in
        outs[0][b] = grad_mid
        grad_attn = row(s_ref, layer) * grad_mid
        add_rows(outs[1], b, [acc * x_hat, acc, grad_mid * a_ref[b], grad_attn])
        return grad_attn.astype(BF16)
    shp = [sds(x_mid.shape, F32), sds((4, x_mid.shape[-1]), F32)]
    return stage_call(cid, True, True, local, part, (x_mid, gain, grad_res, attn_sum, scale), shp, **side)


def back_in(cid, layer, part, x_in, gain, grad_mid, mlp_sum, scale, **side):
    more = layer > 0

    def local(b, acc, ins, outs):
        x_ref, g_ref, m_ref = ins[:3]
        grad_in, x_hat = ln_bwd(acc, x_ref[b], row(g_ref, layer))
        grad = (m_ref[b] + grad_in).astype(BF16)
        outs[0][b] = grad
        sums = [acc * x_hat, acc]
        if not more:
            add_rows(outs[1], b, sums)
            return None
        grad = grad.astype(F32)
        grad_mlp = row(ins[4], layer - 1) * grad
        add_rows(outs[1], b, sums + [grad * ins[3][b], grad_mlp])
        return grad_mlp.astype(BF16)
    ins = (x_in, gain, grad_mid) + ((mlp_sum, scale) if more else ())
    shp = [sds(x_in.shape, BF16), sds((4 if more else 2, x_in.shape[-1]), F32)]
    return stage_call(cid, True, more, local, part, ins, shp, **side)


def qkv_of(normed, w, b):
    return (dot('rd,kfd->krf', flat(normed), w) + b[:, None]).astype(BF16)


def mlp_up(normed, w_up, b_up):
    pre = dot('rd,cdf->crf', flat(normed), w_up) + b_up[:, None]
    return pre, (jax.nn.silu(pre[0]) * pre[1]).astype(BF16)


def mlp_bwd(grad_mlp, pre, w_down):
    grad_hidden = dot('rd,fd->rf', flat(grad_mlp), w_down)
    gate_sig = jax.nn.sigmoid(pre[0])
    grad_gate = grad_hidden * pre[1] * gate_sig * (1.0 + pre[0] * (1.0 - gate_sig))
    grad_lin = grad_hidden * pre[0] * gate_sig
    grad_pre = jnp.stack([grad_gate, grad_lin])
    return grad_pre.astype(BF16), jnp.sum(grad_pre, axis=1)


def device_fn(tokens, grad_y, valid_len, norm1_gain, norm1_bias, w_qkv, b_qkv, w_proj, b_proj, layer_scale1,
              norm2_gain, norm2_bias, w_up, b_up, w_down, b_down, layer_scale2):
    pad = ((0, 0), (0, PAD - TOK), (0, 0))
    x0 = jnp.pad(tokens, pad)
    g_y = jnp.pad(grad_y, pad)
    lens = (valid_len, swap_dp(valid_len))
    wq = w_qkv.transpose(0, 1, 3, 4, 2).reshape(2, 3, 256, 1024)
    bq = b_qkv.reshape(2, 3, 256)
    wp = w_proj.reshape(2, 256, 1024)

    n1_0 = gather_norm(0, 0, x0, norm1_gain, norm1_bias)
    qkv_0 = qkv_of(n1_0, wq[0], bq[0])
    o_0 = attn_fwd(qkv_0, lens[0])
    part = dot('rf,fd->rd', o_0, wp[0]).astype(BF16)
    mid_0, asum_0, n2_0, n1_0x, gm_1a = residual_norm(
        1, 0, shards(part), x0, b_proj, layer_scale1, 0, norm2_gain, norm2_bias, swap=[n1_0],
        extra=(1, 0, g_y, layer_scale2))
    pre_0, hid_0 = mlp_up(n2_0, w_up[0], b_up[0])
    part = dot('rf,fd->rd', hid_0, w_down[0]).astype(BF16)
    x1, msum_0, n1_1, n2_0x, gm_1ax, gm_1b, qkv_0x, o_0x = residual_norm(
        2, 0, shards(part), mid_0, b_down, layer_scale2, 1, norm1_gain, norm1_bias, swap=[n2_0, gm_1a],
        extra=(1, 1, g_y, layer_scale2), fills=[fill_attn_fwd(0, n1_0x, wq, bq, lens[1])])
    gm_1 = jnp.concatenate([gm_1a, gm_1b], axis=0)
    qkv_1 = qkv_of(n1_1, wq[1], bq[1])
    o_1 = attn_fwd(qkv_1, lens[0])
    part = dot('rf,fd->rd', o_1, wp[1]).astype(BF16)
    mid_1, asum_1, n2_1, n1_1x, gm_1bx = residual_norm(
        3, 1, shards(part), x1, b_proj, layer_scale1, 1, norm2_gain, norm2_bias, swap=[n1_1, gm_1b])
    gm_1x = jnp.concatenate([gm_1ax, gm_1bx], axis=0)
    pre_1, hid_1 = mlp_up(n2_1, w_up[1], b_up[1])
    part_y = dot('rf,fd->rd', hid_1, w_down[1]).astype(BF16)

    gp_1, gb_1 = mlp_bwd(gm_1, pre_1, w_down[1])
    part = dot('crf,cdf->rd', gp_1, w_up[1]).astype(BF16)
    gmid_1, rows_mid_1, ga_1, n2_1x, qkv_1x, o_1x = back_mid(
        4, 1, shards(part), mid_1, norm2_gain, g_y, asum_1, layer_scale1, swap=[n2_1],
        fills=[fill_attn_fwd(1, n1_1x, wq, bq, lens[1])])
    do_1 = dot('rd,fd->rf', flat(ga_1), wp[1]).astype(BF16)
    gq_1, gbq_1 = attn_bwd(qkv_1, do_1, lens[0])
    part = dot('krf,kfd->rd', gq_1, wq[1]).astype(BF16)
    grad_1, rows_in_1, gm_0, ga_1x, hid_1x, gp_1x, gb_1x = back_in(
        5, 1, shards(part), x1, norm1_gain, gmid_1, msum_0, layer_scale2, swap=[ga_1],
        fills=[fill_mlp(1, n2_1x, [gm_1ax, gm_1bx], w_up, b_up, w_down)])

    gp_0, gb_0 = mlp_bwd(gm_0, pre_0, w_down[0])
    part = dot('crf,cdf->rd', gp_0, w_up[0]).astype(BF16)
    gmid_0, rows_mid_0, ga_0, gm_0x, gq_1x, gbq_1x, g_down = back_mid(
        6, 0, shards(part), mid_0, norm2_gain, grad_1, asum_0, layer_scale1, swap=[gm_0],
        fills=[fill_attn_bwd(1, qkv_1x, ga_1x, wp, lens[1]),
               fill_wgrad((hid_1, hid_1x), (flat(gm_1), flat(gm_1x)), 1, 4, 1.3)])
    do_0 = dot('rd,fd->rf', flat(ga_0), wp[0]).astype(BF16)
    gq_0, gbq_0 = attn_bwd(qkv_0, do_0, lens[0])
    part = dot('krf,kfd->rd', gq_0, wq[0]).astype(BF16)
    grad_0, rows_in_0, ga_0x, hid_0x, gp_0x, gb_0x, g_proj, g_qkv = back_in(
        7, 0, shards(part), x0, norm1_gain, gmid_0, None, None, swap=[ga_0],
        fills=[fill_mlp(0, n2_0x, [gm_0x], w_up, b_up, w_down),
               fill_wgrad((o_1, o_1x), (flat(ga_1), flat(ga_1x)), 1, 1, 1.3),
               fill_wgrad((gq_1, gq_1x), (flat(n1_1), flat(n1_1x)), 3, 1, 1.3)])
    y_out, rows_mlp_1, sums, gq_0x, gbq_0x, g_up = residual_last(
        8, 1, shards(part_y), mid_1, b_down, layer_scale2, g_y,
        fills=[fill_attn_bwd(0, qkv_0x, ga_0x, wp, lens[1]),
               fill_wgrad((flat(n2_1), flat(n2_1x)), (gp_1, gp_1x), 2, 4, 1.3)],
        sums=(rows_in_1[:2], rows_mid_1, rows_in_0, rows_mid_0, rows_in_1[2:]))

    g_down = wgrad((hid_0, hid_0x), (flat(gm_0), flat(gm_0x)), lambda g, i: (0, i), lambda g, i: (0, 0), g_down, 'wg_down')
    g_up = wgrad((flat(n2_0), flat(n2_0x)), (gp_0, gp_0x), lambda g, i: (0, i), lambda g, i: (g, 0, 0), g_up, 'wg_up')
    g_proj = wgrad((o_0, o_0x), (flat(ga_0), flat(ga_0x)), lambda g, i: (0, i), lambda g, i: (0, 0), g_proj, 'wg_proj')
    g_qkv = wgrad((gq_0, gq_0x), (flat(n1_0), flat(n1_0x)), lambda g, i: (g, 0, 0), lambda g, i: (0, 0), g_qkv, 'wg_qkv')
    g_b_up = [gb_0 + gb_0x, gb_1 + gb_1x]
    g_b_qkv = [gbq_0 + gbq_0x.sum(0), gbq_1 + gbq_1x.sum(0)]
    sums = jnp.stack([sums[8:], jnp.concatenate([sums[2:8], sums[:2]], axis=0)])
    n1g, n1b, n2g, n2b, ls1, bp, ls2, bd = (sums[:, k] for k in range(8))
    return (y_out[:, :TOK], grad_0[:, :TOK], n1g, n1b,
            g_qkv.reshape(2, 3, 4, 64, 1024).transpose(0, 1, 4, 2, 3), jnp.stack(g_b_qkv).reshape(2, 3, 4, 64),
            g_proj.reshape(2, 4, 64, 1024), bp, ls1, n2g, n2b, g_up, jnp.stack(g_b_up),
            g_down.reshape(2, 1024, 1024), bd, ls2)


def solution(mesh):
    rep = P()
    act = P('dp', 'tp', None)
    param_specs = (rep, rep, P(None, None, None, 'tp', None), P(None, None, 'tp', None), P(None, 'tp', None, None), rep,
                   rep, rep, rep, P(None, None, None, 'tp'), P(None, None, 'tp'), P(None, 'tp', None), rep, rep)
    return jax.shard_map(device_fn, mesh=mesh, in_specs=(act, act, P('dp')) + param_specs,
                         out_specs=(act, act) + param_specs, check_vma=False)
```

```python
import jax
import jax.numpy as jnp
from jax import lax
from jax.experimental import pallas as pl
from jax.experimental.pallas import tpu as pltpu
from jax.sharding import PartitionSpec as P

NORM_EPS = 1e-6
NEG_BIG = -1e9
F32 = jnp.float32
BF16 = jnp.bfloat16
TOK = 66
PAD = 72
N_TP = 4
N_SEQ = 2
SEQ = N_TP * PAD
ROWS = N_SEQ * SEQ
MESH_ID = pl.DeviceIdType.MESH
VMEM_SPEC = pl.BlockSpec(memory_space=pltpu.VMEM)
HBM_SPEC = pl.BlockSpec(memory_space=pltpu.HBM)


def sds(shape, dtype):
    return jax.ShapeDtypeStruct(shape, dtype)


def mm(a, b, dims=((1,), (0,))):
    return lax.dot_general(a, b, (dims, ((), ())), preferred_element_type=F32)


NT = ((1,), (1,))
TN = ((0,), (0,))


def load(arr, index=None):
    return arr, True, index


def held(arr):
    return arr, False, None


def first(x):
    return x[:1, :1]


class Work:
    def __init__(self, ins, outs, count, body, cost=1.0, fin=None):
        self.ins, self.outs, self.count, self.body, self.cost, self.fin = ins, outs, count, body, cost, fin


def stage_call(cid, local_fn, ins, out_shapes, ag=True, part=None, pro=None, swap=(), extra=None, trade=(), fills=(),
               sums=None, budget=(4.5, 2.0, 2.5, 3.0)):
    width = ins[0].shape[-1]
    rs = part is not None or pro is not None
    args, in_specs, place = [], [], {}

    def add(arr, spec=VMEM_SPEC):
        key = (id(arr), spec is HBM_SPEC)
        if key not in place:
            place[key] = len(args)
            args.append(arr)
            in_specs.append(spec)
        return place[key]

    outs, out_specs = [], []

    def add_out(shape, spec=VMEM_SPEC):
        outs.append(shape)
        out_specs.append(spec)
        return len(outs) - 1

    scratch = []

    def add_scratch(item):
        scratch.append(item)
        return len(scratch) - 1

    i_part = add(part) if part is not None else None
    i_ins = [add(a) for a in ins]
    i_swap = [add(a) for a in swap]
    i_trade = [add(a) for a in trade]
    i_extra = [add(a) for a in extra[2:]] if extra else []
    i_sums = [add(a) for a in sums] if sums is not None else []
    o_local = [add_out(s) for s in out_shapes]
    full_shape = sds((N_SEQ, N_TP, PAD, width), BF16)
    o_full = add_out(full_shape) if ag else None
    o_swap = [add_out(sds(a.shape, BF16)) for a in swap]
    o_trade = [add_out(sds(a.shape, a.dtype)) for a in trade]
    o_extra = add_out(sds((1, N_TP, PAD, width), BF16)) if extra else None
    o_sums = add_out(sds((16, width), F32)) if sums is not None else None
    works = ([pro] if pro else []) + list(fills)
    w_ins, w_outs = [], []
    n_load = 0
    for work in works:
        got = []
        for arr, copied, index in work.ins:
            if copied:
                k = add_scratch(pltpu.VMEM(arr.shape if index is None else arr.shape[1:], arr.dtype))
                got.append((add(arr, HBM_SPEC), index, k, n_load))
                n_load += 1
            else:
                got.append((add(arr), None, None, None))
        w_ins.append(got)
        w_outs.append([add_out(s) for s in work.outs])
    shard = pltpu.VMEM((N_SEQ, PAD, width), BF16)
    if rs:
        s_bufs = [add_scratch(shard) for _ in range(4)]
        s_part = add_scratch(pltpu.VMEM(full_shape.shape, BF16)) if pro else None
    k_swap = 6 * N_SEQ
    k_extra = k_swap + 4 * len(swap)
    k_sum = k_extra + 3
    k_trade = k_sum + 3
    n_sem = k_trade + len(trade)
    s_send, s_recv = [add_scratch(pltpu.SemaphoreType.DMA((n_sem,))) for _ in range(2)]
    s_load = add_scratch(pltpu.SemaphoreType.DMA((max(n_load, 1),)))
    if sums is not None:
        s_sum = [add_scratch(pltpu.VMEM((3, 16, width), F32)) for _ in range(2)]
    n_in, n_out = len(args), len(outs)

    def kernel(*refs):
        r_in, r_out, r_s = refs[:n_in], refs[n_in:n_in + n_out], refs[n_in + n_out:]
        in_refs = [r_in[k] for k in i_ins]
        out_refs = [r_out[k] for k in o_local]
        full = r_out[o_full] if ag else None
        ssem, rsem, lsem = r_s[s_send], r_s[s_recv], r_s[s_load]
        loads, use_in, use_out = [], [], []
        for got, places in zip(w_ins, w_outs):
            cps, use = [], []
            for k_in, index, k_buf, k_sem in got:
                if k_buf is None:
                    use.append(r_in[k_in])
                    continue
                src = r_in[k_in] if index is None else r_in[k_in].at[index]
                cps.append(pltpu.make_async_copy(src, r_s[k_buf], lsem.at[k_sem]))
                cps[-1].start()
                use.append(r_s[k_buf])
            loads.append(cps)
            use_in.append(use)
            use_out.append([r_out[k] for k in places])
        dp = lax.axis_index('dp')
        t = lax.axis_index('tp')
        core = lax.rem(t, 2)
        mate = t + 1 - 2 * core
        peer = lax.rem(t + 2, N_TP)
        far = lax.rem(mate + 2, N_TP)
        here, there = dp, 1 - dp

        def remote(src, dst, k, dev, line=None):
            return pltpu.make_async_remote_copy(src_ref=src, dst_ref=dst, send_sem=ssem.at[k], recv_sem=rsem.at[k],
                                                device_id=(here if line is None else line, dev), device_id_type=MESH_ID)

        barrier = pltpu.get_barrier_semaphore()
        peers = [(here, mate), (here, peer)]
        if swap or trade or sums is not None:
            peers.append((there, t))
        for dev in peers:
            pl.semaphore_signal(barrier, inc=1, device_id=dev, device_id_type=MESH_ID)
        pl.semaphore_wait(barrier, len(peers))

        first = 1 if pro else 0
        done = [0] * len(works)

        def run(time):
            for f in range(first, len(works)):
                work = works[f]
                left = work.count - done[f]
                n = left if time is None else min(left, int(time / work.cost + 0.5))
                if n <= 0:
                    continue
                if done[f] == 0:
                    for cp in loads[f]:
                        cp.wait()
                lo = done[f]
                done[f] = hi = lo + n
                if n == 1:
                    work.body(lo, use_in[f], use_out[f])
                else:
                    @pl.loop(lo, hi)
                    def _(i, work=work, f=f):
                        work.body(i, use_in[f], use_out[f])
                if time is not None:
                    time -= n * work.cost

        started, landed = [], []
        for k, (a, b) in enumerate(zip(i_trade, o_trade)):
            cp = remote(r_in[a], r_out[b], k_trade + k, t, there)
            cp.start()
            started.append(cp)
            landed.append(cp)
        if extra:
            ex = r_out[o_extra]
            ex[0, t] = (row(r_in[i_extra[1]], extra[0]) * r_in[i_extra[0]][extra[1]].astype(F32)).astype(BF16)
            x_peer = remote(ex.at[0, t], ex.at[0, t], k_extra, peer)
            x_mate = remote(ex.at[0, t], ex.at[0, t], k_extra + 1, mate)
            x_peer.start()
            x_mate.start()
            started += [x_peer, x_mate]
            landed.append(x_mate)
        s_y = []
        for k in range(len(swap)):
            src, dst = r_in[i_swap[k]], r_out[o_swap[k]]
            for j in range(2):
                s_y.append(remote(src.at[:, core + 2 * j], dst.at[:, core + 2 * j], k_swap + 4 * k + j, t, there))
                s_y[-1].start()
        started += s_y
        if rs:
            far_buf, mate_buf, peer_buf, send_buf = [r_s[k] for k in s_bufs]
            part_ref = r_s[s_part] if pro else r_in[i_part]
            c_far = [remote(part_ref.at[b, far], far_buf.at[b], b, mate) for b in range(N_SEQ)]
            c_mate = [remote(part_ref.at[b, mate], mate_buf.at[b], N_SEQ + b, mate) for b in range(N_SEQ)]
            c_peer = [remote(send_buf.at[b], peer_buf.at[b], 2 * N_SEQ + b, peer) for b in range(N_SEQ)]

            def to_mate(b):
                c_far[b].start()
                c_mate[b].start()

            def to_peer(b):
                c_far[b].wait_recv()
                send_buf[b] = (part_ref[b, peer].astype(F32) + far_buf[b].astype(F32)).astype(BF16)
                c_peer[b].start()

            def produce(b):
                @pl.loop(0, pro.count)
                def _(u):
                    pro.body(b, u, use_in[0], use_out[0])

            def finish(b):
                val = pro.fin(b, use_in[0], use_out[0]).astype(BF16)
                for k in range(N_TP):
                    part_ref[b, k] = val[k * PAD:(k + 1) * PAD]

            if pro:
                for cp in loads[0]:
                    cp.wait()
                produce(0)
                finish(0)
                to_mate(0)
                produce(1)
                to_peer(0)
                finish(1)
                to_mate(1)
                run(1.0)
                to_peer(1)
                run(budget[0] - 3.0)
            else:
                for b in range(N_SEQ):
                    to_mate(b)
                for b in range(N_SEQ):
                    to_peer(b)
                run(budget[0])
            started += c_far + c_mate + c_peer
        g_peer, g_mate, g_fwd = [], [], []
        for b in range(N_SEQ):
            acc = None
            if rs:
                if b:
                    run(budget[1])
                c_mate[b].wait_recv()
                acc = part_ref[b, t].astype(F32) + mate_buf[b].astype(F32)
                c_peer[b].wait_recv()
                acc = acc + peer_buf[b].astype(F32)
            val = local_fn(b, acc, in_refs, out_refs)
            if ag:
                full[b, t] = val
                g_peer.append(remote(full.at[b, t], full.at[b, t], 3 * N_SEQ + b, peer))
                g_mate.append(remote(full.at[b, t], full.at[b, t], 4 * N_SEQ + b, mate))
                g_peer[b].start()
                g_mate[b].start()
        if sums is not None:
            sum_src, sum_dst = [r_s[k] for k in s_sum]
            sum_src[0, 0:2, :] = out_refs[-1][...]
            at = 2
            for k in i_sums:
                n_rows = args[k].shape[0]
                sum_src[0, at:at + n_rows, :] = r_in[k][...]
                at += n_rows
            for k, (line, dev) in enumerate([(here, mate), (here, peer), (there, t)]):
                cp = remote(sum_src.at[k], sum_dst.at[k], k_sum + k, dev, line)
                cp.start()
                if k:
                    run(budget[2])
                cp.wait_recv()
                started.append(cp)
                total = sum_src[k] + sum_dst[k]
                if k < 2:
                    sum_src[k + 1] = total
                else:
                    r_out[o_sums][...] = total
        if extra:
            x_peer.wait_recv()
            x_fwd = remote(ex.at[0, peer], ex.at[0, peer], k_extra + 2, mate)
            x_fwd.start()
            started.append(x_fwd)
            landed.append(x_fwd)
        if ag:
            for b in range(N_SEQ):
                run(budget[2 + b])
                g_peer[b].wait_recv()
                g_fwd.append(remote(full.at[b, peer], full.at[b, peer], 5 * N_SEQ + b, mate))
                g_fwd[b].start()
            started += g_peer + g_mate + g_fwd
            landed += g_mate + g_fwd
        for k in range(len(swap)):
            dst = r_out[o_swap[k]]
            for j in range(2):
                s_y[2 * k + j].wait_recv()
                cp = remote(dst.at[:, core + 2 * j], dst.at[:, core + 2 * j], k_swap + 4 * k + 2 + j, mate)
                cp.start()
                started.append(cp)
                landed.append(cp)
        run(None)
        for cp in landed:
            cp.wait_recv()
        for cp in started:
            cp.wait_send()

    return pl.pallas_call(
        kernel,
        out_shape=outs,
        in_specs=in_specs,
        out_specs=out_specs,
        scratch_shapes=scratch,
        compiler_params=pltpu.CompilerParams(collective_id=cid, has_side_effects=True, vmem_limit_bytes=48 * 2 ** 20),
        cost_estimate=pl.CostEstimate(flops=40_000_000, bytes_accessed=4_000_000, transcendentals=0),
        name=f'stage{cid}',
    )(*args)


def row(ref, layer):
    return ref[layer:layer + 1, :]


def ln_stats(x):
    x_f32 = x.astype(F32)
    centered = x_f32 - jnp.mean(x_f32, axis=-1, keepdims=True)
    inv_std = lax.rsqrt(jnp.mean(centered * centered, axis=-1, keepdims=True) + NORM_EPS)
    return centered * inv_std, inv_std


def ln_bwd(grad_out, x, gain):
    x_hat, inv_std = ln_stats(x)
    grad_hat = grad_out * gain
    mean_one = jnp.mean(grad_hat, axis=-1, keepdims=True)
    mean_two = jnp.mean(grad_hat * x_hat, axis=-1, keepdims=True)
    return inv_std * (grad_hat - mean_one - x_hat * mean_two), x_hat


def add_rows(rows_ref, b, rows):
    for k, val in enumerate(rows):
        s = jnp.sum(val, axis=0, keepdims=True)
        rows_ref[k:k + 1, :] = s if b == 0 else rows_ref[k:k + 1, :] + s


def key_valid(seq_len):
    col = lax.broadcasted_iota(jnp.int32, (SEQ, SEQ), 1)
    shard = jnp.zeros_like(col)
    for k in range(1, N_TP):
        shard = shard + (col >= k * PAD).astype(jnp.int32)
    return jnp.logical_and(col - PAD * shard < TOK, col - (PAD - TOK) * shard < seq_len)


def head_probs(q_half, k_pair, valid):
    scores = mm(q_half, k_pair, NT) * 0.125
    scores = jnp.where(valid, scores, NEG_BIG)
    e = jnp.exp(scores - jnp.max(scores, axis=-1, keepdims=True))
    return e / jnp.sum(e, axis=-1, keepdims=True)


def seq_rows(b):
    return pl.ds(b * SEQ if isinstance(b, int) else pl.multiple_of(b * SEQ, SEQ), SEQ)


def pair_cols(pair):
    return pl.ds(pl.multiple_of(pair * 128, 128), 128)


def by_seq(x):
    return x.reshape(-1, SEQ, x.shape[-1])


def flat(x):
    return x.reshape(-1, x.shape[-1])


def attn_fwd_unit(b, pair, x, w_ref, bias, seq_len, qkv_ref, o_ref):
    rows, cols = seq_rows(b), pair_cols(pair)
    pieces = []
    for c in range(3):
        val = (mm(x, w_ref[c, cols, :], NT) + bias[c:c + 1, cols]).astype(BF16)
        qkv_ref[c, rows, cols] = val
        pieces.append(val)
    q, k, v = pieces
    valid = key_valid(seq_len)
    half = lax.broadcasted_iota(jnp.int32, (SEQ, 128), 1) // 64
    res = []
    for h in range(2):
        probs = head_probs(jnp.where(half == h, q, jnp.zeros_like(q)), k, valid)
        res.append(mm(probs.astype(BF16), v))
    o_ref[rows, cols] = jnp.where(half == 0, res[0], res[1]).astype(BF16)


def attn_bwd_unit(b, pair, g, qkv_ref, w_ref, seq_len, dqkv_ref, db_ref):
    rows, cols = seq_rows(b), pair_cols(pair)
    do = mm(g, w_ref[cols, :], NT).astype(BF16)
    q, k, v = (qkv_ref[c, rows, cols] for c in range(3))
    valid = key_valid(seq_len)
    half = lax.broadcasted_iota(jnp.int32, (SEQ, 128), 1) // 64
    dq, dk, dv = [], [], []
    for h in range(2):
        probs = head_probs(jnp.where(half == h, q, jnp.zeros_like(q)), k, valid)
        grad_p = mm(jnp.where(half == h, do, jnp.zeros_like(do)), v, NT)
        grad_s = (probs * (grad_p - jnp.sum(grad_p * probs, axis=-1, keepdims=True)) * 0.125).astype(BF16)
        dv.append(mm(probs.astype(BF16), do, TN))
        dq.append(mm(grad_s, k))
        dk.append(mm(grad_s, q, TN))
    for c, pieces in enumerate((dq, dk, dv)):
        val = jnp.where(half == 0, pieces[0], pieces[1])
        dqkv_ref[c, rows, cols] = val.astype(BF16)
        db_ref[b, c:c + 1, cols] = jnp.sum(val, axis=0, keepdims=True)


def mlp_up_unit(x, u_ref, bias, cols):
    gate = mm(x, u_ref[0, :, cols]) + bias[0:1, cols]
    lin = mm(x, u_ref[1, :, cols]) + bias[1:2, cols]
    return gate, lin


def mlp_bwd_unit(b, u, x, g, u_ref, bias, d_ref, hid_ref, gp_ref, gb_ref):
    rows, cols = seq_rows(b), pl.ds(pl.multiple_of(u * 256, 256), 256)
    gate, lin = mlp_up_unit(x, u_ref, bias, cols)
    grad_hid = mm(g, d_ref[cols, :], NT)
    sig = jax.nn.sigmoid(gate)
    if hid_ref is not None:
        hid_ref[rows, cols] = (gate * sig * lin).astype(BF16)
    grad_gate = grad_hid * lin * sig * (1.0 + gate * (1.0 - sig))
    grad_lin = grad_hid * gate * sig
    for c, val in enumerate((grad_gate, grad_lin)):
        gp_ref[c, rows, cols] = val.astype(BF16)
        gb_ref[b, c:c + 1, cols] = jnp.sum(val, axis=0, keepdims=True)


QKV = sds((3, ROWS, 256), BF16)
HEADS = sds((ROWS, 256), BF16)
HIDDEN = sds((ROWS, 1024), BF16)
GRAD_PRE = sds((2, ROWS, 1024), BF16)
GRAD_BQ = sds((N_SEQ, 3, 256), F32)
GRAD_BU = sds((N_SEQ, 2, 1024), F32)


def fill_attn_fwd(layer, normed, wq, bq, lens):
    def body(i, ins, outs):
        n_ref, w_ref, b_ref, vl_ref = ins
        b = i // 2
        attn_fwd_unit(b, i % 2, n_ref[b], w_ref, b_ref.at[layer], first(vl_ref[b]), *outs)
    return Work([load(by_seq(normed)), load(wq, layer), held(bq), held(lens)],
                [QKV, HEADS], 4, body, 1.7)


def fill_attn_bwd(layer, qkv, grad, wp, lens):
    def body(i, ins, outs):
        qkv_ref, g_ref, w_ref, vl_ref = ins
        b = i // 2
        attn_bwd_unit(b, i % 2, g_ref[b], qkv_ref, w_ref, first(vl_ref[b]), *outs)
    return Work([load(qkv), load(by_seq(grad)), load(wp, layer), held(lens)],
                [QKV, GRAD_BQ], 4, body, 2.0)


def fill_mlp(layer, normed, grad, w_up, b_up, w_down):
    def body(i, ins, outs):
        n_ref, g_ref, u_ref, b_ref, d_ref = ins
        for b in range(N_SEQ):
            mlp_bwd_unit(b, i, n_ref[b], g_ref[b], u_ref, b_ref.at[layer], d_ref, *outs)
    return Work([load(by_seq(normed)), load(by_seq(grad)), load(w_up, layer), held(b_up),
                 load(w_down, layer)], [HIDDEN, GRAD_PRE, GRAD_BU], 4, body, 1.8)


def pro_attn_fwd(layer, normed, wq, bq, wp, lens):
    def body(b, u, ins, outs):
        n_ref, w_ref, b_ref, _, vl_ref = ins
        attn_fwd_unit(b, u, n_ref[b], w_ref, b_ref.at[layer], first(vl_ref[b]), *outs)

    def fin(b, ins, outs):
        return mm(outs[1][seq_rows(b), :], ins[3][...])
    return Work([held(by_seq(normed)), load(wq, layer), held(bq), load(wp, layer),
                 held(lens)], [QKV, HEADS], 2, body, fin=fin)


def pro_mlp_fwd(layer, normed, w_up, b_up, w_down):
    def body(b, u, ins, outs):
        n_ref, u_ref, b_ref, _ = ins
        cols = pl.ds(pl.multiple_of(u * 256, 256), 256)
        gate, lin = mlp_up_unit(n_ref[b], u_ref, b_ref.at[layer], cols)
        outs[0][seq_rows(b), cols] = (jax.nn.silu(gate) * lin).astype(BF16)

    def fin(b, ins, outs):
        return mm(outs[0][seq_rows(b), :], ins[3][...])
    return Work([held(by_seq(normed)), load(w_up, layer), held(b_up), load(w_down, layer)],
                [HIDDEN], 4, body, fin=fin)


def pro_mlp_bwd(layer, normed, grads, w_up, b_up, w_down, forward):
    grads = [by_seq(g) for g in grads]

    def body(b, u, ins, outs):
        n_ref, u_ref, b_ref, d_ref = ins[:4]
        seqs = [ref.at[k] for ref in ins[4:] for k in range(ref.shape[0])]
        mlp_bwd_unit(b, u, n_ref[b], seqs[b][...], u_ref, b_ref.at[layer], d_ref, outs[2] if forward else None, *outs[:2])

    def fin(b, ins, outs):
        rows = seq_rows(b)
        if forward:
            outs[3][rows, :] = mm(outs[2][rows, :], ins[3][...]).astype(BF16)
        return (mm(outs[0][0, rows, :], ins[1][0], NT) + mm(outs[0][1, rows, :], ins[1][1], NT))
    return Work([held(by_seq(normed)), load(w_up, layer), held(b_up), load(w_down, layer)]
                + [held(g) for g in grads],
                [GRAD_PRE, GRAD_BU] + ([HIDDEN, sds((ROWS, 1024), BF16)] if forward else []), 4, body, fin=fin)


def pro_attn_bwd(layer, qkv, grad, wp, wq, lens):
    def body(b, u, ins, outs):
        qkv_ref, g_ref, w_ref, _, vl_ref = ins
        attn_bwd_unit(b, u, g_ref[b], qkv_ref, w_ref, first(vl_ref[b]), *outs)

    def fin(b, ins, outs):
        rows = seq_rows(b)
        return sum(mm(outs[0][c, rows, :], ins[3][c]) for c in range(3))
    return Work([load(qkv), held(by_seq(grad)), load(wp, layer), load(wq, layer),
                 held(lens)], [QKV, GRAD_BQ], 2, body, fin=fin)


def gather_norm(cid, layer, x, gain, bias, **side):
    def local(b, acc, ins, outs):
        x_ref, g_ref, b_ref = ins
        x_hat, _ = ln_stats(x_ref[b])
        return (x_hat * row(g_ref, layer) + row(b_ref, layer)).astype(BF16)
    return stage_call(cid, local, (x, gain, bias), [], **side)


def residual_norm(cid, layer, x, bias, scale, norm_layer, gain, shift, **side):
    def local(b, acc, ins, outs):
        x_ref, b_ref, s_ref, g_ref, h_ref = ins
        total = acc + row(b_ref, layer)
        outs[1][b] = total
        x_new = (x_ref[b].astype(F32) + row(s_ref, layer) * total).astype(BF16)
        outs[0][b] = x_new
        x_hat, _ = ln_stats(x_new)
        return (x_hat * row(g_ref, norm_layer) + row(h_ref, norm_layer)).astype(BF16)
    return stage_call(cid, local, (x, bias, scale, gain, shift), [sds(x.shape, BF16), sds(x.shape, F32)], **side)


def residual_last(cid, layer, x, bias, scale, grad_y, **side):
    def local(b, acc, ins, outs):
        x_ref, b_ref, s_ref, g_ref = ins
        total = acc + row(b_ref, layer)
        outs[0][b] = (x_ref[b].astype(F32) + row(s_ref, layer) * total).astype(BF16)
        grad = g_ref[b].astype(F32)
        add_rows(outs[1], b, [grad * total, row(s_ref, layer) * grad])
    return stage_call(cid, local, (x, bias, scale, grad_y), [sds(x.shape, BF16), sds((2, x.shape[-1]), F32)], ag=False, **side)


def back_mid(cid, layer, x_mid, gain, grad_res, attn_sum, scale, **side):
    def local(b, acc, ins, outs):
        x_ref, g_ref, r_ref, a_ref, s_ref = ins
        grad_in, x_hat = ln_bwd(acc, x_ref[b], row(g_ref, layer))
        grad_mid = r_ref[b].astype(F32) + grad_in
        outs[0][b] = grad_mid
        grad_attn = row(s_ref, layer) * grad_mid
        add_rows(outs[1], b, [acc * x_hat, acc, grad_mid * a_ref[b], grad_attn])
        return grad_attn.astype(BF16)
    return stage_call(cid, local, (x_mid, gain, grad_res, attn_sum, scale),
                      [sds(x_mid.shape, F32), sds((4, x_mid.shape[-1]), F32)], **side)


def back_in(cid, layer, x_in, gain, grad_mid, mlp_sum, scale, **side):
    more = layer > 0

    def local(b, acc, ins, outs):
        x_ref, g_ref, m_ref = ins[:3]
        grad_in, x_hat = ln_bwd(acc, x_ref[b], row(g_ref, layer))
        grad = (m_ref[b] + grad_in).astype(BF16)
        outs[0][b] = grad
        if not more:
            add_rows(outs[1], b, [acc * x_hat, acc])
            return None
        grad = grad.astype(F32)
        grad_mlp = row(ins[4], layer - 1) * grad
        add_rows(outs[1], b, [acc * x_hat, acc])
        add_rows(outs[2], b, [grad * ins[3][b], grad_mlp])
        return grad_mlp.astype(BF16)
    shapes = [sds(x_in.shape, BF16)] + [sds((2, x_in.shape[-1]), F32)] * (2 if more else 1)
    return stage_call(cid, local, (x_in, gain, grad_mid) + ((mlp_sum, scale) if more else ()), shapes, ag=more, **side)


def grads_call(jobs, biases_up, biases_qkv, sums):
    args, specs = [], []
    for job in jobs:
        for arr in job[2:]:
            args.append(arr)
            specs.append(HBM_SPEC)
    n_op = len(args)
    small = [x for pair in biases_up + biases_qkv for x in pair] + [sums]
    args += small
    specs += [VMEM_SPEC] * len(small)
    width = sums.shape[-1]
    shapes = [(groups, total, width) for groups, total in ((2, 1024), (1, 1024), (3, 256), (1, 256))]
    shapes += [x[0].shape[1:] for x in (biases_up[0], biases_qkv[0])] + [(width,)] * 8
    outs = [sds((2, *shape), F32) for shape in shapes]
    stage_rows = 512

    def kernel(*refs):
        ops, smalls = refs[:n_op], refs[n_op:n_op + len(small)]
        out = refs[n_op + len(small):n_op + len(small) + len(outs)]
        bufs = refs[n_op + len(small) + len(outs):][:n_op]
        stage, lsem, osem = refs[-3:]
        loads = [pltpu.make_async_copy(ops[k], bufs[k], lsem.at[k]) for k in range(n_op)]
        for cp in loads:
            cp.start()
        for l in range(2):
            for k, pairs in enumerate((smalls[:4], smalls[4:])):
                out[4 + k][l] = jnp.sum(pairs[2 * l][...] + pairs[2 * l + 1][...], axis=0)
        rows = smalls[-1]
        for k in range(8):
            for l, at in enumerate((8 + k, 2 + k if k < 6 else k - 6)):
                out[6 + k][l:l + 1, :] = rows[at:at + 1, :]
        pending = [None] * 2
        step = 0
        for j, (slot, layer, *_) in enumerate(jobs):
            a_pair, b_pair = bufs[4 * j:4 * j + 2], bufs[4 * j + 2:4 * j + 4]
            for cp in loads[4 * j:4 * j + 4]:
                cp.wait()
            groups, total = outs[slot].shape[1:3]
            blk = min(stage_rows, total)
            for g in range(groups):
                for i in range(total // blk):
                    cols = slice(i * blk, (i + 1) * blk)
                    acc = None
                    for a_ref, b_ref in zip(a_pair, b_pair):
                        a = a_ref[g, :, cols] if len(a_ref.shape) == 3 else a_ref[:, cols]
                        b = b_ref[g] if len(b_ref.shape) == 3 else b_ref[...]
                        term = mm(a, b, TN)
                        acc = term if acc is None else acc + term
                    s = step % 2
                    if pending[s] is not None:
                        pending[s].wait()
                    stage[s, :blk] = acc
                    pending[s] = pltpu.make_async_copy(stage.at[s, pl.ds(0, blk)], out[slot].at[layer, g, pl.ds(i * blk, blk)],
                                                       osem.at[s])
                    pending[s].start()
                    step += 1
        for cp in pending:
            cp.wait()

    return pl.pallas_call(
        kernel,
        out_shape=outs,
        in_specs=specs,
        out_specs=[HBM_SPEC] * 4 + [VMEM_SPEC] * 10,
        scratch_shapes=[pltpu.VMEM(a.shape, a.dtype) for a in args[:n_op]]
        + [pltpu.VMEM((2, stage_rows, width), F32), pltpu.SemaphoreType.DMA((n_op,)), pltpu.SemaphoreType.DMA((2,))],
        compiler_params=pltpu.CompilerParams(vmem_limit_bytes=60 * 2 ** 20),
        cost_estimate=pl.CostEstimate(flops=40_000_000_000, bytes_accessed=80_000_000, transcendentals=0),
        name='grads')(*args)


def device_fn(tokens, grad_y, valid_len, norm1_gain, norm1_bias, w_qkv, b_qkv, w_proj, b_proj, layer_scale1,
              norm2_gain, norm2_bias, w_up, b_up, w_down, b_down, layer_scale2):
    pad = ((0, 0), (0, PAD - TOK), (0, 0))
    x0 = jnp.pad(tokens, pad)
    g_y = jnp.pad(grad_y, pad)
    lens = jnp.broadcast_to(valid_len[:, None, None], (N_SEQ, 8, 128))
    wq = w_qkv.transpose(0, 1, 3, 4, 2).reshape(2, 3, 256, 1024)
    bq = b_qkv.reshape(2, 3, 256)
    wp = w_proj.reshape(2, 256, 1024)

    n1_0, lens_x = gather_norm(0, 0, x0, norm1_gain, norm1_bias, trade=[lens])
    mid_0, asum_0, n2_0, n1_0x, gm_1a, qkv_0, o_0 = residual_norm(
        1, 0, x0, b_proj, layer_scale1, 0, norm2_gain, norm2_bias, pro=pro_attn_fwd(0, n1_0, wq, bq, wp, lens),
        swap=[n1_0], extra=(1, 0, g_y, layer_scale2))
    x1, msum_0, n1_1, n2_0x, gm_1ax, gm_1b, hid_0, qkv_0x, o_0x = residual_norm(
        2, 0, mid_0, b_down, layer_scale2, 1, norm1_gain, norm1_bias, pro=pro_mlp_fwd(0, n2_0, w_up, b_up, w_down),
        swap=[n2_0, gm_1a], extra=(1, 1, g_y, layer_scale2), fills=[fill_attn_fwd(0, n1_0x, wq, bq, lens_x)])
    mid_1, asum_1, n2_1, n1_1x, gm_1bx, qkv_1, o_1 = residual_norm(
        3, 1, x1, b_proj, layer_scale1, 1, norm2_gain, norm2_bias, pro=pro_attn_fwd(1, n1_1, wq, bq, wp, lens),
        swap=[n1_1, gm_1b])

    gmid_1, rows_mid_1, ga_1, n2_1x, gp_1, gb_1, hid_1, part_y, qkv_1x, o_1x = back_mid(
        4, 1, mid_1, norm2_gain, g_y, asum_1, layer_scale1,
        pro=pro_mlp_bwd(1, n2_1, [gm_1a, gm_1b], w_up, b_up, w_down, True),
        swap=[n2_1], fills=[fill_attn_fwd(1, n1_1x, wq, bq, lens_x)])
    gm_1 = jnp.concatenate([gm_1a, gm_1b], axis=0)
    gm_1x = jnp.concatenate([gm_1ax, gm_1bx], axis=0)
    grad_1, rows_in_1, rows_mlp_0, gm_0, ga_1x, gq_1, gbq_1, hid_1x, gp_1x, gb_1x = back_in(
        5, 1, x1, norm1_gain, gmid_1, msum_0, layer_scale2, pro=pro_attn_bwd(1, qkv_1, ga_1, wp, wq, lens), swap=[ga_1],
        fills=[fill_mlp(1, n2_1x, gm_1x, w_up, b_up, w_down)])

    gmid_0, rows_mid_0, ga_0, gm_0x, gp_0, gb_0, gq_1x, gbq_1x = back_mid(
        6, 0, mid_0, norm2_gain, grad_1, asum_0, layer_scale1,
        pro=pro_mlp_bwd(0, n2_0, [gm_0], w_up, b_up, w_down, False),
        swap=[gm_0], fills=[fill_attn_bwd(1, qkv_1x, ga_1x, wp, lens_x)])
    grad_0, rows_in_0, ga_0x, gq_0, gbq_0, hid_0x, gp_0x, gb_0x = back_in(
        7, 0, x0, norm1_gain, gmid_0, None, None, pro=pro_attn_bwd(0, qkv_0, ga_0, wp, wq, lens), swap=[ga_0],
        fills=[fill_mlp(0, n2_0x, gm_0x, w_up, b_up, w_down)])
    y_out, _, sums, gq_0x, gbq_0x = residual_last(
        8, 1, mid_1, b_down, layer_scale2, g_y, part=part_y.reshape(N_SEQ, N_TP, PAD, -1),
        fills=[fill_attn_bwd(0, qkv_0x, ga_0x, wp, lens_x)],
        sums=(rows_in_1, rows_mid_1, rows_in_0, rows_mid_0, rows_mlp_0))

    operands = (
        (n2_1, n2_1x, gp_1, gp_1x, hid_1, hid_1x, gm_1, gm_1x, gq_1, gq_1x, n1_1, n1_1x, o_1, o_1x, ga_1, ga_1x),
        (n2_0, n2_0x, gp_0, gp_0x, hid_0, hid_0x, gm_0, gm_0x, gq_0, gq_0x, n1_0, n1_0x, o_0, o_0x, ga_0, ga_0x))
    jobs = []
    for k, arrs in enumerate(operands):
        arrs = [a if a.shape[-2] == ROWS else flat(a) for a in arrs]
        jobs += [(slot, 1 - k, *arrs[4 * slot:4 * slot + 4]) for slot in range(4)]
    g_up, g_down, g_qkv, g_proj, g_b_up, g_b_qkv, n1g, n1b, n2g, n2b, ls1, bp, ls2, bd = grads_call(
        jobs, [(gb_0, gb_0x), (gb_1, gb_1x)], [(gbq_0, gbq_0x), (gbq_1, gbq_1x)], sums)
    return (y_out[:, :TOK], grad_0[:, :TOK], n1g, n1b,
            g_qkv.reshape(2, 3, 4, 64, 1024).transpose(0, 1, 4, 2, 3), g_b_qkv.reshape(2, 3, 4, 64),
            g_proj.reshape(2, 4, 64, 1024), bp, ls1, n2g, n2b, g_up, g_b_up,
            g_down.reshape(2, 1024, 1024), bd, ls2)


def solution(mesh):
    rep = P()
    act = P('dp', 'tp', None)
    param_specs = (rep, rep, P(None, None, None, 'tp', None), P(None, None, 'tp', None), P(None, 'tp', None, None), rep,
                   rep, rep, rep, P(None, None, None, 'tp'), P(None, None, 'tp'), P(None, 'tp', None), rep, rep)
    return jax.shard_map(device_fn, mesh=mesh, in_specs=(act, act, P('dp')) + param_specs,
                         out_specs=(act, act) + param_specs, check_vma=False)
```

```python
import jax
import jax.numpy as jnp
from jax import lax
from jax.experimental import pallas as pl
from jax.experimental.pallas import tpu as pltpu
from jax.sharding import PartitionSpec as P

NORM_EPS = 1e-6
NEG_BIG = -1e9
F32 = jnp.float32
BF16 = jnp.bfloat16
TOK = 66
PAD = 72
N_TP = 4
N_SEQ = 2
SEQ = N_TP * PAD
ROWS = N_SEQ * SEQ
MESH_ID = pl.DeviceIdType.MESH
VMEM_SPEC = pl.BlockSpec(memory_space=pltpu.VMEM)
HBM_SPEC = pl.BlockSpec(memory_space=pltpu.HBM)


def sds(shape, dtype):
    return jax.ShapeDtypeStruct(shape, dtype)


def mm(a, b, dims=((1,), (0,))):
    return lax.dot_general(a, b, (dims, ((), ())), preferred_element_type=F32)


NT = ((1,), (1,))
TN = ((0,), (0,))


def load(arr, index=None):
    return arr, True, index


def held(arr):
    return arr, False, None


def first(x):
    return x[:1, :1]


class Work:
    def __init__(self, ins, outs, count, body, cost=1.0, fin=None):
        self.ins, self.outs, self.count, self.body, self.cost, self.fin = ins, outs, count, body, cost, fin


def stage_call(cid, local_fn, ins, out_shapes, ag=True, part=None, pro=None, swap=(), save=(), extra=None, trade=(),
               fills=(), sums=None, budget=(4.5, 2.0, 2.5, 3.0)):
    width = ins[0].shape[-1]
    rs = part is not None or pro is not None
    args, in_specs, place = [], [], {}

    def add(arr, spec=VMEM_SPEC):
        key = (id(arr), spec is HBM_SPEC)
        if key not in place:
            place[key] = len(args)
            args.append(arr)
            in_specs.append(spec)
        return place[key]

    outs, out_specs = [], []

    def add_out(shape, spec=VMEM_SPEC):
        outs.append(pltpu.HBM(shape.shape, shape.dtype) if spec is HBM_SPEC else shape)
        out_specs.append(spec)
        return len(outs) - 1

    scratch = []

    def add_scratch(item):
        scratch.append(item)
        return len(scratch) - 1

    i_part = add(part) if part is not None else None
    i_ins = [add(a) for a in ins]
    i_swap = [add(a) for a in swap]
    i_save = [add(a) for a in save]
    i_trade = [add(a) for a in trade]
    i_extra = [add(a) for a in extra[2:]] if extra else []
    i_sums = [add(a) for a in sums] if sums is not None else []
    o_local = [add_out(s) for s in out_shapes]
    full_shape = sds((N_SEQ, N_TP, PAD, width), BF16)
    o_full = add_out(full_shape) if ag else None
    o_swap = [add_out(sds(a.shape, BF16)) for a in swap]
    o_save = [add_out(sds(a.shape, BF16), HBM_SPEC) for a in save]
    o_trade = [add_out(sds(a.shape, a.dtype)) for a in trade]
    o_extra = add_out(sds((1, N_TP, PAD, width), BF16)) if extra else None
    o_sums = add_out(sds((16, width), F32)) if sums is not None else None
    works = ([pro] if pro else []) + list(fills)
    w_ins, w_outs = [], []
    n_load = n_store = 0
    for work in works:
        got = []
        for arr, copied, index in work.ins:
            if copied:
                k = add_scratch(pltpu.VMEM(arr.shape if index is None else arr.shape[1:], arr.dtype))
                got.append((add(arr, HBM_SPEC), index, k, n_load))
                n_load += 1
            else:
                got.append((add(arr), None, None, None))
        w_ins.append(got)
        kept = []
        for shape in work.outs:
            if shape.dtype == BF16:
                kept.append((add_out(shape, HBM_SPEC), add_scratch(pltpu.VMEM(shape.shape, shape.dtype)), n_store))
                n_store += 1
            else:
                kept.append((add_out(shape), None, None))
        w_outs.append(kept)
    shard = pltpu.VMEM((N_SEQ, PAD, width), BF16)
    if rs:
        s_bufs = [add_scratch(shard) for _ in range(4)]
        s_part = add_scratch(pltpu.VMEM(full_shape.shape, BF16)) if pro else None
    k_swap = 6 * N_SEQ
    k_extra = k_swap + 4 * len(swap)
    k_sum = k_extra + 3
    k_trade = k_sum + 3
    n_sem = k_trade + len(trade)
    s_send, s_recv = [add_scratch(pltpu.SemaphoreType.DMA((n_sem,))) for _ in range(2)]
    s_load = add_scratch(pltpu.SemaphoreType.DMA((n_load + n_store + len(save) + 1,)))
    if sums is not None:
        s_sum = [add_scratch(pltpu.VMEM((3, 16, width), F32)) for _ in range(2)]
    n_in, n_out = len(args), len(outs)

    def kernel(*refs):
        r_in, r_out, r_s = refs[:n_in], refs[n_in:n_in + n_out], refs[n_in + n_out:]
        in_refs = [r_in[k] for k in i_ins]
        out_refs = [r_out[k] for k in o_local]
        full = r_out[o_full] if ag else None
        ssem, rsem, lsem = r_s[s_send], r_s[s_recv], r_s[s_load]
        loads, use_in, use_out, stores, leaving = [], [], [], [], []
        for got, kept in zip(w_ins, w_outs):
            cps, use = [], []
            for k_in, index, k_buf, k_sem in got:
                if k_buf is None:
                    use.append(r_in[k_in])
                    continue
                src = r_in[k_in] if index is None else r_in[k_in].at[index]
                cps.append(pltpu.make_async_copy(src, r_s[k_buf], lsem.at[k_sem]))
                cps[-1].start()
                use.append(r_s[k_buf])
            loads.append(cps)
            use_in.append(use)
            use_out.append([r_out[k] if k_buf is None else r_s[k_buf] for k, k_buf, _ in kept])
            stores.append([pltpu.make_async_copy(r_s[k_buf], r_out[k], lsem.at[n_load + k_sem])
                           for k, k_buf, k_sem in kept if k_buf is not None])
        dp = lax.axis_index('dp')
        t = lax.axis_index('tp')
        core = lax.rem(t, 2)
        mate = t + 1 - 2 * core
        peer = lax.rem(t + 2, N_TP)
        far = lax.rem(mate + 2, N_TP)
        here, there = dp, 1 - dp

        def remote(src, dst, k, dev, line=None):
            return pltpu.make_async_remote_copy(src_ref=src, dst_ref=dst, send_sem=ssem.at[k], recv_sem=rsem.at[k],
                                                device_id=(here if line is None else line, dev), device_id_type=MESH_ID)

        def leave(cps):
            for cp in cps:
                cp.start()
            leaving.extend(cps)

        leave([pltpu.make_async_copy(r_in[a], r_out[b], lsem.at[n_load + n_store + k])
               for k, (a, b) in enumerate(zip(i_save, o_save))])
        barrier = pltpu.get_barrier_semaphore()
        peers = [(here, mate), (here, peer)]
        if swap or trade or sums is not None:
            peers.append((there, t))
        for dev in peers:
            pl.semaphore_signal(barrier, inc=1, device_id=dev, device_id_type=MESH_ID)
        pl.semaphore_wait(barrier, len(peers))

        first = 1 if pro else 0
        done = [0] * len(works)

        def run(time):
            for f in range(first, len(works)):
                work = works[f]
                left = work.count - done[f]
                n = left if time is None else min(left, int(time / work.cost + 0.5))
                if n <= 0:
                    continue
                if done[f] == 0:
                    for cp in loads[f]:
                        cp.wait()
                lo = done[f]
                done[f] = hi = lo + n
                if n == 1:
                    work.body(lo, use_in[f], use_out[f])
                else:
                    @pl.loop(lo, hi)
                    def _(i, work=work, f=f):
                        work.body(i, use_in[f], use_out[f])
                if hi == work.count:
                    leave(stores[f])
                if time is not None:
                    time -= n * work.cost

        started, landed = [], []
        for k, (a, b) in enumerate(zip(i_trade, o_trade)):
            cp = remote(r_in[a], r_out[b], k_trade + k, t, there)
            cp.start()
            started.append(cp)
            landed.append(cp)
        if extra:
            ex = r_out[o_extra]
            ex[0, t] = (row(r_in[i_extra[1]], extra[0]) * r_in[i_extra[0]][extra[1]].astype(F32)).astype(BF16)
            x_peer = remote(ex.at[0, t], ex.at[0, t], k_extra, peer)
            x_mate = remote(ex.at[0, t], ex.at[0, t], k_extra + 1, mate)
            x_peer.start()
            x_mate.start()
            started += [x_peer, x_mate]
            landed.append(x_mate)
        s_y = []
        for k in range(len(swap)):
            src, dst = r_in[i_swap[k]], r_out[o_swap[k]]
            for j in range(2):
                s_y.append(remote(src.at[:, core + 2 * j], dst.at[:, core + 2 * j], k_swap + 4 * k + j, t, there))
                s_y[-1].start()
        started += s_y
        if rs:
            far_buf, mate_buf, peer_buf, send_buf = [r_s[k] for k in s_bufs]
            part_ref = r_s[s_part] if pro else r_in[i_part]
            c_far = [remote(part_ref.at[b, far], far_buf.at[b], b, mate) for b in range(N_SEQ)]
            c_mate = [remote(part_ref.at[b, mate], mate_buf.at[b], N_SEQ + b, mate) for b in range(N_SEQ)]
            c_peer = [remote(send_buf.at[b], peer_buf.at[b], 2 * N_SEQ + b, peer) for b in range(N_SEQ)]

            def to_mate(b):
                c_far[b].start()
                c_mate[b].start()

            def to_peer(b):
                c_far[b].wait_recv()
                send_buf[b] = (part_ref[b, peer].astype(F32) + far_buf[b].astype(F32)).astype(BF16)
                c_peer[b].start()

            def produce(b, lo, hi):
                @pl.loop(lo, hi)
                def _(u):
                    pro.body(b, u, use_in[0], use_out[0])

            def finish(b):
                val = pro.fin(b, use_in[0], use_out[0]).astype(BF16)
                for k in range(N_TP):
                    part_ref[b, k] = val[k * PAD:(k + 1) * PAD]

            if pro:
                for cp in loads[0]:
                    cp.wait()
                half = pro.count // 2
                produce(0, 0, pro.count)
                finish(0)
                to_mate(0)
                produce(1, 0, half)
                to_peer(0)
                produce(1, half, pro.count)
                finish(1)
                to_mate(1)
                leave(stores[0])
                run(1.0)
                to_peer(1)
                run(budget[0] - 3.0)
            else:
                for b in range(N_SEQ):
                    to_mate(b)
                for b in range(N_SEQ):
                    to_peer(b)
                run(budget[0])
            started += c_far + c_mate + c_peer
        g_peer, g_mate, g_fwd = [], [], []
        for b in range(N_SEQ):
            acc = None
            if rs:
                if b:
                    run(budget[1])
                c_mate[b].wait_recv()
                acc = part_ref[b, t].astype(F32) + mate_buf[b].astype(F32)
                c_peer[b].wait_recv()
                acc = acc + peer_buf[b].astype(F32)
            val = local_fn(b, acc, in_refs, out_refs)
            if ag:
                full[b, t] = val
                g_peer.append(remote(full.at[b, t], full.at[b, t], 3 * N_SEQ + b, peer))
                g_mate.append(remote(full.at[b, t], full.at[b, t], 4 * N_SEQ + b, mate))
                g_peer[b].start()
                g_mate[b].start()
        if sums is not None:
            sum_src, sum_dst = [r_s[k] for k in s_sum]
            sum_src[0, 0:2, :] = out_refs[-1][...]
            at = 2
            for k in i_sums:
                n_rows = args[k].shape[0]
                sum_src[0, at:at + n_rows, :] = r_in[k][...]
                at += n_rows
            for k, (line, dev) in enumerate([(here, mate), (here, peer), (there, t)]):
                cp = remote(sum_src.at[k], sum_dst.at[k], k_sum + k, dev, line)
                cp.start()
                if k:
                    run(budget[2])
                cp.wait_recv()
                started.append(cp)
                total = sum_src[k] + sum_dst[k]
                if k < 2:
                    sum_src[k + 1] = total
                else:
                    r_out[o_sums][...] = total
        if extra:
            x_peer.wait_recv()
            x_fwd = remote(ex.at[0, peer], ex.at[0, peer], k_extra + 2, mate)
            x_fwd.start()
            started.append(x_fwd)
            landed.append(x_fwd)
        if ag:
            for b in range(N_SEQ):
                run(budget[2 + b])
                g_peer[b].wait_recv()
                g_fwd.append(remote(full.at[b, peer], full.at[b, peer], 5 * N_SEQ + b, mate))
                g_fwd[b].start()
            started += g_peer + g_mate + g_fwd
            landed += g_mate + g_fwd
        for k in range(len(swap)):
            dst = r_out[o_swap[k]]
            for j in range(2):
                s_y[2 * k + j].wait_recv()
                cp = remote(dst.at[:, core + 2 * j], dst.at[:, core + 2 * j], k_swap + 4 * k + 2 + j, mate)
                cp.start()
                started.append(cp)
                landed.append(cp)
        run(None)
        for cp in landed:
            cp.wait_recv()
        for cp in started:
            cp.wait_send()
        for cp in leaving:
            cp.wait()

    return pl.pallas_call(
        kernel,
        out_shape=outs,
        in_specs=in_specs,
        out_specs=out_specs,
        scratch_shapes=scratch,
        compiler_params=pltpu.CompilerParams(collective_id=cid, has_side_effects=True, vmem_limit_bytes=40 * 2 ** 20),
        cost_estimate=pl.CostEstimate(flops=40_000_000, bytes_accessed=4_000_000, transcendentals=0),
        name=f'stage{cid}',
    )(*args)


def row(ref, layer):
    return ref[layer:layer + 1, :]


def ln_stats(x):
    x_f32 = x.astype(F32)
    centered = x_f32 - jnp.mean(x_f32, axis=-1, keepdims=True)
    inv_std = lax.rsqrt(jnp.mean(centered * centered, axis=-1, keepdims=True) + NORM_EPS)
    return centered * inv_std, inv_std


def ln_bwd(grad_out, x, gain):
    x_hat, inv_std = ln_stats(x)
    grad_hat = grad_out * gain
    mean_one = jnp.mean(grad_hat, axis=-1, keepdims=True)
    mean_two = jnp.mean(grad_hat * x_hat, axis=-1, keepdims=True)
    return inv_std * (grad_hat - mean_one - x_hat * mean_two), x_hat


def add_rows(rows_ref, b, rows):
    for k, val in enumerate(rows):
        s = jnp.sum(val, axis=0, keepdims=True)
        rows_ref[k:k + 1, :] = s if b == 0 else rows_ref[k:k + 1, :] + s


def key_valid(seq_len):
    col = lax.broadcasted_iota(jnp.int32, (SEQ, SEQ), 1)
    shard = jnp.zeros_like(col)
    for k in range(1, N_TP):
        shard = shard + (col >= k * PAD).astype(jnp.int32)
    return jnp.logical_and(col - PAD * shard < TOK, col - (PAD - TOK) * shard < seq_len)


def head_probs(q_half, k_pair, valid):
    scores = mm(q_half, k_pair, NT) * 0.125
    scores = jnp.where(valid, scores, NEG_BIG)
    e = jnp.exp(scores - jnp.max(scores, axis=-1, keepdims=True))
    return e / jnp.sum(e, axis=-1, keepdims=True)


def seq_rows(b):
    return pl.ds(b * SEQ if isinstance(b, int) else pl.multiple_of(b * SEQ, SEQ), SEQ)


def pair_cols(pair):
    return pl.ds(pl.multiple_of(pair * 128, 128), 128)


def by_seq(x):
    return x.reshape(-1, SEQ, x.shape[-1])


def flat(x):
    return x.reshape(-1, x.shape[-1])


def each_seq(refs):
    return [ref.at[k] for ref in refs for k in range(ref.shape[0])]


def attn_fwd_unit(b, pair, x, w_ref, bias, seq_len, qkv_ref, o_ref):
    rows, cols = seq_rows(b), pair_cols(pair)
    pieces = []
    for c in range(3):
        val = (mm(x, w_ref[c, cols, :], NT) + bias[c:c + 1, cols]).astype(BF16)
        qkv_ref[c, rows, cols] = val
        pieces.append(val)
    q, k, v = pieces
    valid = key_valid(seq_len)
    half = lax.broadcasted_iota(jnp.int32, (SEQ, 128), 1) // 64
    res = []
    for h in range(2):
        probs = head_probs(jnp.where(half == h, q, jnp.zeros_like(q)), k, valid)
        res.append(mm(probs.astype(BF16), v))
    o_ref[rows, cols] = jnp.where(half == 0, res[0], res[1]).astype(BF16)


def attn_bwd_unit(b, pair, g, qkv_ref, w_ref, seq_len, dqkv_ref, db_ref):
    rows, cols = seq_rows(b), pair_cols(pair)
    do = mm(g, w_ref[cols, :], NT).astype(BF16)
    q, k, v = (qkv_ref[c, rows, cols] for c in range(3))
    valid = key_valid(seq_len)
    half = lax.broadcasted_iota(jnp.int32, (SEQ, 128), 1) // 64
    dq, dk, dv = [], [], []
    for h in range(2):
        probs = head_probs(jnp.where(half == h, q, jnp.zeros_like(q)), k, valid)
        grad_p = mm(jnp.where(half == h, do, jnp.zeros_like(do)), v, NT)
        grad_s = (probs * (grad_p - jnp.sum(grad_p * probs, axis=-1, keepdims=True)) * 0.125).astype(BF16)
        dv.append(mm(probs.astype(BF16), do, TN))
        dq.append(mm(grad_s, k))
        dk.append(mm(grad_s, q, TN))
    for c, pieces in enumerate((dq, dk, dv)):
        val = jnp.where(half == 0, pieces[0], pieces[1])
        dqkv_ref[c, rows, cols] = val.astype(BF16)
        db_ref[b, c:c + 1, cols] = jnp.sum(val, axis=0, keepdims=True)


def mlp_up_unit(x, u_ref, bias, cols):
    gate = mm(x, u_ref[0, :, cols]) + bias[0:1, cols]
    lin = mm(x, u_ref[1, :, cols]) + bias[1:2, cols]
    return gate, lin


def mlp_bwd_unit(b, u, x, g, u_ref, bias, d_ref, hid_ref, gp_ref, gb_ref):
    rows, cols = seq_rows(b), pl.ds(pl.multiple_of(u * 256, 256), 256)
    gate, lin = mlp_up_unit(x, u_ref, bias, cols)
    grad_hid = mm(g, d_ref[cols, :], NT)
    sig = jax.nn.sigmoid(gate)
    if hid_ref is not None:
        hid_ref[rows, cols] = (gate * sig * lin).astype(BF16)
    grad_gate = grad_hid * lin * sig * (1.0 + gate * (1.0 - sig))
    grad_lin = grad_hid * gate * sig
    for c, val in enumerate((grad_gate, grad_lin)):
        gp_ref[c, rows, cols] = val.astype(BF16)
        gb_ref[b, c:c + 1, cols] = jnp.sum(val, axis=0, keepdims=True)


QKV = sds((3, ROWS, 256), BF16)
HEADS = sds((ROWS, 256), BF16)
HIDDEN = sds((ROWS, 1024), BF16)
GRAD_PRE = sds((2, ROWS, 1024), BF16)
GRAD_BQ = sds((N_SEQ, 3, 256), F32)
GRAD_BU = sds((N_SEQ, 2, 1024), F32)


def fill_attn_fwd(layer, normed, wq, bq, lens):
    def body(i, ins, outs):
        n_ref, w_ref, b_ref, vl_ref = ins
        b = i // 2
        attn_fwd_unit(b, i % 2, n_ref[b], w_ref, b_ref.at[layer], first(vl_ref[b]), *outs)
    return Work([held(by_seq(normed)), load(wq, layer), held(bq), held(lens)],
                [QKV, HEADS], 4, body, 1.7)


def fill_attn_bwd(layer, qkv, grad, wp, lens):
    def body(i, ins, outs):
        qkv_ref, g_ref, w_ref, vl_ref = ins
        b = i // 2
        attn_bwd_unit(b, i % 2, g_ref[b], qkv_ref, w_ref, first(vl_ref[b]), *outs)
    return Work([load(qkv), held(by_seq(grad)), load(wp, layer), held(lens)],
                [QKV, GRAD_BQ], 4, body, 2.0)


def fill_mlp(layer, normed, grads, w_up, b_up, w_down):
    grads = [by_seq(g) for g in grads]

    def body(i, ins, outs):
        n_ref, u_ref, b_ref, d_ref = ins[:4]
        for b, g in enumerate(each_seq(ins[4:])):
            mlp_bwd_unit(b, i, n_ref[b], g[...], u_ref, b_ref.at[layer], d_ref, *outs)
    return Work([load(by_seq(normed)), load(w_up, layer), held(b_up), load(w_down, layer)] + [held(g) for g in grads],
                [HIDDEN, GRAD_PRE, GRAD_BU], 4, body, 1.8)


def pro_attn_fwd(layer, normed, wq, bq, wp, lens):
    def body(b, u, ins, outs):
        n_ref, w_ref, b_ref, _, vl_ref = ins
        attn_fwd_unit(b, u, n_ref[b], w_ref, b_ref.at[layer], first(vl_ref[b]), *outs)

    def fin(b, ins, outs):
        return mm(outs[1][seq_rows(b), :], ins[3][...])
    return Work([held(by_seq(normed)), load(wq, layer), held(bq), load(wp, layer),
                 held(lens)], [QKV, HEADS], 2, body, fin=fin)


def pro_mlp_fwd(layer, normed, w_up, b_up, w_down):
    def body(b, u, ins, outs):
        n_ref, u_ref, b_ref, _ = ins
        cols = pl.ds(pl.multiple_of(u * 256, 256), 256)
        gate, lin = mlp_up_unit(n_ref[b], u_ref, b_ref.at[layer], cols)
        outs[0][seq_rows(b), cols] = (jax.nn.silu(gate) * lin).astype(BF16)

    def fin(b, ins, outs):
        return mm(outs[0][seq_rows(b), :], ins[3][...])
    return Work([held(by_seq(normed)), load(w_up, layer), held(b_up), load(w_down, layer)],
                [HIDDEN], 4, body, fin=fin)


def pro_mlp_bwd(layer, normed, grads, w_up, b_up, w_down, forward):
    grads = [by_seq(g) for g in grads]

    def body(b, u, ins, outs):
        n_ref, u_ref, b_ref, d_ref = ins[:4]
        seqs = each_seq(ins[4:])
        mlp_bwd_unit(b, u, n_ref[b], seqs[b][...], u_ref, b_ref.at[layer], d_ref, outs[2] if forward else None, *outs[:2])

    def fin(b, ins, outs):
        rows = seq_rows(b)
        if forward:
            outs[3][rows, :] = mm(outs[2][rows, :], ins[3][...]).astype(BF16)
        return (mm(outs[0][0, rows, :], ins[1][0], NT) + mm(outs[0][1, rows, :], ins[1][1], NT))
    return Work([held(by_seq(normed)), load(w_up, layer), held(b_up), load(w_down, layer)]
                + [held(g) for g in grads],
                [GRAD_PRE, GRAD_BU] + ([HIDDEN, sds((ROWS, 1024), BF16)] if forward else []), 4, body, fin=fin)


def pro_attn_bwd(layer, qkv, grad, wp, wq, lens):
    def body(b, u, ins, outs):
        qkv_ref, g_ref, w_ref, _, vl_ref = ins
        attn_bwd_unit(b, u, g_ref[b], qkv_ref, w_ref, first(vl_ref[b]), *outs)

    def fin(b, ins, outs):
        rows = seq_rows(b)
        return sum(mm(outs[0][c, rows, :], ins[3][c]) for c in range(3))
    return Work([load(qkv), held(by_seq(grad)), load(wp, layer), load(wq, layer),
                 held(lens)], [QKV, GRAD_BQ], 2, body, fin=fin)


def gather_norm(cid, layer, x, gain, bias, **side):
    def local(b, acc, ins, outs):
        x_ref, g_ref, b_ref = ins
        x_hat, _ = ln_stats(x_ref[b])
        return (x_hat * row(g_ref, layer) + row(b_ref, layer)).astype(BF16)
    return stage_call(cid, local, (x, gain, bias), [], **side)


def residual_norm(cid, layer, x, bias, scale, norm_layer, gain, shift, **side):
    def local(b, acc, ins, outs):
        x_ref, b_ref, s_ref, g_ref, h_ref = ins
        total = acc + row(b_ref, layer)
        outs[1][b] = total
        x_new = (x_ref[b].astype(F32) + row(s_ref, layer) * total).astype(BF16)
        outs[0][b] = x_new
        x_hat, _ = ln_stats(x_new)
        return (x_hat * row(g_ref, norm_layer) + row(h_ref, norm_layer)).astype(BF16)
    return stage_call(cid, local, (x, bias, scale, gain, shift), [sds(x.shape, BF16), sds(x.shape, F32)], **side)


def residual_last(cid, layer, x, bias, scale, grad_y, **side):
    def local(b, acc, ins, outs):
        x_ref, b_ref, s_ref, g_ref = ins
        total = acc + row(b_ref, layer)
        outs[0][b] = (x_ref[b].astype(F32) + row(s_ref, layer) * total).astype(BF16)
        grad = g_ref[b].astype(F32)
        add_rows(outs[1], b, [grad * total, row(s_ref, layer) * grad])
    return stage_call(cid, local, (x, bias, scale, grad_y), [sds(x.shape, BF16), sds((2, x.shape[-1]), F32)], ag=False, **side)


def back_mid(cid, layer, x_mid, gain, grad_res, attn_sum, scale, **side):
    def local(b, acc, ins, outs):
        x_ref, g_ref, r_ref, a_ref, s_ref = ins
        grad_in, x_hat = ln_bwd(acc, x_ref[b], row(g_ref, layer))
        grad_mid = r_ref[b].astype(F32) + grad_in
        outs[0][b] = grad_mid
        grad_attn = row(s_ref, layer) * grad_mid
        add_rows(outs[1], b, [acc * x_hat, acc, grad_mid * a_ref[b], grad_attn])
        return grad_attn.astype(BF16)
    return stage_call(cid, local, (x_mid, gain, grad_res, attn_sum, scale),
                      [sds(x_mid.shape, F32), sds((4, x_mid.shape[-1]), F32)], **side)


def back_in(cid, layer, x_in, gain, grad_mid, mlp_sum, scale, **side):
    more = layer > 0

    def local(b, acc, ins, outs):
        x_ref, g_ref, m_ref = ins[:3]
        grad_in, x_hat = ln_bwd(acc, x_ref[b], row(g_ref, layer))
        grad = (m_ref[b] + grad_in).astype(BF16)
        outs[0][b] = grad
        if not more:
            add_rows(outs[1], b, [acc * x_hat, acc])
            return None
        grad = grad.astype(F32)
        grad_mlp = row(ins[4], layer - 1) * grad
        add_rows(outs[1], b, [acc * x_hat, acc])
        add_rows(outs[2], b, [grad * ins[3][b], grad_mlp])
        return grad_mlp.astype(BF16)
    shapes = [sds(x_in.shape, BF16)] + [sds((2, x_in.shape[-1]), F32)] * (2 if more else 1)
    return stage_call(cid, local, (x_in, gain, grad_mid) + ((mlp_sum, scale) if more else ()), shapes, ag=more, **side)


def grads_call(jobs, biases, sums):
    args, bufs, loads = [], [], []
    for job in jobs:
        for arrs in job[2:]:
            at = 0
            for arr in arrs:
                loads.append((len(args), len(bufs), at))
                args.append(arr)
                at += arr.shape[-2]
            bufs.append(pltpu.VMEM((*arrs[0].shape[:-2], at, arrs[0].shape[-1]), BF16))
    n_op = len(args)
    small = [x for group in biases for pair in group for x in pair] + [sums]
    args += small
    specs = [HBM_SPEC] * n_op + [VMEM_SPEC] * len(small)
    width = sums.shape[-1]
    shapes = [(groups, total, width) for groups, total in ((2, 1024), (1, 1024), (3, 256), (1, 256))]
    shapes += [group[0][0].shape[1:] for group in biases] + [(width,)] * 8
    outs = [sds((2, *shape), F32) for shape in shapes]
    stage_rows = 512

    def kernel(*refs):
        ops, smalls = refs[:n_op], refs[n_op:len(args)]
        out = refs[len(args):len(args) + len(outs)]
        buf = refs[len(args) + len(outs):]
        stage, lsem, osem = buf[len(bufs):]
        copies = []
        for k, k_buf, at in loads:
            rows = pl.ds(at, ops[k].shape[-2])
            dst = buf[k_buf].at[:, rows] if len(ops[k].shape) == 3 else buf[k_buf].at[rows]
            copies.append(pltpu.make_async_copy(ops[k], dst, lsem.at[k]))

        def fetch(j, act):
            for cp, (_, k_buf, _) in zip(copies, loads):
                if k_buf // 2 == j:
                    act(cp)

        for j in range(2):
            fetch(j, lambda cp: cp.start())
        for l in range(2):
            for k, pairs in enumerate((smalls[:4], smalls[4:])):
                out[4 + k][l] = jnp.sum(pairs[2 * l][...] + pairs[2 * l + 1][...], axis=0)
        rows = smalls[-1]
        for k in range(8):
            for l, at in enumerate((8 + k, 2 + k if k < 6 else k - 6)):
                out[6 + k][l:l + 1, :] = rows[at:at + 1, :]
        pending = [None] * 2
        step = 0
        for j, (slot, layer, *_) in enumerate(jobs):
            a_ref, b_ref = buf[2 * j:2 * j + 2]
            fetch(j, lambda cp: cp.wait())
            fetch(j + 2, lambda cp: cp.start())
            groups, total = outs[slot].shape[1:3]
            blk = min(stage_rows, total)
            for g in range(groups):
                for i in range(total // blk):
                    cols = slice(i * blk, (i + 1) * blk)
                    a = a_ref[g, :, cols] if len(a_ref.shape) == 3 else a_ref[:, cols]
                    b = b_ref[g] if len(b_ref.shape) == 3 else b_ref[...]
                    s = step % 2
                    if pending[s] is not None:
                        pending[s].wait()
                    stage[s, :blk] = mm(a, b, TN)
                    pending[s] = pltpu.make_async_copy(stage.at[s, pl.ds(0, blk)], out[slot].at[layer, g, pl.ds(i * blk, blk)],
                                                       osem.at[s])
                    pending[s].start()
                    step += 1
        for cp in pending:
            cp.wait()

    return pl.pallas_call(
        kernel,
        out_shape=outs,
        in_specs=specs,
        out_specs=[HBM_SPEC] * 4 + [VMEM_SPEC] * 10,
        scratch_shapes=bufs + [pltpu.VMEM((2, stage_rows, width), F32), pltpu.SemaphoreType.DMA((n_op,)),
                               pltpu.SemaphoreType.DMA((2,))],
        compiler_params=pltpu.CompilerParams(vmem_limit_bytes=60 * 2 ** 20),
        cost_estimate=pl.CostEstimate(flops=40_000_000_000, bytes_accessed=80_000_000, transcendentals=0),
        name='grads')(*args)


def device_fn(tokens, grad_y, valid_len, norm1_gain, norm1_bias, w_qkv, b_qkv, w_proj, b_proj, layer_scale1,
              norm2_gain, norm2_bias, w_up, b_up, w_down, b_down, layer_scale2):
    pad = ((0, 0), (0, PAD - TOK), (0, 0))
    x0 = jnp.pad(tokens, pad)
    g_y = jnp.pad(grad_y, pad)
    lens = jnp.broadcast_to(valid_len[:, None, None], (N_SEQ, 8, 128))
    wq = w_qkv.transpose(0, 1, 3, 4, 2).reshape(2, 3, 256, 1024)
    bq = b_qkv.reshape(2, 3, 256)
    wp = w_proj.reshape(2, 256, 1024)

    n1_0, lens_x = gather_norm(0, 0, x0, norm1_gain, norm1_bias, trade=[lens])
    mid_0, asum_0, n2_0, n1_0x, n1_0h, gm_1a, qkv_0, o_0 = residual_norm(
        1, 0, x0, b_proj, layer_scale1, 0, norm2_gain, norm2_bias, pro=pro_attn_fwd(0, n1_0, wq, bq, wp, lens),
        swap=[n1_0], save=[n1_0], extra=(1, 0, g_y, layer_scale2))
    x1, msum_0, n1_1, n2_0x, gm_1ax, n2_0h, n1_0xh, gm_1ah, gm_1b, hid_0, qkv_0x, o_0x = residual_norm(
        2, 0, mid_0, b_down, layer_scale2, 1, norm1_gain, norm1_bias, pro=pro_mlp_fwd(0, n2_0, w_up, b_up, w_down),
        swap=[n2_0, gm_1a], save=[n2_0, n1_0x, gm_1a], extra=(1, 1, g_y, layer_scale2),
        fills=[fill_attn_fwd(0, n1_0x, wq, bq, lens_x)])
    mid_1, asum_1, n2_1, n1_1x, gm_1bx, n1_1h, gm_1bh, gm_1axh, qkv_1, o_1 = residual_norm(
        3, 1, x1, b_proj, layer_scale1, 1, norm2_gain, norm2_bias, pro=pro_attn_fwd(1, n1_1, wq, bq, wp, lens),
        swap=[n1_1, gm_1b], save=[n1_1, gm_1b, gm_1ax])

    gmid_1, rows_mid_1, ga_1, n2_1x, n2_1h, n1_1xh, gm_1bxh, gp_1, gb_1, hid_1, part_y, qkv_1x, o_1x = back_mid(
        4, 1, mid_1, norm2_gain, g_y, asum_1, layer_scale1,
        pro=pro_mlp_bwd(1, n2_1, [gm_1a, gm_1b], w_up, b_up, w_down, True),
        swap=[n2_1], save=[n2_1, n1_1x, gm_1bx], fills=[fill_attn_fwd(1, n1_1x, wq, bq, lens_x)])
    grad_1, rows_in_1, rows_mlp_0, gm_0, ga_1x, ga_1h, gq_1, gbq_1, hid_1x, gp_1x, gb_1x = back_in(
        5, 1, x1, norm1_gain, gmid_1, msum_0, layer_scale2, pro=pro_attn_bwd(1, qkv_1, ga_1, wp, wq, lens), swap=[ga_1],
        save=[ga_1], fills=[fill_mlp(1, n2_1x, [gm_1ax, gm_1bx], w_up, b_up, w_down)])

    gmid_0, rows_mid_0, ga_0, gm_0x, gm_0h, ga_1xh, gp_0, gb_0, gq_1x, gbq_1x = back_mid(
        6, 0, mid_0, norm2_gain, grad_1, asum_0, layer_scale1,
        pro=pro_mlp_bwd(0, n2_0, [gm_0], w_up, b_up, w_down, False),
        swap=[gm_0], save=[gm_0, ga_1x], fills=[fill_attn_bwd(1, qkv_1x, ga_1x, wp, lens_x)])
    grad_0, rows_in_0, ga_0x, ga_0h, gm_0xh, gq_0, gbq_0, hid_0x, gp_0x, gb_0x = back_in(
        7, 0, x0, norm1_gain, gmid_0, None, None, pro=pro_attn_bwd(0, qkv_0, ga_0, wp, wq, lens), swap=[ga_0],
        save=[ga_0, gm_0x], fills=[fill_mlp(0, n2_0x, [gm_0x], w_up, b_up, w_down)])
    y_out, _, ga_0xh, sums, gq_0x, gbq_0x = residual_last(
        8, 1, mid_1, b_down, layer_scale2, g_y, part=part_y.reshape(N_SEQ, N_TP, PAD, -1), save=[ga_0x],
        fills=[fill_attn_bwd(0, qkv_0x, ga_0x, wp, lens_x)],
        sums=(rows_in_1, rows_mid_1, rows_in_0, rows_mid_0, rows_mlp_0))

    operands = (
        ((n2_1h, n2_1x), (gp_1, gp_1x), (hid_1, hid_1x), (gm_1ah, gm_1bh, gm_1axh, gm_1bxh), (gq_1, gq_1x), (n1_1h, n1_1xh),
         (o_1, o_1x), (ga_1h, ga_1xh)),
        ((n2_0h, n2_0x), (gp_0, gp_0x), (hid_0, hid_0x), (gm_0h, gm_0xh), (gq_0, gq_0x), (n1_0h, n1_0xh),
         (o_0, o_0x), (ga_0h, ga_0xh)))
    jobs = []
    for k, ops in enumerate(operands):
        ops = [[a if a.ndim < 4 else flat(a) for a in arrs] for arrs in ops]
        jobs += [(slot, 1 - k, *ops[2 * slot:2 * slot + 2]) for slot in reversed(range(4))]
    g_up, g_down, g_qkv, g_proj, g_b_up, g_b_qkv, n1g, n1b, n2g, n2b, ls1, bp, ls2, bd = grads_call(
        jobs, [[(gb_0, gb_0x), (gb_1, gb_1x)], [(gbq_0, gbq_0x), (gbq_1, gbq_1x)]], sums)
    return (y_out[:, :TOK], grad_0[:, :TOK], n1g, n1b,
            g_qkv.reshape(2, 3, 4, 64, 1024).transpose(0, 1, 4, 2, 3), g_b_qkv.reshape(2, 3, 4, 64),
            g_proj.reshape(2, 4, 64, 1024), bp, ls1, n2g, n2b, g_up, g_b_up,
            g_down.reshape(2, 1024, 1024), bd, ls2)


def solution(mesh):
    rep = P()
    act = P('dp', 'tp', None)
    param_specs = (rep, rep, P(None, None, None, 'tp', None), P(None, None, 'tp', None), P(None, 'tp', None, None), rep,
                   rep, rep, rep, P(None, None, None, 'tp'), P(None, None, 'tp'), P(None, 'tp', None), rep, rep)
    return jax.shard_map(device_fn, mesh=mesh, in_specs=(act, act, P('dp')) + param_specs,
                         out_specs=(act, act) + param_specs, check_vma=False)
```

```python
import itertools

import jax
import jax.numpy as jnp
from jax import lax
from jax.experimental import pallas as pl
from jax.experimental.pallas import tpu as pltpu
from jax.sharding import PartitionSpec as P

NORM_EPS = 1e-6
NEG_BIG = -1e9
F32 = jnp.float32
BF16 = jnp.bfloat16
TOK = 66
PAD = 72
N_TP = 4
N_SEQ = 2
SEQ = N_TP * PAD
ROWS = N_SEQ * SEQ
WIDTH = 1024
HEADS = 256
LANES = 128
MIB = 2 ** 20
MESH_ID = pl.DeviceIdType.MESH
VMEM_SPEC = pl.BlockSpec(memory_space=pltpu.VMEM)
HBM_SPEC = pl.BlockSpec(memory_space=pltpu.HBM)


def sds(shape, dtype):
    return jax.ShapeDtypeStruct(shape, dtype)


def mm(a, b, dims=((1,), (0,))):
    return lax.dot_general(a, b, (dims, ((), ())), preferred_element_type=F32)


NT = ((1,), (1,))
TN = ((0,), (0,))


def load(arr, index=None):
    return arr, True, index


def held(arr):
    return arr, False, None


def first(x):
    return x[:1, :1]


class Work:
    def __init__(self, ins, outs, count, body, cost=1.0, fin=None, x=None):
        self.ins, self.outs, self.count, self.body, self.cost, self.fin, self.x = ins, outs, count, body, cost, fin, x


def sequence(ref, b=0):
    return jnp.concatenate([ref[b, k] for k in range(N_TP)], axis=0)


def stage_call(cid, local_fn, ins, out_shapes, ag=True, parts=(), pro=None, nxt=None, swap=(), save=(), extra=None, trade=(),
               fills=(), sums=None, second=None, budget=(4.5, 2.0, 2.5, 3.0)):
    width = ins[0].shape[-1]
    rs = bool(parts)
    args, in_specs, place = [], [], {}

    def add(arr, spec=VMEM_SPEC):
        key = (id(arr), spec is HBM_SPEC)
        if key not in place:
            place[key] = len(args)
            args.append(pltpu.with_memory_space_constraint(arr, pltpu.HBM) if spec is HBM_SPEC else arr)
            in_specs.append(spec)
        return place[key]

    outs, out_specs = [], []

    def add_out(shape, spec=VMEM_SPEC):
        outs.append(pltpu.HBM(shape.shape, shape.dtype) if spec is HBM_SPEC else shape)
        out_specs.append(spec)
        return len(outs) - 1

    scratch = []

    def add_scratch(item):
        scratch.append(item)
        return len(scratch) - 1

    i_parts = [add(a) for a in parts]
    i_x = add(pro.x) if pro else None
    parts2, local2, ins2, shapes2 = second or ((), None, (), ())
    i_parts2 = [add(a) for a in parts2]
    i_ins2 = [add(a) for a in ins2]
    i_ins = [add(a) for a in ins]
    i_swap = [add(a) for a in swap]
    i_save = [add(a) for a in save]
    i_trade = [add(a) for a in trade]
    i_extra = [add(a) for a in extra[2:]] if extra else []
    i_sums = [add(a) for a in sums] if sums is not None else []
    o_local = [add_out(s) for s in out_shapes]
    o_local2 = [add_out(s) for s in shapes2]
    full_shape = sds((N_SEQ, N_TP, PAD, width), BF16)
    o_full = add_out(full_shape) if ag else None
    o_swap = [add_out(sds(a.shape, BF16)) for a in swap]
    o_save = [add_out(sds(a.shape, BF16), HBM_SPEC) for a in save]
    o_trade = [add_out(sds(a.shape, a.dtype)) for a in trade]
    o_extra = add_out(sds((1, N_TP, PAD, width), BF16)) if extra else None
    o_sums = add_out(sds((16, width), F32)) if sums is not None else None
    works = ([pro] if pro else []) + ([nxt] if nxt else []) + list(fills)
    o_part = add_out(sds((N_TP, PAD, width), BF16)) if nxt else None
    s_x = [add_scratch(pltpu.VMEM((SEQ, width), BF16)) for _ in range(2)]
    w_ins, w_outs = [], []
    n_load = n_store = 0
    for work in works:
        got = []
        for arr, copied, index in work.ins:
            if copied:
                k = add_scratch(pltpu.VMEM(arr.shape if index is None else arr.shape[1:], arr.dtype))
                got.append((add(arr, HBM_SPEC), index, k, n_load))
                n_load += 1
            else:
                got.append((add(arr), None, None, None))
        w_ins.append(got)
        kept = []
        for shape in work.outs:
            if shape.dtype == BF16:
                kept.append((add_out(shape, HBM_SPEC), add_scratch(pltpu.VMEM(shape.shape, shape.dtype)), n_store))
                n_store += 1
            else:
                kept.append((add_out(shape), None, None))
        w_outs.append(kept)
    shard = pltpu.VMEM((N_SEQ, PAD, width), BF16)
    s_bufs2 = [add_scratch(shard) for _ in range(4)] if second else []
    if rs:
        s_bufs = [add_scratch(shard) for _ in range(4)]
        s_part = add_scratch(pltpu.VMEM((N_TP, PAD, width), BF16)) if pro else None
    k_swap = 6 * N_SEQ
    k_extra = k_swap + 4 * len(swap)
    k_sum = k_extra + 3
    k_trade = k_sum + 3
    k_second = k_trade + len(trade)
    n_sem = k_second + 3 * N_SEQ * bool(second)
    s_send, s_recv = [add_scratch(pltpu.SemaphoreType.DMA((n_sem,))) for _ in range(2)]
    s_load = add_scratch(pltpu.SemaphoreType.DMA((n_load + n_store + len(save) + 1,)))
    if sums is not None:
        s_sum = [add_scratch(pltpu.VMEM((3, 16, width), F32)) for _ in range(2)]
    n_in, n_out = len(args), len(outs)

    def kernel(*refs):
        r_in, r_out, r_s = refs[:n_in], refs[n_in:n_in + n_out], refs[n_in + n_out:]
        in_refs = [r_in[k] for k in i_ins]
        out_refs = [r_out[k] for k in o_local]
        full = r_out[o_full] if ag else None
        ssem, rsem, lsem = r_s[s_send], r_s[s_recv], r_s[s_load]
        loads, use_in, use_out, stores, leaving = [], [], [], [], []
        for got, kept in zip(w_ins, w_outs):
            cps, use = [], []
            for k_in, index, k_buf, k_sem in got:
                if k_buf is None:
                    use.append(r_in[k_in])
                    continue
                src = r_in[k_in] if index is None else r_in[k_in].at[index]
                cps.append(pltpu.make_async_copy(src, r_s[k_buf], lsem.at[k_sem]))
                cps[-1].start()
                use.append(r_s[k_buf])
            loads.append(cps)
            use_in.append(use)
            use_out.append([r_out[k] if k_buf is None else r_s[k_buf] for k, k_buf, _ in kept])
            stores.append([pltpu.make_async_copy(r_s[k_buf], r_out[k], lsem.at[n_load + k_sem])
                           for k, k_buf, k_sem in kept if k_buf is not None])
        dp = lax.axis_index('dp')
        t = lax.axis_index('tp')
        core = lax.rem(t, 2)
        mate = t + 1 - 2 * core
        peer = lax.rem(t + 2, N_TP)
        far = lax.rem(mate + 2, N_TP)
        here, there = dp, 1 - dp

        def remote(src, dst, k, dev, line=None):
            return pltpu.make_async_remote_copy(src_ref=src, dst_ref=dst, send_sem=ssem.at[k], recv_sem=rsem.at[k],
                                                device_id=(here if line is None else line, dev), device_id_type=MESH_ID)

        def leave(cps):
            for cp in cps:
                cp.start()
            leaving.extend(cps)

        leave([pltpu.make_async_copy(r_in[a], r_out[b], lsem.at[n_load + n_store + k])
               for k, (a, b) in enumerate(zip(i_save, o_save))])
        barrier = pltpu.get_barrier_semaphore()
        peers = [(here, mate), (here, peer)]
        if swap or trade or sums is not None:
            peers.append((there, t))
        for dev in peers:
            pl.semaphore_signal(barrier, inc=1, device_id=dev, device_id_type=MESH_ID)
        pl.semaphore_wait(barrier, len(peers))

        first = bool(pro) + bool(nxt)
        done = [0] * len(works)

        def run(time):
            for f in range(first, len(works)):
                work = works[f]
                left = work.count - done[f]
                n = left if time is None else min(left, int(time / work.cost + 0.5))
                if n <= 0:
                    continue
                if done[f] == 0:
                    for cp in loads[f]:
                        cp.wait()
                lo = done[f]
                done[f] = hi = lo + n
                if n == 1:
                    work.body(lo, use_in[f], use_out[f])
                else:
                    @pl.loop(lo, hi)
                    def _(i, work=work, f=f):
                        work.body(i, use_in[f], use_out[f])
                if hi == work.count:
                    leave(stores[f])
                if time is not None:
                    time -= n * work.cost

        def channel(part_refs, bufs, k0):
            far_buf, mate_buf, peer_buf, send_buf = [r_s[k] for k in bufs]
            c_far = [remote(part_refs[b].at[far], far_buf.at[b], k0 + b, mate) for b in range(N_SEQ)]
            c_mate = [remote(part_refs[b].at[mate], mate_buf.at[b], k0 + N_SEQ + b, mate) for b in range(N_SEQ)]
            c_peer = [remote(send_buf.at[b], peer_buf.at[b], k0 + 2 * N_SEQ + b, peer) for b in range(N_SEQ)]
            started.extend(c_far + c_mate + c_peer)

            def to_mate(b):
                c_far[b].start()
                c_mate[b].start()

            def to_peer(b):
                c_far[b].wait_recv()
                send_buf[b] = (part_refs[b][peer].astype(F32) + far_buf[b].astype(F32)).astype(BF16)
                c_peer[b].start()

            def total(b):
                c_mate[b].wait_recv()
                acc = part_refs[b][t].astype(F32) + mate_buf[b].astype(F32)
                c_peer[b].wait_recv()
                return acc + peer_buf[b].astype(F32)
            return to_mate, to_peer, total

        def begin(w, ref, b):
            for cp in loads[w]:
                cp.wait()
            r_s[s_x[w]][...] = sequence(ref, b)

        def produce(w, last):
            half = works[w].count // 2

            @pl.loop(half if last else 0, works[w].count if last else half)
            def _(u):
                works[w].body(u, r_s[s_x[w]], use_in[w], use_out[w])

        def finish(w, dst):
            val = works[w].fin(use_in[w], use_out[w]).astype(BF16)
            for k in range(N_TP):
                dst[k] = val[k * PAD:(k + 1) * PAD]

        started, landed = [], []
        for k, (a, b) in enumerate(zip(i_trade, o_trade)):
            cp = remote(r_in[a], r_out[b], k_trade + k, t, there)
            cp.start()
            started.append(cp)
            landed.append(cp)
        if extra:
            ex = r_out[o_extra]
            ex[0, t] = (row(r_in[i_extra[1]], extra[0]) * r_in[i_extra[0]][extra[1]].astype(F32)).astype(BF16)
            x_peer = remote(ex.at[0, t], ex.at[0, t], k_extra, peer)
            x_mate = remote(ex.at[0, t], ex.at[0, t], k_extra + 1, mate)
            x_peer.start()
            x_mate.start()
            started += [x_peer, x_mate]
            landed.append(x_mate)
        s_y = []
        for k in range(len(swap)):
            src, dst = r_in[i_swap[k]], r_out[o_swap[k]]
            for j in range(2):
                s_y.append(remote(src.at[:, core + 2 * j], dst.at[:, core + 2 * j], k_swap + 4 * k + j, t, there))
                s_y[-1].start()
        started += s_y
        if rs:
            part_refs = [r_in[k] for k in i_parts] + ([r_s[s_part]] if pro else [])
            to_mate, to_peer, total = channel(part_refs, s_bufs, 0)
            to_mate(0)
            if second:
                to_mate2, to_peer2, total2 = channel([r_in[k] for k in i_parts2], s_bufs2, k_second)
                for b in range(N_SEQ):
                    to_mate2(b)
            if pro:
                begin(0, r_in[i_x], 1)
                produce(0, False)
                to_peer(0)
                produce(0, True)
                finish(0, part_refs[1])
                to_mate(1)
                leave(stores[0])
                run(1.0)
                to_peer(1)
                if second:
                    for b in range(N_SEQ):
                        to_peer2(b)
                run(budget[0] - 3.0)
        g_peer, g_mate, g_fwd = [], [], []
        for b in range(N_SEQ) if local_fn else ():
            if rs and b:
                run(budget[1])
            val = local_fn(b, total(b) if rs else None, in_refs, out_refs)
            if ag:
                full[b, t] = val
                g_peer.append(remote(full.at[b, t], full.at[b, t], 3 * N_SEQ + b, peer))
                g_mate.append(remote(full.at[b, t], full.at[b, t], 4 * N_SEQ + b, mate))
                g_peer[b].start()
                g_mate[b].start()
        if second:
            for b in range(N_SEQ):
                local2(b, total2(b), [r_in[k] for k in i_ins2], [r_out[k] for k in o_local2])
        if sums is not None:
            sum_src, sum_dst = [r_s[k] for k in s_sum]
            at = 0
            for k in i_sums:
                n_rows = args[k].shape[0]
                sum_src[0, at:at + n_rows, :] = r_in[k][...]
                at += n_rows
            for k, (line, dev) in enumerate([(here, mate), (here, peer), (there, t)]):
                cp = remote(sum_src.at[k], sum_dst.at[k], k_sum + k, dev, line)
                cp.start()
                if k:
                    run(budget[2])
                cp.wait_recv()
                started.append(cp)
                total = sum_src[k] + sum_dst[k]
                if k < 2:
                    sum_src[k + 1] = total
                else:
                    r_out[o_sums][...] = total
        if extra:
            x_peer.wait_recv()
            x_fwd = remote(ex.at[0, peer], ex.at[0, peer], k_extra + 2, mate)
            x_fwd.start()
            started.append(x_fwd)
            landed.append(x_fwd)
        if ag:
            def forward(b):
                g_peer[b].wait_recv()
                g_fwd.append(remote(full.at[b, peer], full.at[b, peer], 5 * N_SEQ + b, mate))
                g_fwd[b].start()

            run(budget[2])
            forward(0)
            run(1.0)
            if nxt:
                w = int(bool(pro))
                g_mate[0].wait_recv()
                g_fwd[0].wait_recv()
                begin(w, full, 0)
                produce(w, False)
                forward(1)
                produce(w, True)
                finish(w, r_out[o_part])
                leave(stores[w])
            else:
                run(budget[3])
                forward(1)
            started += g_peer + g_mate + g_fwd
            landed += (g_mate + g_fwd) if not nxt else (g_mate[1:] + g_fwd[1:])
        for k in range(len(swap)):
            dst = r_out[o_swap[k]]
            for j in range(2):
                s_y[2 * k + j].wait_recv()
                cp = remote(dst.at[:, core + 2 * j], dst.at[:, core + 2 * j], k_swap + 4 * k + 2 + j, mate)
                cp.start()
                started.append(cp)
                landed.append(cp)
        run(None)
        for cp in landed:
            cp.wait_recv()
        for cp in started:
            cp.wait_send()
        for cp in leaving:
            cp.wait()

    return pl.pallas_call(
        kernel,
        out_shape=outs,
        in_specs=in_specs,
        out_specs=out_specs,
        scratch_shapes=scratch,
        compiler_params=pltpu.CompilerParams(collective_id=cid, has_side_effects=True, vmem_limit_bytes=40 * MIB),
        cost_estimate=pl.CostEstimate(flops=40_000_000, bytes_accessed=4_000_000, transcendentals=0),
        name=f'stage{cid}',
    )(*args)


def row(ref, layer):
    return ref[layer:layer + 1, :]


def row_sum(x):
    return jnp.sum(x, axis=-1, keepdims=True)


def row_mean(x):
    return row_sum(x) / x.shape[-1]


def col_sum(x):
    return jnp.sum(x, axis=0, keepdims=True)


def ln_stats(x):
    x_f32 = x.astype(F32)
    centered = x_f32 - row_mean(x_f32)
    inv_std = lax.rsqrt(row_mean(centered * centered) + NORM_EPS)
    return centered * inv_std, inv_std


def ln_bwd(grad_out, x, gain):
    x_hat, inv_std = ln_stats(x)
    grad_hat = grad_out * gain
    mean_one = row_mean(grad_hat)
    mean_two = row_mean(grad_hat * x_hat)
    return inv_std * (grad_hat - mean_one - x_hat * mean_two), x_hat


def add_rows(rows_ref, b, rows):
    for k, val in enumerate(rows):
        s = col_sum(val)
        rows_ref[k:k + 1, :] = s if b == 0 else rows_ref[k:k + 1, :] + s


def key_valid(seq_len):
    col = lax.broadcasted_iota(jnp.int32, (SEQ, SEQ), 1)
    shard = jnp.zeros_like(col)
    for k in range(1, N_TP):
        shard = shard + (col >= k * PAD).astype(jnp.int32)
    return jnp.logical_and(col - PAD * shard < TOK, col - (PAD - TOK) * shard < seq_len)


def head_probs(q_half, k_pair, valid):
    scores = mm(q_half, k_pair, NT) * 0.125
    scores = jnp.where(valid, scores, NEG_BIG)
    e = jnp.exp(scores - jnp.max(scores, axis=-1, keepdims=True))
    return e / row_sum(e)


def seq_rows(b):
    return pl.ds(b * SEQ if isinstance(b, int) else pl.multiple_of(b * SEQ, SEQ), SEQ)


def pair_cols(pair):
    return pl.ds(pl.multiple_of(pair * LANES, LANES), LANES)


def flat(x):
    return x.reshape(-1, x.shape[-1])


def attn_fwd_unit(rows, pair, x, w_ref, bias, seq_len, qkv_ref, o_ref):
    cols = pair_cols(pair)
    pieces = []
    for c in range(3):
        val = (mm(x, w_ref[c, cols, :], NT) + bias[c:c + 1, cols]).astype(BF16)
        qkv_ref[c, rows, cols] = val
        pieces.append(val)
    q, k, v = pieces
    valid = key_valid(seq_len)
    half = lax.broadcasted_iota(jnp.int32, (SEQ, LANES), 1) // 64
    res = []
    for h in range(2):
        probs = head_probs(jnp.where(half == h, q, jnp.zeros_like(q)), k, valid)
        res.append(mm(probs.astype(BF16), v))
    o_ref[rows, cols] = jnp.where(half == 0, res[0], res[1]).astype(BF16)


def attn_bwd_unit(rows, pair, g, qkv_ref, w_ref, seq_len, dqkv_ref, db_ref):
    cols = pair_cols(pair)
    do = mm(g, w_ref[cols, :], NT).astype(BF16)
    q, k, v = (qkv_ref[c, rows, cols] for c in range(3))
    valid = key_valid(seq_len)
    half = lax.broadcasted_iota(jnp.int32, (SEQ, LANES), 1) // 64
    dq, dk, dv = [], [], []
    for h in range(2):
        probs = head_probs(jnp.where(half == h, q, jnp.zeros_like(q)), k, valid)
        grad_p = mm(jnp.where(half == h, do, jnp.zeros_like(do)), v, NT)
        grad_s = (probs * (grad_p - row_sum(grad_p * probs)) * 0.125).astype(BF16)
        dv.append(mm(probs.astype(BF16), do, TN))
        dq.append(mm(grad_s, k))
        dk.append(mm(grad_s, q, TN))
    for c, pieces in enumerate((dq, dk, dv)):
        val = jnp.where(half == 0, pieces[0], pieces[1])
        dqkv_ref[c, rows, cols] = val.astype(BF16)
        db_ref[c:c + 1, cols] = col_sum(val)


def mlp_up_unit(x, u_ref, bias, cols):
    gate = mm(x, u_ref[0, :, cols]) + bias[0:1, cols]
    lin = mm(x, u_ref[1, :, cols]) + bias[1:2, cols]
    return gate, lin


def mlp_bwd_unit(rows, u, x, g, u_ref, bias, d_ref, hid_ref, gp_ref, gb_ref):
    cols = pl.ds(pl.multiple_of(u * HEADS, HEADS), HEADS)
    gate, lin = mlp_up_unit(x, u_ref, bias, cols)
    grad_hid = mm(g, d_ref[cols, :], NT)
    sig = jax.nn.sigmoid(gate)
    if hid_ref is not None:
        hid_ref[rows, cols] = (gate * sig * lin).astype(BF16)
    grad_gate = grad_hid * lin * sig * (1.0 + gate * (1.0 - sig))
    grad_lin = grad_hid * gate * sig
    for c, val in enumerate((grad_gate, grad_lin)):
        gp_ref[c, rows, cols] = val.astype(BF16)
        gb_ref[c:c + 1, cols] = col_sum(val)


def qkv_shape(rows):
    return sds((3, rows, HEADS), BF16)


def heads_shape(rows):
    return sds((rows, HEADS), BF16)


def hidden_shape(rows):
    return sds((rows, WIDTH), BF16)


def grad_pre_shape(rows):
    return sds((2, rows, WIDTH), BF16)


ALL = pl.ds(0, SEQ)
GRAD_BQ = sds((3, HEADS), F32)
GRAD_BU = sds((2, WIDTH), F32)
BOTH_BQ = sds((N_SEQ, 3, HEADS), F32)


def fill_attn_fwd(layer, normed, wq, bq, lens):
    def body(i, ins, outs):
        n_ref, w_ref, b_ref, vl_ref = ins
        b = i // 2
        attn_fwd_unit(seq_rows(b), i % 2, sequence(n_ref, b), w_ref, b_ref.at[layer], first(vl_ref[b]), *outs)
    return Work([held(normed), load(wq, layer), held(bq), held(lens)], [qkv_shape(ROWS), heads_shape(ROWS)], 4, body, 1.8)


def fill_attn_bwd(layer, qkv, grad, wp, lens):
    def body(i, ins, outs):
        qkv_ref, g_ref, w_ref, vl_ref = ins
        b = i // 2
        attn_bwd_unit(seq_rows(b), i % 2, sequence(g_ref, b), qkv_ref, w_ref, first(vl_ref[b]), outs[0], outs[1].at[b])
    return Work([load(qkv), held(grad), load(wp, layer), held(lens)], [qkv_shape(ROWS), BOTH_BQ], 4, body, 2.0)


def fill_mlp(layer, normed, grads, w_up, b_up, w_down):
    def body(i, ins, outs):
        n_ref, u_ref, b_ref, d_ref = ins[:4]
        n, g = (jnp.concatenate([sequence(ref, b) for ref in refs for b in range(ref.shape[0])], axis=0)
                for refs in ([n_ref], ins[4:]))
        mlp_bwd_unit(pl.ds(0, ROWS), i, n, g, u_ref, b_ref.at[layer], d_ref, *outs[:2], outs[2].at[0])
    return Work([normed, load(w_up, layer), held(b_up), load(w_down, layer)] + [held(g) for g in grads],
                [hidden_shape(ROWS), grad_pre_shape(ROWS), sds((1, 2, WIDTH), F32)], 4, body, 1.6)


def pro_attn_fwd(b, layer, normed, wq, bq, wp, lens):
    def body(u, x, ins, outs):
        w_ref, b_ref, _, vl_ref = ins
        attn_fwd_unit(ALL, u, x[...], w_ref, b_ref.at[layer], first(vl_ref[b]), *outs)

    def fin(ins, outs):
        return mm(outs[1][...], ins[2][...])
    return Work([load(wq, layer), held(bq), load(wp, layer), held(lens)], [qkv_shape(SEQ), heads_shape(SEQ)], 2, body,
                fin=fin, x=normed)


def pro_mlp_fwd(layer, normed, w_up, b_up, w_down):
    def body(u, x, ins, outs):
        u_ref, b_ref, _ = ins
        cols = pl.ds(pl.multiple_of(u * HEADS, HEADS), HEADS)
        gate, lin = mlp_up_unit(x[...], u_ref, b_ref.at[layer], cols)
        outs[0][:, cols] = (jax.nn.silu(gate) * lin).astype(BF16)

    def fin(ins, outs):
        return mm(outs[0][...], ins[2][...])
    return Work([load(w_up, layer), held(b_up), load(w_down, layer)], [hidden_shape(SEQ)], 4, body, fin=fin, x=normed)


def pro_mlp_bwd(b, layer, normed, grad, w_up, b_up, w_down, forward):
    extra = grad if forward else normed

    def body(u, x, ins, outs):
        u_ref, b_ref, d_ref, e_ref = ins
        pair = (x[...], sequence(e_ref, b if e_ref.shape[0] > 1 else 0))
        n, g = pair if forward else pair[::-1]
        mlp_bwd_unit(ALL, u, n, g, u_ref, b_ref.at[layer], d_ref, outs[2] if forward else None, *outs[:2])

    def fin(ins, outs):
        if forward:
            val = mm(outs[2][...], ins[2][...]).astype(BF16)
            for k in range(N_TP):
                outs[3][k] = val[k * PAD:(k + 1) * PAD]
        return sum(mm(outs[0][c], ins[0][c], NT) for c in range(2))
    return Work([load(w_up, layer), held(b_up), load(w_down, layer), extra],
                [grad_pre_shape(SEQ), GRAD_BU] + ([hidden_shape(SEQ), sds((N_TP, PAD, WIDTH), BF16)] if forward else []),
                4, body, fin=fin, x=normed if forward else grad)


def pro_attn_bwd(b, layer, qkv, grad, wp, wq, lens):
    def body(u, x, ins, outs):
        qkv_ref, w_ref, _, vl_ref = ins
        attn_bwd_unit(ALL, u, x[...], qkv_ref, w_ref, first(vl_ref[b]), *outs)

    def fin(ins, outs):
        return sum(mm(outs[0][c], ins[2][c]) for c in range(3))
    return Work([load(qkv), load(wp, layer), load(wq, layer), held(lens)], [qkv_shape(SEQ), GRAD_BQ], 2, body, fin=fin,
                x=grad)


def gather_norm(cid, layer, x, gain, bias, **side):
    def local(b, acc, ins, outs):
        x_ref, g_ref, b_ref = ins
        x_hat, _ = ln_stats(x_ref[b])
        return (x_hat * row(g_ref, layer) + row(b_ref, layer)).astype(BF16)
    return stage_call(cid, local, (x, gain, bias), [], **side)


def residual_norm(cid, layer, x, bias, scale, norm_layer, gain, shift, **side):
    def local(b, acc, ins, outs):
        x_ref, b_ref, s_ref, g_ref, h_ref = ins
        total = acc + row(b_ref, layer)
        outs[1][b] = total
        x_new = (x_ref[b].astype(F32) + row(s_ref, layer) * total).astype(BF16)
        outs[0][b] = x_new
        x_hat, _ = ln_stats(x_new)
        return (x_hat * row(g_ref, norm_layer) + row(h_ref, norm_layer)).astype(BF16)
    return stage_call(cid, local, (x, bias, scale, gain, shift), [sds(x.shape, BF16), sds(x.shape, F32)], **side)


def residual_last(layer, parts, x, bias, scale, grad_y):
    def local(b, acc, ins, outs):
        x_ref, b_ref, s_ref, g_ref = ins
        total = acc + row(b_ref, layer)
        outs[0][b] = (x_ref[b].astype(F32) + row(s_ref, layer) * total).astype(BF16)
        grad = g_ref[b].astype(F32)
        add_rows(outs[1], b, [grad * total, row(s_ref, layer) * grad])
    return parts, local, (x, bias, scale, grad_y), [sds(x.shape, BF16), sds((2, x.shape[-1]), F32)]


def back_mid(cid, layer, x_mid, gain, grad_res, attn_sum, scale, **side):
    def local(b, acc, ins, outs):
        x_ref, g_ref, r_ref, a_ref, s_ref = ins
        grad_in, x_hat = ln_bwd(acc, x_ref[b], row(g_ref, layer))
        grad_mid = r_ref[b].astype(F32) + grad_in
        outs[0][b] = grad_mid
        grad_attn = row(s_ref, layer) * grad_mid
        add_rows(outs[1], b, [acc * x_hat, acc, grad_mid * a_ref[b], grad_attn])
        return grad_attn.astype(BF16)
    return stage_call(cid, local, (x_mid, gain, grad_res, attn_sum, scale),
                      [sds(x_mid.shape, F32), sds((4, x_mid.shape[-1]), F32)], **side)


def back_in(cid, layer, x_in, gain, grad_mid, mlp_sum, scale, **side):
    more = layer > 0

    def local(b, acc, ins, outs):
        x_ref, g_ref, m_ref = ins[:3]
        grad_in, x_hat = ln_bwd(acc, x_ref[b], row(g_ref, layer))
        grad = (m_ref[b] + grad_in).astype(BF16)
        outs[0][b] = grad
        if not more:
            add_rows(outs[1], b, [acc * x_hat, acc])
            return None
        grad = grad.astype(F32)
        grad_mlp = row(ins[4], layer - 1) * grad
        add_rows(outs[1], b, [acc * x_hat, acc])
        add_rows(outs[2], b, [grad * ins[3][b], grad_mlp])
        return grad_mlp.astype(BF16)
    shapes = [sds(x_in.shape, BF16)] + [sds((2, x_in.shape[-1]), F32)] * (2 if more else 1)
    return stage_call(cid, local, (x_in, gain, grad_mid) + ((mlp_sum, scale) if more else ()), shapes, ag=more, **side)


def grads_call(jobs, biases, sums):
    args, bufs, loads = [], [], []
    for job in jobs:
        for arrs in job[2:]:
            at = 0
            for arr in arrs:
                loads.append((len(args), len(bufs), at))
                args.append(arr)
                at += arr.shape[-2]
            wide = arrs[0].shape[0] if job[0] == 2 and arrs[0].ndim > 2 else 1
            lead = arrs[0].shape[:-2] if wide == 1 else ()
            bufs.append(pltpu.VMEM((*lead, at, wide * arrs[0].shape[-1]), BF16))
    n_op = len(args)
    small = [x for group in biases for trio in group for x in trio] + [sums]
    args = [pltpu.with_memory_space_constraint(a, pltpu.HBM) for a in args] + small
    specs = [HBM_SPEC] * n_op + [VMEM_SPEC] * len(small)
    width = sums.shape[-1]
    shapes = [(groups, total, width) for groups, total in ((2, WIDTH), (1, WIDTH), (3, HEADS), (1, HEADS))]
    shapes += [group[0][0].shape for group in biases] + [(width,)] * 8
    outs = [sds((2, *shape), F32) for shape in shapes]
    stage_rows = WIDTH

    def kernel(*refs):
        ops, smalls = refs[:n_op], refs[n_op:len(args)]
        out = refs[len(args):len(args) + len(outs)]
        buf = refs[len(args) + len(outs):]
        stage, lsem, osem = buf[len(bufs):]
        copies = []
        for k, k_buf, at in loads:
            n_rows, n_cols = ops[k].shape[-2:]
            rows, dst = pl.ds(at, n_rows), buf[k_buf]
            if len(ops[k].shape) == len(dst.shape):
                pairs = [(ops[k], dst.at[:, rows] if len(dst.shape) == 3 else dst.at[rows])]
            else:
                pairs = [(ops[k].at[c], dst.at[rows, pl.ds(c * n_cols, n_cols)]) for c in range(ops[k].shape[0])]
            for src, to in pairs:
                copies.append((pltpu.make_async_copy(src, to, lsem.at[len(copies)]), k_buf // 2))

        def fetch(j, act):
            for cp, owner in copies:
                if owner == j:
                    act(cp)

        for j in range(2):
            fetch(j, lambda cp: cp.start())
        for l in range(2):
            for k in range(2):
                own_a, own_b, oth = smalls[6 * k + 3 * l:][:3]
                out[4 + k][l] = sum((oth[b] for b in range(oth.shape[0])), own_a[...] + own_b[...])
        rows = smalls[-1]
        for k in range(8):
            for l, at in enumerate((8 + k, 2 + k if k < 6 else k - 6)):
                out[6 + k][l:l + 1, :] = rows[at:at + 1, :]
        pending = [[]] * 2
        step = 0
        for j, (slot, layer, *_) in enumerate(jobs):
            a_ref, b_ref = buf[2 * j:2 * j + 2]
            fetch(j, lambda cp: cp.wait())
            fetch(j + 2, lambda cp: cp.start())
            total = outs[slot].shape[2]
            split_b = len(b_ref.shape) > 2
            for g in range(b_ref.shape[0] if split_b else 1):
                s = step % 2
                val = mm(a_ref[...], b_ref[g] if split_b else b_ref[...], TN)
                for cp in pending[s]:
                    cp.wait()
                stage[s, :val.shape[0]] = val
                pending[s] = [pltpu.make_async_copy(stage.at[s, pl.ds(k * total, total)], out[slot].at[layer, g + k], osem.at[s, k])
                              for k in range(val.shape[0] // total)]
                for cp in pending[s]:
                    cp.start()
                step += 1
        for cp in pending[0] + pending[1]:
            cp.wait()

    return pl.pallas_call(
        kernel,
        out_shape=outs,
        in_specs=specs,
        out_specs=[HBM_SPEC] * 4 + [VMEM_SPEC] * 10,
        scratch_shapes=bufs + [pltpu.VMEM((2, stage_rows, width), F32), pltpu.SemaphoreType.DMA((2 * n_op,)),
                               pltpu.SemaphoreType.DMA((2, 3))],
        compiler_params=pltpu.CompilerParams(vmem_limit_bytes=60 * MIB),
        cost_estimate=pl.CostEstimate(flops=40_000_000_000, bytes_accessed=80_000_000, transcendentals=0),
        name='grads')(*args)


def device_fn(tokens, grad_y, valid_len, norm1_gain, norm1_bias, w_qkv, b_qkv, w_proj, b_proj, layer_scale1,
              norm2_gain, norm2_bias, w_up, b_up, w_down, b_down, layer_scale2):
    pad = ((0, 0), (0, PAD - TOK), (0, 0))
    x0 = jnp.pad(tokens, pad)
    g_y = jnp.pad(grad_y, pad)
    lens = jnp.broadcast_to(valid_len[:, None, None], (N_SEQ, 8, LANES))
    wq = w_qkv.transpose(0, 1, 3, 4, 2).reshape(2, 3, HEADS, WIDTH)
    bq = b_qkv.reshape(2, 3, HEADS)
    wp = w_proj.reshape(2, HEADS, WIDTH)

    mlp = w_up, b_up, w_down
    ids = itertools.count()
    n1_0, lens_x, part, qkv_0a, o_0a = gather_norm(
        next(ids), 0, x0, norm1_gain, norm1_bias, trade=[lens], nxt=pro_attn_fwd(0, 0, None, wq, bq, wp, lens))
    mid_0, asum_0, n2_0, n1_0x, n1_0h, gm_1a, part, qkv_0b, o_0b, hid_0a = residual_norm(
        next(ids), 0, x0, b_proj, layer_scale1, 0, norm2_gain, norm2_bias, parts=[part],
        pro=pro_attn_fwd(1, 0, n1_0, wq, bq, wp, lens), nxt=pro_mlp_fwd(0, None, *mlp),
        swap=[n1_0], save=[n1_0], extra=(1, 0, g_y, layer_scale2))
    x1, msum_0, n1_1, n2_0x, gm_1ax, n2_0h, n1_0xh, gm_1ah, gm_1b, part, hid_0b, qkv_1a, o_1a, qkv_0x, o_0x = residual_norm(
        next(ids), 0, mid_0, b_down, layer_scale2, 1, norm1_gain, norm1_bias, parts=[part],
        pro=pro_mlp_fwd(0, n2_0, *mlp), nxt=pro_attn_fwd(0, 1, None, wq, bq, wp, lens),
        swap=[n2_0, gm_1a], save=[n2_0, n1_0x, gm_1a], extra=(1, 1, g_y, layer_scale2),
        fills=[fill_attn_fwd(0, n1_0x, wq, bq, lens_x)])
    (mid_1, asum_1, n2_1, n1_1x, gm_1bx, n1_1h, gm_1bh, gm_1axh, n2_0xh, part, qkv_1b, o_1b, gp_1a, gb_1a, hid_1a,
     part_ya) = residual_norm(
        next(ids), 1, x1, b_proj, layer_scale1, 1, norm2_gain, norm2_bias, parts=[part],
        pro=pro_attn_fwd(1, 1, n1_1, wq, bq, wp, lens), nxt=pro_mlp_bwd(0, 1, None, held(gm_1a), *mlp, True),
        swap=[n1_1, gm_1b], save=[n1_1, gm_1b, gm_1ax, n2_0x])

    (gmid_1, rows_mid_1, ga_1, n2_1x, n2_1h, n1_1xh, gm_1bxh, part, gp_1b, gb_1b, hid_1b, part_yb, gq_1a, gbq_1a, qkv_1x,
     o_1x) = back_mid(
        next(ids), 1, mid_1, norm2_gain, g_y, asum_1, layer_scale1, parts=[part],
        pro=pro_mlp_bwd(1, 1, n2_1, held(gm_1b), *mlp, True), nxt=pro_attn_bwd(0, 1, qkv_1a, None, wp, wq, lens),
        swap=[n2_1], save=[n2_1, n1_1x, gm_1bx], fills=[fill_attn_fwd(1, n1_1x, wq, bq, lens_x)])
    (grad_1, rows_in_1, rows_mlp_0, gm_0, ga_1x, ga_1h, n2_1xh, part, gq_1b, gbq_1b, gp_0a, gb_0a, hid_1x, gp_1x,
     gb_1x) = back_in(
        next(ids), 1, x1, norm1_gain, gmid_1, msum_0, layer_scale2, parts=[part],
        pro=pro_attn_bwd(1, 1, qkv_1b, ga_1, wp, wq, lens), nxt=pro_mlp_bwd(0, 0, load(n2_0h), None, *mlp, False),
        swap=[ga_1], save=[ga_1, n2_1x], fills=[fill_mlp(1, held(n2_1x), [gm_1ax, gm_1bx], *mlp)])

    gmid_0, rows_mid_0, ga_0, gm_0x, gm_0h, ga_1xh, part, gp_0b, gb_0b, gq_0a, gbq_0a, gq_1x, gbq_1x = back_mid(
        next(ids), 0, mid_0, norm2_gain, grad_1, asum_0, layer_scale1, parts=[part],
        pro=pro_mlp_bwd(1, 0, load(n2_0h), gm_0, *mlp, False), nxt=pro_attn_bwd(0, 0, qkv_0a, None, wp, wq, lens),
        swap=[gm_0], save=[gm_0, ga_1x], fills=[fill_attn_bwd(1, qkv_1x, ga_1x, wp, lens_x)])
    grad_0, rows_in_0, y_out, rows_mlp_1, ga_0x, ga_0h, gm_0xh, gq_0b, gbq_0b, hid_0x, gp_0x, gb_0x = back_in(
        next(ids), 0, x0, norm1_gain, gmid_0, None, None, parts=[part], pro=pro_attn_bwd(1, 0, qkv_0b, ga_0, wp, wq, lens),
        second=residual_last(1, (part_ya, part_yb), mid_1, b_down, layer_scale2, g_y),
        swap=[ga_0], save=[ga_0, gm_0x], fills=[fill_mlp(0, load(n2_0xh), [gm_0x], *mlp)])
    ga_0xh, sums, gq_0x, gbq_0x = stage_call(
        next(ids), None, [rows_mlp_1], [], ag=False, save=[ga_0x], fills=[fill_attn_bwd(0, qkv_0x, ga_0x, wp, lens_x)],
        sums=(rows_mlp_1, rows_in_1, rows_mid_1, rows_in_0, rows_mid_0, rows_mlp_0))

    operands = (
        ((n2_1h, n2_1xh), (gp_1a, gp_1b, gp_1x), (hid_1a, hid_1b, hid_1x), (gm_1ah, gm_1bh, gm_1axh, gm_1bxh),
         (gq_1a, gq_1b, gq_1x), (n1_1h, n1_1xh), (o_1a, o_1b, o_1x), (ga_1h, ga_1xh)),
        ((n2_0h, n2_0xh), (gp_0a, gp_0b, gp_0x), (hid_0a, hid_0b, hid_0x), (gm_0h, gm_0xh),
         (gq_0a, gq_0b, gq_0x), (n1_0h, n1_0xh), (o_0a, o_0b, o_0x), (ga_0h, ga_0xh)))
    jobs = []
    for k, ops in enumerate(operands):
        ops = [[a if a.ndim < 4 else flat(a) for a in arrs] for arrs in ops]
        jobs += [(slot, 1 - k, *ops[2 * slot:2 * slot + 2]) for slot in reversed(range(4))]
    g_up, g_down, g_qkv, g_proj, g_b_up, g_b_qkv, n1g, n1b, n2g, n2b, ls1, bp, ls2, bd = grads_call(
        jobs, [[(gb_0a, gb_0b, gb_0x), (gb_1a, gb_1b, gb_1x)], [(gbq_0a, gbq_0b, gbq_0x), (gbq_1a, gbq_1b, gbq_1x)]], sums)
    return (y_out[:, :TOK], grad_0[:, :TOK], n1g, n1b,
            g_qkv.reshape(2, 3, 4, 64, WIDTH).transpose(0, 1, 4, 2, 3), g_b_qkv.reshape(2, 3, 4, 64),
            g_proj.reshape(2, 4, 64, WIDTH), bp, ls1, n2g, n2b, g_up, g_b_up,
            g_down.reshape(2, WIDTH, WIDTH), bd, ls2)


def split(axis, ndim):
    return P(*('tp' if k == axis else None for k in range(ndim)))


def solution(mesh):
    rep = P()
    act = P('dp', 'tp', None)
    param_specs = (rep, rep, split(3, 5), split(2, 4), split(1, 4), rep, rep, rep, rep, split(3, 4), split(2, 3), split(1, 3),
                   rep, rep)
    return jax.shard_map(device_fn, mesh=mesh, in_specs=(act, act, P('dp')) + param_specs,
                         out_specs=(act, act) + param_specs, check_vma=False)
```

```python
import itertools

import jax
import jax.numpy as jnp
from jax import lax
from jax.experimental import pallas as pl
from jax.experimental.pallas import tpu as pltpu
from jax.sharding import PartitionSpec as P

NORM_EPS = 1e-6
NEG_BIG = -1e9
F32 = jnp.float32
BF16 = jnp.bfloat16
TOK = 66
PAD = 72
N_TP = 4
N_SEQ = 2
SEQ = N_TP * PAD
ROWS = N_SEQ * SEQ
WIDTH = 1024
HEADS = 256
LANES = 128
MIB = 2 ** 20
MESH_ID = pl.DeviceIdType.MESH
VMEM_SPEC = pl.BlockSpec(memory_space=pltpu.VMEM)
HBM_SPEC = pl.BlockSpec(memory_space=pltpu.HBM)


def sds(shape, dtype):
    return jax.ShapeDtypeStruct(shape, dtype)


def mm(a, b, dims=((1,), (0,))):
    return lax.dot_general(a, b, (dims, ((), ())), preferred_element_type=F32)


NT = ((1,), (1,))
TN = ((0,), (0,))


def load(arr, index=None):
    return arr, True, index


def held(arr):
    return arr, False, None


def first(x):
    return x[:1, :1]


class Work:
    def __init__(self, ins, outs, count, body, cost=1.0, fin=None, x=None):
        self.ins, self.outs, self.count, self.body, self.cost, self.fin, self.x = ins, outs, count, body, cost, fin, x


def sequence(ref, b=0):
    return jnp.concatenate([ref[b, k] for k in range(N_TP)], axis=0)


def stage_call(cid, local_fn, ins, out_shapes, ag=True, parts=(), pro=None, nxt=None, swap=(), save=(), extra=None, trade=(),
               fills=(), sums=None, second=None, budget=(4.5, 2.0, 2.5, 3.0)):
    width = ins[0].shape[-1]
    rs = bool(parts)
    args, in_specs, place = [], [], {}

    def add(arr, spec=VMEM_SPEC, pin=False):
        key = (id(arr), spec is HBM_SPEC)
        if key not in place:
            place[key] = len(args)
            args.append(pltpu.with_memory_space_constraint(arr, pltpu.HBM) if pin else arr)
            in_specs.append(spec)
        return place[key]

    outs, out_specs = [], []

    def add_out(shape, spec=VMEM_SPEC):
        outs.append(pltpu.HBM(shape.shape, shape.dtype) if spec is HBM_SPEC else shape)
        out_specs.append(spec)
        return len(outs) - 1

    scratch = []

    def add_scratch(item):
        scratch.append(item)
        return len(scratch) - 1

    i_parts = [add(a) for a in parts]
    i_x = add(pro.x) if pro else None
    parts2, local2, ins2, shapes2 = second or ((), None, (), ())
    i_parts2 = [add(a) for a in parts2]
    i_ins2 = [add(a) for a in ins2]
    i_ins = [add(a) for a in ins]
    i_swap = [add(a) for a in swap]
    i_save = [add(a) for a in save]
    i_trade = [add(a) for a in trade]
    i_extra = [add(a) for a in extra[2:]] if extra else []
    i_sums = [add(a) for a in sums] if sums is not None else []
    o_local = [add_out(s) for s in out_shapes]
    o_local2 = [add_out(s) for s in shapes2]
    full_shape = sds((N_SEQ, N_TP, PAD, width), BF16)
    o_full = add_out(full_shape) if ag else None
    o_swap = [add_out(sds(a.shape, BF16)) for a in swap]
    o_save = [add_out(sds(a.shape, BF16), HBM_SPEC) for a in save]
    o_trade = [add_out(sds(a.shape, a.dtype)) for a in trade]
    o_extra = add_out(sds((1, N_TP, PAD, width), BF16)) if extra else None
    o_sums = add_out(sds((16, width), F32)) if sums is not None else None
    works = ([pro] if pro else []) + ([nxt] if nxt else []) + list(fills)
    o_part = add_out(sds((N_TP, PAD, width), BF16)) if nxt else None
    s_x = [add_scratch(pltpu.VMEM((SEQ, width), BF16)) for _ in range(2)]
    w_ins, w_outs = [], []
    n_load = n_store = 0
    for work in works:
        got = []
        for arr, copied, index in work.ins:
            if copied:
                k = add_scratch(pltpu.VMEM(arr.shape if index is None else arr.shape[1:], arr.dtype))
                got.append((add(arr, HBM_SPEC, index is None), index, k, n_load))
                n_load += 1
            else:
                got.append((add(arr), None, None, None))
        w_ins.append(got)
        kept = []
        for shape in work.outs:
            if shape.dtype == BF16:
                kept.append((add_out(shape, HBM_SPEC), add_scratch(pltpu.VMEM(shape.shape, shape.dtype)), n_store))
                n_store += 1
            else:
                kept.append((add_out(shape), None, None))
        w_outs.append(kept)
    shard = pltpu.VMEM((N_SEQ, PAD, width), BF16)
    s_bufs2 = [add_scratch(shard) for _ in range(4)] if second else []
    if rs:
        s_bufs = [add_scratch(shard) for _ in range(4)]
        s_part = add_scratch(pltpu.VMEM((N_TP, PAD, width), BF16)) if pro else None
    k_swap = 6 * N_SEQ
    k_extra = k_swap + 4 * len(swap)
    k_sum = k_extra + 3
    k_trade = k_sum + 3
    k_second = k_trade + len(trade)
    n_sem = k_second + 3 * N_SEQ * bool(second)
    s_send, s_recv = [add_scratch(pltpu.SemaphoreType.DMA((n_sem,))) for _ in range(2)]
    s_load = add_scratch(pltpu.SemaphoreType.DMA((n_load + n_store + len(save) + 1,)))
    if sums is not None:
        s_sum = [add_scratch(pltpu.VMEM((3, 16, width), F32)) for _ in range(2)]
    n_in, n_out = len(args), len(outs)

    def kernel(*refs):
        r_in, r_out, r_s = refs[:n_in], refs[n_in:n_in + n_out], refs[n_in + n_out:]
        in_refs = [r_in[k] for k in i_ins]
        out_refs = [r_out[k] for k in o_local]
        full = r_out[o_full] if ag else None
        ssem, rsem, lsem = r_s[s_send], r_s[s_recv], r_s[s_load]
        loads, use_in, use_out, stores, leaving = [], [], [], [], []
        for got, kept in zip(w_ins, w_outs):
            cps, use = [], []
            for k_in, index, k_buf, k_sem in got:
                if k_buf is None:
                    use.append(r_in[k_in])
                    continue
                src = r_in[k_in] if index is None else r_in[k_in].at[index]
                cps.append(pltpu.make_async_copy(src, r_s[k_buf], lsem.at[k_sem]))
                cps[-1].start()
                use.append(r_s[k_buf])
            loads.append(cps)
            use_in.append(use)
            use_out.append([r_out[k] if k_buf is None else r_s[k_buf] for k, k_buf, _ in kept])
            stores.append([pltpu.make_async_copy(r_s[k_buf], r_out[k], lsem.at[n_load + k_sem])
                           for k, k_buf, k_sem in kept if k_buf is not None])
        dp = lax.axis_index('dp')
        t = lax.axis_index('tp')
        core = lax.rem(t, 2)
        mate = t + 1 - 2 * core
        peer = lax.rem(t + 2, N_TP)
        far = lax.rem(mate + 2, N_TP)
        here, there = dp, 1 - dp

        def remote(src, dst, k, dev, line=None):
            return pltpu.make_async_remote_copy(src_ref=src, dst_ref=dst, send_sem=ssem.at[k], recv_sem=rsem.at[k],
                                                device_id=(here if line is None else line, dev), device_id_type=MESH_ID)

        def leave(cps):
            for cp in cps:
                cp.start()
            leaving.extend(cps)

        leave([pltpu.make_async_copy(r_in[a], r_out[b], lsem.at[n_load + n_store + k])
               for k, (a, b) in enumerate(zip(i_save, o_save))])
        barrier = pltpu.get_barrier_semaphore()
        peers = [(here, mate), (here, peer)]
        if swap or trade or sums is not None:
            peers.append((there, t))
        for dev in peers:
            pl.semaphore_signal(barrier, inc=1, device_id=dev, device_id_type=MESH_ID)
        pl.semaphore_wait(barrier, len(peers))

        first = bool(pro) + bool(nxt)
        done = [0] * len(works)

        def run(time):
            for f in range(first, len(works)):
                work = works[f]
                left = work.count - done[f]
                n = left if time is None else min(left, int(time / work.cost + 0.5))
                if n <= 0:
                    continue
                if done[f] == 0:
                    for cp in loads[f]:
                        cp.wait()
                lo = done[f]
                done[f] = hi = lo + n
                if n == 1:
                    work.body(lo, use_in[f], use_out[f])
                else:
                    @pl.loop(lo, hi)
                    def _(i, work=work, f=f):
                        work.body(i, use_in[f], use_out[f])
                if hi == work.count:
                    leave(stores[f])
                if time is not None:
                    time -= n * work.cost

        def channel(part_refs, bufs, k0):
            far_buf, mate_buf, peer_buf, send_buf = [r_s[k] for k in bufs]
            c_far = [remote(part_refs[b].at[far], far_buf.at[b], k0 + b, mate) for b in range(N_SEQ)]
            c_mate = [remote(part_refs[b].at[mate], mate_buf.at[b], k0 + N_SEQ + b, mate) for b in range(N_SEQ)]
            c_peer = [remote(send_buf.at[b], peer_buf.at[b], k0 + 2 * N_SEQ + b, peer) for b in range(N_SEQ)]
            started.extend(c_far + c_mate + c_peer)

            def to_mate(b):
                c_far[b].start()
                c_mate[b].start()

            def to_peer(b):
                c_far[b].wait_recv()
                send_buf[b] = (part_refs[b][peer].astype(F32) + far_buf[b].astype(F32)).astype(BF16)
                c_peer[b].start()

            def total(b):
                c_mate[b].wait_recv()
                acc = part_refs[b][t].astype(F32) + mate_buf[b].astype(F32)
                c_peer[b].wait_recv()
                return acc + peer_buf[b].astype(F32)
            return to_mate, to_peer, total

        def begin(w, ref, b):
            for cp in loads[w]:
                cp.wait()
            r_s[s_x[w]][...] = sequence(ref, b)

        def produce(w, last):
            half = works[w].count // 2

            @pl.loop(half if last else 0, works[w].count if last else half)
            def _(u):
                works[w].body(u, r_s[s_x[w]], use_in[w], use_out[w])

        def finish(w, dst):
            val = works[w].fin(use_in[w], use_out[w]).astype(BF16)
            for k in range(N_TP):
                dst[k] = val[k * PAD:(k + 1) * PAD]

        started, landed = [], []
        for k, (a, b) in enumerate(zip(i_trade, o_trade)):
            cp = remote(r_in[a], r_out[b], k_trade + k, t, there)
            cp.start()
            started.append(cp)
            landed.append(cp)
        if extra:
            ex = r_out[o_extra]
            ex[0, t] = (row(r_in[i_extra[1]], extra[0]) * r_in[i_extra[0]][extra[1]].astype(F32)).astype(BF16)
            x_peer = remote(ex.at[0, t], ex.at[0, t], k_extra, peer)
            x_mate = remote(ex.at[0, t], ex.at[0, t], k_extra + 1, mate)
            x_peer.start()
            x_mate.start()
            started += [x_peer, x_mate]
            landed.append(x_mate)
        s_y = []
        for k in range(len(swap)):
            src, dst = r_in[i_swap[k]], r_out[o_swap[k]]
            for j in range(2):
                s_y.append(remote(src.at[:, core + 2 * j], dst.at[:, core + 2 * j], k_swap + 4 * k + j, t, there))
                s_y[-1].start()
        started += s_y
        if rs:
            part_refs = [r_in[k] for k in i_parts] + ([r_s[s_part]] if pro else [])
            to_mate, to_peer, total = channel(part_refs, s_bufs, 0)
            to_mate(0)
            if second:
                to_mate2, to_peer2, total2 = channel([r_in[k] for k in i_parts2], s_bufs2, k_second)
                for b in range(N_SEQ):
                    to_mate2(b)
            if pro:
                begin(0, r_in[i_x], 1)
                produce(0, False)
                to_peer(0)
                produce(0, True)
                finish(0, part_refs[1])
                to_mate(1)
                leave(stores[0])
                run(1.0)
                to_peer(1)
                if second:
                    for b in range(N_SEQ):
                        to_peer2(b)
                run(budget[0] - 3.0)
        g_peer, g_mate, g_fwd = [], [], []
        for b in range(N_SEQ) if local_fn else ():
            if rs and b:
                run(budget[1])
            val = local_fn(b, total(b) if rs else None, in_refs, out_refs)
            if ag:
                full[b, t] = val
                g_peer.append(remote(full.at[b, t], full.at[b, t], 3 * N_SEQ + b, peer))
                g_mate.append(remote(full.at[b, t], full.at[b, t], 4 * N_SEQ + b, mate))
                g_peer[b].start()
                g_mate[b].start()
        if second:
            for b in range(N_SEQ):
                local2(b, total2(b), [r_in[k] for k in i_ins2], [r_out[k] for k in o_local2])
        if sums is not None:
            sum_src, sum_dst = [r_s[k] for k in s_sum]
            at = 0
            for k in i_sums:
                n_rows = args[k].shape[0]
                sum_src[0, at:at + n_rows, :] = r_in[k][...]
                at += n_rows
            for k, (line, dev) in enumerate([(here, mate), (here, peer), (there, t)]):
                cp = remote(sum_src.at[k], sum_dst.at[k], k_sum + k, dev, line)
                cp.start()
                if k:
                    run(budget[2])
                cp.wait_recv()
                started.append(cp)
                total = sum_src[k] + sum_dst[k]
                if k < 2:
                    sum_src[k + 1] = total
                else:
                    r_out[o_sums][...] = total
        if extra:
            x_peer.wait_recv()
            x_fwd = remote(ex.at[0, peer], ex.at[0, peer], k_extra + 2, mate)
            x_fwd.start()
            started.append(x_fwd)
            landed.append(x_fwd)
        if ag:
            def forward(b):
                g_peer[b].wait_recv()
                g_fwd.append(remote(full.at[b, peer], full.at[b, peer], 5 * N_SEQ + b, mate))
                g_fwd[b].start()

            run(budget[2])
            forward(0)
            run(1.0)
            if nxt:
                w = int(bool(pro))
                g_mate[0].wait_recv()
                g_fwd[0].wait_recv()
                begin(w, full, 0)
                produce(w, False)
                forward(1)
                produce(w, True)
                finish(w, r_out[o_part])
                leave(stores[w])
            else:
                run(budget[3])
                forward(1)
            started += g_peer + g_mate + g_fwd
            landed += (g_mate + g_fwd) if not nxt else (g_mate[1:] + g_fwd[1:])
        for k in range(len(swap)):
            dst = r_out[o_swap[k]]
            for j in range(2):
                s_y[2 * k + j].wait_recv()
                cp = remote(dst.at[:, core + 2 * j], dst.at[:, core + 2 * j], k_swap + 4 * k + 2 + j, mate)
                cp.start()
                started.append(cp)
                landed.append(cp)
        run(None)
        for cp in landed:
            cp.wait_recv()
        for cp in started:
            cp.wait_send()
        for cp in leaving:
            cp.wait()

    return pl.pallas_call(
        kernel,
        out_shape=outs,
        in_specs=in_specs,
        out_specs=out_specs,
        scratch_shapes=scratch,
        compiler_params=pltpu.CompilerParams(collective_id=cid, has_side_effects=True, vmem_limit_bytes=40 * MIB),
        cost_estimate=pl.CostEstimate(flops=40_000_000, bytes_accessed=4_000_000, transcendentals=0),
        name=f'stage{cid}',
    )(*args)


def row(ref, layer):
    return ref[layer:layer + 1, :]


def row_sum(x):
    return jnp.sum(x, axis=-1, keepdims=True)


def row_mean(x):
    return row_sum(x) / x.shape[-1]


def col_sum(x):
    return jnp.sum(x, axis=0, keepdims=True)


def ln_stats(x):
    x_f32 = x.astype(F32)
    centered = x_f32 - row_mean(x_f32)
    inv_std = lax.rsqrt(row_mean(centered * centered) + NORM_EPS)
    return centered * inv_std, inv_std


def ln_bwd(grad_out, x, gain):
    x_hat, inv_std = ln_stats(x)
    grad_hat = grad_out * gain
    mean_one = row_mean(grad_hat)
    mean_two = row_mean(grad_hat * x_hat)
    return inv_std * (grad_hat - mean_one - x_hat * mean_two), x_hat


def add_rows(rows_ref, b, rows):
    for k, val in enumerate(rows):
        s = col_sum(val)
        rows_ref[k:k + 1, :] = s if b == 0 else rows_ref[k:k + 1, :] + s


def key_valid(seq_len):
    col = lax.broadcasted_iota(jnp.int32, (SEQ, SEQ), 1)
    shard = jnp.zeros_like(col)
    for k in range(1, N_TP):
        shard = shard + (col >= k * PAD).astype(jnp.int32)
    return jnp.logical_and(col - PAD * shard < TOK, col - (PAD - TOK) * shard < seq_len)


def head_probs(q_half, k_pair, valid):
    scores = mm(q_half, k_pair, NT) * 0.125
    scores = jnp.where(valid, scores, NEG_BIG)
    e = jnp.exp(scores - jnp.max(scores, axis=-1, keepdims=True))
    return e / row_sum(e)


def seq_rows(b):
    return pl.ds(b * SEQ if isinstance(b, int) else pl.multiple_of(b * SEQ, SEQ), SEQ)


def pair_cols(pair):
    return pl.ds(pl.multiple_of(pair * LANES, LANES), LANES)


def flat(x):
    return x.reshape(-1, x.shape[-1])


def attn_fwd_unit(rows, pair, x, w_ref, bias, seq_len, qkv_ref, o_ref):
    cols = pair_cols(pair)
    pieces = []
    for c in range(3):
        val = (mm(x, w_ref[c, cols, :], NT) + bias[c:c + 1, cols]).astype(BF16)
        qkv_ref[c, rows, cols] = val
        pieces.append(val)
    q, k, v = pieces
    valid = key_valid(seq_len)
    half = lax.broadcasted_iota(jnp.int32, (SEQ, LANES), 1) // 64
    res = []
    for h in range(2):
        probs = head_probs(jnp.where(half == h, q, jnp.zeros_like(q)), k, valid)
        res.append(mm(probs.astype(BF16), v))
    o_ref[rows, cols] = jnp.where(half == 0, res[0], res[1]).astype(BF16)


def attn_bwd_unit(rows, pair, g, qkv_ref, w_ref, seq_len, dqkv_ref, db_ref):
    cols = pair_cols(pair)
    do = mm(g, w_ref[cols, :], NT).astype(BF16)
    q, k, v = (qkv_ref[c, rows, cols] for c in range(3))
    valid = key_valid(seq_len)
    half = lax.broadcasted_iota(jnp.int32, (SEQ, LANES), 1) // 64
    dq, dk, dv = [], [], []
    for h in range(2):
        probs = head_probs(jnp.where(half == h, q, jnp.zeros_like(q)), k, valid)
        grad_p = mm(jnp.where(half == h, do, jnp.zeros_like(do)), v, NT)
        grad_s = (probs * (grad_p - row_sum(grad_p * probs)) * 0.125).astype(BF16)
        dv.append(mm(probs.astype(BF16), do, TN))
        dq.append(mm(grad_s, k))
        dk.append(mm(grad_s, q, TN))
    for c, pieces in enumerate((dq, dk, dv)):
        val = jnp.where(half == 0, pieces[0], pieces[1])
        dqkv_ref[c, rows, cols] = val.astype(BF16)
        db_ref[c:c + 1, cols] = col_sum(val)


def mlp_up_unit(x, u_ref, bias, cols):
    gate = mm(x, u_ref[0, :, cols]) + bias[0:1, cols]
    lin = mm(x, u_ref[1, :, cols]) + bias[1:2, cols]
    return gate, lin


def mlp_bwd_unit(rows, u, x, g, u_ref, bias, d_ref, hid_ref, gp_ref, gb_ref):
    cols = pl.ds(pl.multiple_of(u * HEADS, HEADS), HEADS)
    gate, lin = mlp_up_unit(x, u_ref, bias, cols)
    grad_hid = mm(g, d_ref[cols, :], NT)
    sig = jax.nn.sigmoid(gate)
    if hid_ref is not None:
        hid_ref[rows, cols] = (gate * sig * lin).astype(BF16)
    grad_gate = grad_hid * lin * sig * (1.0 + gate * (1.0 - sig))
    grad_lin = grad_hid * gate * sig
    for c, val in enumerate((grad_gate, grad_lin)):
        gp_ref[c, rows, cols] = val.astype(BF16)
        gb_ref[c:c + 1, cols] = col_sum(val)


def qkv_shape(rows):
    return sds((3, rows, HEADS), BF16)


def heads_shape(rows):
    return sds((rows, HEADS), BF16)


def hidden_shape(rows):
    return sds((rows, WIDTH), BF16)


def grad_pre_shape(rows):
    return sds((2, rows, WIDTH), BF16)


ALL = pl.ds(0, SEQ)
GRAD_BQ = sds((3, HEADS), F32)
GRAD_BU = sds((2, WIDTH), F32)
BOTH_BQ = sds((N_SEQ, 3, HEADS), F32)


def fill_attn_fwd(layer, normed, wq, bq, lens):
    def body(i, ins, outs):
        n_ref, w_ref, b_ref, vl_ref = ins
        b = i // 2
        attn_fwd_unit(seq_rows(b), i % 2, sequence(n_ref, b), w_ref, b_ref.at[layer], first(vl_ref[b]), *outs)
    return Work([held(normed), load(wq, layer), held(bq), held(lens)], [qkv_shape(ROWS), heads_shape(ROWS)], 4, body, 1.8)


def fill_attn_bwd(layer, qkv, grad, wp, lens):
    def body(i, ins, outs):
        qkv_ref, g_ref, w_ref, vl_ref = ins
        b = i // 2
        attn_bwd_unit(seq_rows(b), i % 2, sequence(g_ref, b), qkv_ref, w_ref, first(vl_ref[b]), outs[0], outs[1].at[b])
    return Work([load(qkv), held(grad), load(wp, layer), held(lens)], [qkv_shape(ROWS), BOTH_BQ], 4, body, 2.0)


def fill_mlp(layer, normed, grads, w_up, b_up, w_down):
    def body(i, ins, outs):
        n_ref, u_ref, b_ref, d_ref = ins[:4]
        n, g = (jnp.concatenate([sequence(ref, b) for ref in refs for b in range(ref.shape[0])], axis=0)
                for refs in ([n_ref], ins[4:]))
        mlp_bwd_unit(pl.ds(0, ROWS), i, n, g, u_ref, b_ref.at[layer], d_ref, *outs[:2], outs[2].at[0])
    return Work([normed, load(w_up, layer), held(b_up), load(w_down, layer)] + [held(g) for g in grads],
                [hidden_shape(ROWS), grad_pre_shape(ROWS), sds((1, 2, WIDTH), F32)], 4, body, 1.6)


def pro_attn_fwd(b, layer, normed, wq, bq, wp, lens):
    def body(u, x, ins, outs):
        w_ref, b_ref, _, vl_ref = ins
        attn_fwd_unit(ALL, u, x[...], w_ref, b_ref.at[layer], first(vl_ref[b]), *outs)

    def fin(ins, outs):
        return mm(outs[1][...], ins[2][...])
    return Work([load(wq, layer), held(bq), load(wp, layer), held(lens)], [qkv_shape(SEQ), heads_shape(SEQ)], 2, body,
                fin=fin, x=normed)


def pro_mlp_fwd(layer, normed, w_up, b_up, w_down):
    def body(u, x, ins, outs):
        u_ref, b_ref, _ = ins
        cols = pl.ds(pl.multiple_of(u * HEADS, HEADS), HEADS)
        gate, lin = mlp_up_unit(x[...], u_ref, b_ref.at[layer], cols)
        outs[0][:, cols] = (jax.nn.silu(gate) * lin).astype(BF16)

    def fin(ins, outs):
        return mm(outs[0][...], ins[2][...])
    return Work([load(w_up, layer), held(b_up), load(w_down, layer)], [hidden_shape(SEQ)], 4, body, fin=fin, x=normed)


def pro_mlp_bwd(b, layer, normed, grad, w_up, b_up, w_down, forward):
    extra = grad if forward else normed

    def body(u, x, ins, outs):
        u_ref, b_ref, d_ref, e_ref = ins
        pair = (x[...], sequence(e_ref, b if e_ref.shape[0] > 1 else 0))
        n, g = pair if forward else pair[::-1]
        mlp_bwd_unit(ALL, u, n, g, u_ref, b_ref.at[layer], d_ref, outs[2] if forward else None, *outs[:2])

    def fin(ins, outs):
        if forward:
            val = mm(outs[2][...], ins[2][...]).astype(BF16)
            for k in range(N_TP):
                outs[3][k] = val[k * PAD:(k + 1) * PAD]
        return sum(mm(outs[0][c], ins[0][c], NT) for c in range(2))
    return Work([load(w_up, layer), held(b_up), load(w_down, layer), extra],
                [grad_pre_shape(SEQ), GRAD_BU] + ([hidden_shape(SEQ), sds((N_TP, PAD, WIDTH), BF16)] if forward else []),
                4, body, fin=fin, x=normed if forward else grad)


def pro_attn_bwd(b, layer, qkv, grad, wp, wq, lens):
    def body(u, x, ins, outs):
        qkv_ref, w_ref, _, vl_ref = ins
        attn_bwd_unit(ALL, u, x[...], qkv_ref, w_ref, first(vl_ref[b]), *outs)

    def fin(ins, outs):
        return sum(mm(outs[0][c], ins[2][c]) for c in range(3))
    return Work([load(qkv), load(wp, layer), load(wq, layer), held(lens)], [qkv_shape(SEQ), GRAD_BQ], 2, body, fin=fin,
                x=grad)


def gather_norm(cid, layer, x, gain, bias, **side):
    def local(b, acc, ins, outs):
        x_ref, g_ref, b_ref = ins
        x_hat, _ = ln_stats(x_ref[b])
        return (x_hat * row(g_ref, layer) + row(b_ref, layer)).astype(BF16)
    return stage_call(cid, local, (x, gain, bias), [], **side)


def residual_norm(cid, layer, x, bias, scale, norm_layer, gain, shift, **side):
    def local(b, acc, ins, outs):
        x_ref, b_ref, s_ref, g_ref, h_ref = ins
        total = acc + row(b_ref, layer)
        outs[1][b] = total
        x_new = (x_ref[b].astype(F32) + row(s_ref, layer) * total).astype(BF16)
        outs[0][b] = x_new
        x_hat, _ = ln_stats(x_new)
        return (x_hat * row(g_ref, norm_layer) + row(h_ref, norm_layer)).astype(BF16)
    return stage_call(cid, local, (x, bias, scale, gain, shift), [sds(x.shape, BF16), sds(x.shape, F32)], **side)


def residual_last(layer, parts, x, bias, scale, grad_y):
    def local(b, acc, ins, outs):
        x_ref, b_ref, s_ref, g_ref = ins
        total = acc + row(b_ref, layer)
        outs[0][b] = (x_ref[b].astype(F32) + row(s_ref, layer) * total).astype(BF16)
        grad = g_ref[b].astype(F32)
        add_rows(outs[1], b, [grad * total, row(s_ref, layer) * grad])
    return parts, local, (x, bias, scale, grad_y), [sds(x.shape, BF16), sds((2, x.shape[-1]), F32)]


def back_mid(cid, layer, x_mid, gain, grad_res, attn_sum, scale, **side):
    def local(b, acc, ins, outs):
        x_ref, g_ref, r_ref, a_ref, s_ref = ins
        grad_in, x_hat = ln_bwd(acc, x_ref[b], row(g_ref, layer))
        grad_mid = r_ref[b].astype(F32) + grad_in
        outs[0][b] = grad_mid
        grad_attn = row(s_ref, layer) * grad_mid
        add_rows(outs[1], b, [acc * x_hat, acc, grad_mid * a_ref[b], grad_attn])
        return grad_attn.astype(BF16)
    return stage_call(cid, local, (x_mid, gain, grad_res, attn_sum, scale),
                      [sds(x_mid.shape, F32), sds((4, x_mid.shape[-1]), F32)], **side)


def back_in(cid, layer, x_in, gain, grad_mid, mlp_sum, scale, **side):
    more = layer > 0

    def local(b, acc, ins, outs):
        x_ref, g_ref, m_ref = ins[:3]
        grad_in, x_hat = ln_bwd(acc, x_ref[b], row(g_ref, layer))
        grad = (m_ref[b] + grad_in).astype(BF16)
        outs[0][b] = grad
        if not more:
            add_rows(outs[1], b, [acc * x_hat, acc])
            return None
        grad = grad.astype(F32)
        grad_mlp = row(ins[4], layer - 1) * grad
        add_rows(outs[1], b, [acc * x_hat, acc])
        add_rows(outs[2], b, [grad * ins[3][b], grad_mlp])
        return grad_mlp.astype(BF16)
    shapes = [sds(x_in.shape, BF16)] + [sds((2, x_in.shape[-1]), F32)] * (2 if more else 1)
    return stage_call(cid, local, (x_in, gain, grad_mid) + ((mlp_sum, scale) if more else ()), shapes, ag=more, **side)


def grads_call(jobs, biases, sums):
    args, bufs, loads = [], [], []
    for job in jobs:
        for arrs in job[2:]:
            at = 0
            for arr in arrs:
                loads.append((len(args), len(bufs), at))
                args.append(arr)
                at += arr.shape[-2]
            wide = arrs[0].shape[0] if job[0] == 2 and arrs[0].ndim > 2 else 1
            lead = arrs[0].shape[:-2] if wide == 1 else ()
            bufs.append(pltpu.VMEM((*lead, at, wide * arrs[0].shape[-1]), BF16))
    n_op = len(args)
    small = [x for group in biases for trio in group for x in trio] + [sums]
    args = [pltpu.with_memory_space_constraint(a, pltpu.HBM) for a in args] + small
    specs = [HBM_SPEC] * n_op + [VMEM_SPEC] * len(small)
    width = sums.shape[-1]
    shapes = [(groups, total, width) for groups, total in ((2, WIDTH), (1, WIDTH), (3, HEADS), (1, HEADS))]
    shapes += [biases[0][0][0].shape, (3, N_TP, HEADS // N_TP)] + [(width,)] * 8
    outs = [sds((2, *shape), F32) for shape in shapes]
    stage_rows = WIDTH

    def kernel(*refs):
        ops, smalls = refs[:n_op], refs[n_op:len(args)]
        out = refs[len(args):len(args) + len(outs)]
        buf = refs[len(args) + len(outs):]
        stage, lsem, osem = buf[len(bufs):]
        copies = []
        for k, k_buf, at in loads:
            n_rows, n_cols = ops[k].shape[-2:]
            rows, dst = pl.ds(at, n_rows), buf[k_buf]
            if len(ops[k].shape) == len(dst.shape):
                pairs = [(ops[k], dst.at[:, rows] if len(dst.shape) == 3 else dst.at[rows])]
            else:
                pairs = [(ops[k].at[c], dst.at[rows, pl.ds(c * n_cols, n_cols)]) for c in range(ops[k].shape[0])]
            for src, to in pairs:
                copies.append((pltpu.make_async_copy(src, to, lsem.at[len(copies)]), k_buf // 2))

        def fetch(j, act):
            for cp, owner in copies:
                if owner == j:
                    act(cp)

        for j in range(2):
            fetch(j, lambda cp: cp.start())
        for l in range(2):
            for k in range(2):
                own_a, own_b, oth = smalls[6 * k + 3 * l:][:3]
                val = sum((oth[b] for b in range(oth.shape[0])), own_a[...] + own_b[...])
                if k:
                    n = out[5].shape[-1]
                    for h in range(N_TP):
                        out[5][l, :, h, :] = val[:, h * n:(h + 1) * n]
                else:
                    out[4][l] = val
        rows = smalls[-1]
        for k in range(8):
            for l, at in enumerate((8 + k, 2 + k if k < 6 else k - 6)):
                out[6 + k][l:l + 1, :] = rows[at:at + 1, :]
        pending = [[]] * 2
        step = 0
        for j, (slot, layer, *_) in enumerate(jobs):
            a_ref, b_ref = buf[2 * j:2 * j + 2]
            fetch(j, lambda cp: cp.wait())
            fetch(j + 2, lambda cp: cp.start())
            total = outs[slot].shape[2]
            split_b = len(b_ref.shape) > 2
            for g in range(b_ref.shape[0] if split_b else 1):
                s = step % 2
                val = mm(a_ref[...], b_ref[g] if split_b else b_ref[...], TN)
                for cp in pending[s]:
                    cp.wait()
                stage[s, :val.shape[0]] = val
                pending[s] = [pltpu.make_async_copy(stage.at[s, pl.ds(k * total, total)], out[slot].at[layer, g + k], osem.at[s, k])
                              for k in range(val.shape[0] // total)]
                for cp in pending[s]:
                    cp.start()
                step += 1
        for cp in pending[0] + pending[1]:
            cp.wait()

    return pl.pallas_call(
        kernel,
        out_shape=outs,
        in_specs=specs,
        out_specs=[HBM_SPEC] * 4 + [VMEM_SPEC] * 10,
        scratch_shapes=bufs + [pltpu.VMEM((2, stage_rows, width), F32), pltpu.SemaphoreType.DMA((2 * n_op,)),
                               pltpu.SemaphoreType.DMA((2, 3))],
        compiler_params=pltpu.CompilerParams(vmem_limit_bytes=60 * MIB),
        cost_estimate=pl.CostEstimate(flops=40_000_000_000, bytes_accessed=80_000_000, transcendentals=0),
        name='grads')(*args)


def device_fn(tokens, grad_y, valid_len, norm1_gain, norm1_bias, w_qkv, b_qkv, w_proj, b_proj, layer_scale1,
              norm2_gain, norm2_bias, w_up, b_up, w_down, b_down, layer_scale2):
    pad = ((0, 0), (0, PAD - TOK), (0, 0))
    x0 = jnp.pad(tokens, pad)
    g_y = jnp.pad(grad_y, pad)
    lens = jnp.broadcast_to(valid_len[:, None, None], (N_SEQ, 8, LANES))
    wq = w_qkv.transpose(0, 1, 3, 4, 2).reshape(2, 3, HEADS, WIDTH)
    bq = b_qkv.reshape(2, 3, HEADS)
    wp = w_proj.reshape(2, HEADS, WIDTH)

    mlp = w_up, b_up, w_down
    ids = itertools.count()
    n1_0, lens_x, part, qkv_0a, o_0a = gather_norm(
        next(ids), 0, x0, norm1_gain, norm1_bias, trade=[lens], nxt=pro_attn_fwd(0, 0, None, wq, bq, wp, lens))
    mid_0, asum_0, n2_0, n1_0x, n1_0h, gm_1a, part, qkv_0b, o_0b, hid_0a = residual_norm(
        next(ids), 0, x0, b_proj, layer_scale1, 0, norm2_gain, norm2_bias, parts=[part],
        pro=pro_attn_fwd(1, 0, n1_0, wq, bq, wp, lens), nxt=pro_mlp_fwd(0, None, *mlp),
        swap=[n1_0], save=[n1_0], extra=(1, 0, g_y, layer_scale2))
    x1, msum_0, n1_1, n2_0x, gm_1ax, n2_0h, n1_0xh, gm_1ah, gm_1b, part, hid_0b, qkv_1a, o_1a, qkv_0x, o_0x = residual_norm(
        next(ids), 0, mid_0, b_down, layer_scale2, 1, norm1_gain, norm1_bias, parts=[part],
        pro=pro_mlp_fwd(0, n2_0, *mlp), nxt=pro_attn_fwd(0, 1, None, wq, bq, wp, lens),
        swap=[n2_0, gm_1a], save=[n2_0, n1_0x, gm_1a], extra=(1, 1, g_y, layer_scale2),
        fills=[fill_attn_fwd(0, n1_0x, wq, bq, lens_x)])
    (mid_1, asum_1, n2_1, n1_1x, gm_1bx, n1_1h, gm_1bh, gm_1axh, n2_0xh, part, qkv_1b, o_1b, gp_1a, gb_1a, hid_1a,
     part_ya) = residual_norm(
        next(ids), 1, x1, b_proj, layer_scale1, 1, norm2_gain, norm2_bias, parts=[part],
        pro=pro_attn_fwd(1, 1, n1_1, wq, bq, wp, lens), nxt=pro_mlp_bwd(0, 1, None, held(gm_1a), *mlp, True),
        swap=[n1_1, gm_1b], save=[n1_1, gm_1b, gm_1ax, n2_0x])

    (gmid_1, rows_mid_1, ga_1, n2_1x, n2_1h, n1_1xh, gm_1bxh, part, gp_1b, gb_1b, hid_1b, part_yb, gq_1a, gbq_1a, qkv_1x,
     o_1x) = back_mid(
        next(ids), 1, mid_1, norm2_gain, g_y, asum_1, layer_scale1, parts=[part],
        pro=pro_mlp_bwd(1, 1, n2_1, held(gm_1b), *mlp, True), nxt=pro_attn_bwd(0, 1, qkv_1a, None, wp, wq, lens),
        swap=[n2_1], save=[n2_1, n1_1x, gm_1bx], fills=[fill_attn_fwd(1, n1_1x, wq, bq, lens_x)])
    (grad_1, rows_in_1, rows_mlp_0, gm_0, ga_1x, ga_1h, n2_1xh, part, gq_1b, gbq_1b, gp_0a, gb_0a, hid_1x, gp_1x,
     gb_1x) = back_in(
        next(ids), 1, x1, norm1_gain, gmid_1, msum_0, layer_scale2, parts=[part],
        pro=pro_attn_bwd(1, 1, qkv_1b, ga_1, wp, wq, lens), nxt=pro_mlp_bwd(0, 0, load(n2_0h), None, *mlp, False),
        swap=[ga_1], save=[ga_1, n2_1x], fills=[fill_mlp(1, held(n2_1x), [gm_1ax, gm_1bx], *mlp)])

    gmid_0, rows_mid_0, ga_0, gm_0x, gm_0h, ga_1xh, part, gp_0b, gb_0b, gq_0a, gbq_0a, gq_1x, gbq_1x = back_mid(
        next(ids), 0, mid_0, norm2_gain, grad_1, asum_0, layer_scale1, parts=[part],
        pro=pro_mlp_bwd(1, 0, load(n2_0h), gm_0, *mlp, False), nxt=pro_attn_bwd(0, 0, qkv_0a, None, wp, wq, lens),
        swap=[gm_0], save=[gm_0, ga_1x], fills=[fill_attn_bwd(1, qkv_1x, ga_1x, wp, lens_x)])
    grad_0, rows_in_0, y_out, rows_mlp_1, ga_0x, ga_0h, gm_0xh, gq_0b, gbq_0b, hid_0x, gp_0x, gb_0x = back_in(
        next(ids), 0, x0, norm1_gain, gmid_0, None, None, parts=[part], pro=pro_attn_bwd(1, 0, qkv_0b, ga_0, wp, wq, lens),
        second=residual_last(1, (part_ya, part_yb), mid_1, b_down, layer_scale2, g_y),
        swap=[ga_0], save=[ga_0, gm_0x], fills=[fill_mlp(0, load(n2_0xh), [gm_0x], *mlp)])
    ga_0xh, sums, gq_0x, gbq_0x = stage_call(
        next(ids), None, [rows_mlp_1], [], ag=False, save=[ga_0x], fills=[fill_attn_bwd(0, qkv_0x, ga_0x, wp, lens_x)],
        sums=(rows_mlp_1, rows_in_1, rows_mid_1, rows_in_0, rows_mid_0, rows_mlp_0))

    operands = (
        ((n2_1h, n2_1xh), (gp_1a, gp_1b, gp_1x), (hid_1a, hid_1b, hid_1x), (gm_1ah, gm_1bh, gm_1axh, gm_1bxh),
         (gq_1a, gq_1b, gq_1x), (n1_1h, n1_1xh), (o_1a, o_1b, o_1x), (ga_1h, ga_1xh)),
        ((n2_0h, n2_0xh), (gp_0a, gp_0b, gp_0x), (hid_0a, hid_0b, hid_0x), (gm_0h, gm_0xh),
         (gq_0a, gq_0b, gq_0x), (n1_0h, n1_0xh), (o_0a, o_0b, o_0x), (ga_0h, ga_0xh)))
    jobs = []
    for k, ops in enumerate(operands):
        ops = [[a if a.ndim < 4 else flat(a) for a in arrs] for arrs in ops]
        jobs += [(slot, 1 - k, *ops[2 * slot:2 * slot + 2]) for slot in (range(4) if k else reversed(range(4)))]
    g_up, g_down, g_qkv, g_proj, g_b_up, g_b_qkv, n1g, n1b, n2g, n2b, ls1, bp, ls2, bd = grads_call(
        jobs, [[(gb_0a, gb_0b, gb_0x), (gb_1a, gb_1b, gb_1x)], [(gbq_0a, gbq_0b, gbq_0x), (gbq_1a, gbq_1b, gbq_1x)]], sums)
    return (y_out[:, :TOK], grad_0[:, :TOK], n1g, n1b,
            g_qkv.reshape(2, 3, 4, 64, WIDTH).transpose(0, 1, 4, 2, 3), g_b_qkv,
            g_proj.reshape(2, 4, 64, WIDTH), bp, ls1, n2g, n2b, g_up, g_b_up,
            g_down.reshape(2, WIDTH, WIDTH), bd, ls2)


def split(axis, ndim):
    return P(*('tp' if k == axis else None for k in range(ndim)))


def solution(mesh):
    rep = P()
    act = P('dp', 'tp', None)
    param_specs = (rep, rep, split(3, 5), split(2, 4), split(1, 4), rep, rep, rep, rep, split(3, 4), split(2, 3), split(1, 3),
                   rep, rep)
    return jax.shard_map(device_fn, mesh=mesh, in_specs=(act, act, P('dp')) + param_specs,
                         out_specs=(act, act) + param_specs, check_vma=False)
```

```python
import itertools

import jax
import jax.numpy as jnp
from jax import lax
from jax.experimental import pallas as pl
from jax.experimental.pallas import tpu as pltpu
from jax.sharding import PartitionSpec as P

NORM_EPS = 1e-6
NEG_BIG = -1e9
F32 = jnp.float32
BF16 = jnp.bfloat16
TOK = 66
PAD = 72
N_TP = 4
N_SEQ = 2
SEQ = N_TP * PAD
ROWS = N_SEQ * SEQ
WIDTH = 1024
HEADS = 256
LANES = 128
MIB = 2 ** 20
MESH_ID = pl.DeviceIdType.MESH
VMEM_SPEC = pl.BlockSpec(memory_space=pltpu.VMEM)
HBM_SPEC = pl.BlockSpec(memory_space=pltpu.HBM)


def sds(shape, dtype):
    return jax.ShapeDtypeStruct(shape, dtype)


def mm(a, b, dims=((1,), (0,))):
    return lax.dot_general(a, b, (dims, ((), ())), preferred_element_type=F32)


NT = ((1,), (1,))
TN = ((0,), (0,))


def load(arr, index=None, pin=False):
    return arr, True, index, pin or index is None


def held(arr):
    return arr, False, None, None


def first(x):
    return x[:1, :1]


class Work:
    def __init__(self, ins, outs, count, body, cost=1.0, fin=None, x=None):
        self.ins, self.outs, self.count, self.body, self.cost, self.fin, self.x = ins, outs, count, body, cost, fin, x


def sequence(ref, b=0):
    return jnp.concatenate([ref[b, k] for k in range(N_TP)], axis=0)


def stage_call(cid, local_fn, ins, out_shapes, ag=True, parts=(), pro=None, nxt=None, swap=(), save=(), extra=None, trade=(),
               fills=(), sums=None, second=None, budget=(4.5, 2.0, 2.5, 3.0)):
    width = ins[0].shape[-1]
    rs = bool(parts)
    args, in_specs, place = [], [], {}

    def add(arr, spec=VMEM_SPEC, pin=False):
        key = (id(arr), spec is HBM_SPEC)
        if key not in place:
            place[key] = len(args)
            args.append(pltpu.with_memory_space_constraint(arr, pltpu.HBM) if pin else arr)
            in_specs.append(spec)
        return place[key]

    outs, out_specs = [], []

    def add_out(shape, spec=VMEM_SPEC):
        outs.append(pltpu.HBM(shape.shape, shape.dtype) if spec is HBM_SPEC else shape)
        out_specs.append(spec)
        return len(outs) - 1

    scratch = []

    def add_scratch(item):
        scratch.append(item)
        return len(scratch) - 1

    i_parts = [add(a) for a in parts]
    i_x = add(pro.x) if pro else None
    parts2, local2, ins2, shapes2 = second or ((), None, (), ())
    i_parts2 = [add(a) for a in parts2]
    i_ins2 = [add(a) for a in ins2]
    i_ins = [add(a) for a in ins]
    i_swap = [add(a) for a in swap]
    i_save = [add(a) for a in save]
    i_trade = [add(a) for a in trade]
    i_extra = [add(a) for a in extra[2:]] if extra else []
    i_sums = [add(a) for a in sums] if sums is not None else []
    o_local = [add_out(s) for s in out_shapes]
    o_local2 = [add_out(s) for s in shapes2]
    full_shape = sds((N_SEQ, N_TP, PAD, width), BF16)
    o_full = add_out(full_shape) if ag else None
    o_swap = [add_out(sds(a.shape, BF16)) for a in swap]
    o_save = [add_out(sds(a.shape, BF16), HBM_SPEC) for a in save]
    o_trade = [add_out(sds(a.shape, a.dtype)) for a in trade]
    o_extra = add_out(sds((1, N_TP, PAD, width), BF16)) if extra else None
    o_sums = add_out(sds((16, width), F32)) if sums is not None else None
    works = ([pro] if pro else []) + ([nxt] if nxt else []) + list(fills)
    o_part = add_out(sds((N_TP, PAD, width), BF16)) if nxt else None
    s_x = [add_scratch(pltpu.VMEM((SEQ, width), BF16)) for _ in range(2)]
    w_ins, w_outs = [], []
    n_load = n_store = 0
    for work in works:
        got = []
        for arr, copied, index, pin in work.ins:
            if copied:
                k = add_scratch(pltpu.VMEM(arr.shape if index is None else arr.shape[1:], arr.dtype))
                got.append((add(arr, HBM_SPEC, pin), index, k, n_load))
                n_load += 1
            else:
                got.append((add(arr), None, None, None))
        w_ins.append(got)
        kept = []
        for shape in work.outs:
            if shape.dtype == BF16:
                kept.append((add_out(shape, HBM_SPEC), add_scratch(pltpu.VMEM(shape.shape, shape.dtype)), n_store))
                n_store += 1
            else:
                kept.append((add_out(shape), None, None))
        w_outs.append(kept)
    shard = pltpu.VMEM((N_SEQ, PAD, width), BF16)
    s_bufs2 = [add_scratch(shard) for _ in range(4)] if second else []
    if rs:
        s_bufs = [add_scratch(shard) for _ in range(4)]
        s_part = add_scratch(pltpu.VMEM((N_TP, PAD, width), BF16)) if pro else None
    k_swap = 6 * N_SEQ
    k_extra = k_swap + 4 * len(swap)
    k_sum = k_extra + 3
    k_trade = k_sum + 3
    k_second = k_trade + len(trade)
    n_sem = k_second + 3 * N_SEQ * bool(second)
    s_send, s_recv = [add_scratch(pltpu.SemaphoreType.DMA((n_sem,))) for _ in range(2)]
    s_load = add_scratch(pltpu.SemaphoreType.DMA((n_load + n_store + len(save) + 1,)))
    if sums is not None:
        s_sum = [add_scratch(pltpu.VMEM((3, 16, width), F32)) for _ in range(2)]
    n_in, n_out = len(args), len(outs)

    def kernel(*refs):
        r_in, r_out, r_s = refs[:n_in], refs[n_in:n_in + n_out], refs[n_in + n_out:]
        in_refs = [r_in[k] for k in i_ins]
        out_refs = [r_out[k] for k in o_local]
        full = r_out[o_full] if ag else None
        ssem, rsem, lsem = r_s[s_send], r_s[s_recv], r_s[s_load]
        loads, use_in, use_out, stores, leaving = [], [], [], [], []
        for got, kept in zip(w_ins, w_outs):
            cps, use = [], []
            for k_in, index, k_buf, k_sem in got:
                if k_buf is None:
                    use.append(r_in[k_in])
                    continue
                src = r_in[k_in] if index is None else r_in[k_in].at[index]
                cps.append(pltpu.make_async_copy(src, r_s[k_buf], lsem.at[k_sem]))
                cps[-1].start()
                use.append(r_s[k_buf])
            loads.append(cps)
            use_in.append(use)
            use_out.append([r_out[k] if k_buf is None else r_s[k_buf] for k, k_buf, _ in kept])
            stores.append([pltpu.make_async_copy(r_s[k_buf], r_out[k], lsem.at[n_load + k_sem])
                           for k, k_buf, k_sem in kept if k_buf is not None])
        dp = lax.axis_index('dp')
        t = lax.axis_index('tp')
        core = lax.rem(t, 2)
        mate = t + 1 - 2 * core
        peer = lax.rem(t + 2, N_TP)
        far = lax.rem(mate + 2, N_TP)
        here, there = dp, 1 - dp

        def remote(src, dst, k, dev, line=None):
            return pltpu.make_async_remote_copy(src_ref=src, dst_ref=dst, send_sem=ssem.at[k], recv_sem=rsem.at[k],
                                                device_id=(here if line is None else line, dev), device_id_type=MESH_ID)

        def leave(cps):
            for cp in cps:
                cp.start()
            leaving.extend(cps)

        leave([pltpu.make_async_copy(r_in[a], r_out[b], lsem.at[n_load + n_store + k])
               for k, (a, b) in enumerate(zip(i_save, o_save))])
        barrier = pltpu.get_barrier_semaphore()
        peers = [(here, mate), (here, peer)]
        if swap or trade or sums is not None:
            peers.append((there, t))
        for dev in peers:
            pl.semaphore_signal(barrier, inc=1, device_id=dev, device_id_type=MESH_ID)
        pl.semaphore_wait(barrier, len(peers))

        first = bool(pro) + bool(nxt)
        done = [0] * len(works)

        def run(time):
            for f in range(first, len(works)):
                work = works[f]
                left = work.count - done[f]
                n = left if time is None else min(left, int(time / work.cost + 0.5))
                if n <= 0:
                    continue
                if done[f] == 0:
                    for cp in loads[f]:
                        cp.wait()
                lo = done[f]
                done[f] = hi = lo + n
                if n == 1:
                    work.body(lo, use_in[f], use_out[f])
                else:
                    @pl.loop(lo, hi)
                    def _(i, work=work, f=f):
                        work.body(i, use_in[f], use_out[f])
                if hi == work.count:
                    leave(stores[f])
                if time is not None:
                    time -= n * work.cost

        def channel(part_refs, bufs, k0):
            far_buf, mate_buf, peer_buf, send_buf = [r_s[k] for k in bufs]
            c_far = [remote(part_refs[b].at[far], far_buf.at[b], k0 + b, mate) for b in range(N_SEQ)]
            c_mate = [remote(part_refs[b].at[mate], mate_buf.at[b], k0 + N_SEQ + b, mate) for b in range(N_SEQ)]
            c_peer = [remote(send_buf.at[b], peer_buf.at[b], k0 + 2 * N_SEQ + b, peer) for b in range(N_SEQ)]
            started.extend(c_far + c_mate + c_peer)

            def to_mate(b):
                c_far[b].start()
                c_mate[b].start()

            def to_peer(b):
                c_far[b].wait_recv()
                send_buf[b] = (part_refs[b][peer].astype(F32) + far_buf[b].astype(F32)).astype(BF16)
                c_peer[b].start()

            def total(b):
                c_mate[b].wait_recv()
                acc = part_refs[b][t].astype(F32) + mate_buf[b].astype(F32)
                c_peer[b].wait_recv()
                return acc + peer_buf[b].astype(F32)
            return to_mate, to_peer, total

        def begin(w, ref, b):
            for cp in loads[w]:
                cp.wait()
            r_s[s_x[w]][...] = sequence(ref, b)

        def produce(w, last):
            half = works[w].count // 2

            @pl.loop(half if last else 0, works[w].count if last else half)
            def _(u):
                works[w].body(u, r_s[s_x[w]], use_in[w], use_out[w])

        def finish(w, dst):
            val = works[w].fin(use_in[w], use_out[w]).astype(BF16)
            for k in range(N_TP):
                dst[k] = val[k * PAD:(k + 1) * PAD]

        started, landed = [], []
        for k, (a, b) in enumerate(zip(i_trade, o_trade)):
            cp = remote(r_in[a], r_out[b], k_trade + k, t, there)
            cp.start()
            started.append(cp)
            landed.append(cp)
        if extra:
            ex = r_out[o_extra]
            ex[0, t] = (row(r_in[i_extra[1]], extra[0]) * r_in[i_extra[0]][extra[1]].astype(F32)).astype(BF16)
            x_peer = remote(ex.at[0, t], ex.at[0, t], k_extra, peer)
            x_mate = remote(ex.at[0, t], ex.at[0, t], k_extra + 1, mate)
            x_peer.start()
            x_mate.start()
            started += [x_peer, x_mate]
            landed.append(x_mate)
        s_y = []
        for k in range(len(swap)):
            src, dst = r_in[i_swap[k]], r_out[o_swap[k]]
            for j in range(2):
                s_y.append(remote(src.at[:, core + 2 * j], dst.at[:, core + 2 * j], k_swap + 4 * k + j, t, there))
                s_y[-1].start()
        started += s_y
        if rs:
            part_refs = [r_in[k] for k in i_parts] + ([r_s[s_part]] if pro else [])
            to_mate, to_peer, total = channel(part_refs, s_bufs, 0)
            to_mate(0)
            if second:
                to_mate2, to_peer2, total2 = channel([r_in[k] for k in i_parts2], s_bufs2, k_second)
                for b in range(N_SEQ):
                    to_mate2(b)
            if pro:
                begin(0, r_in[i_x], 1)
                produce(0, False)
                to_peer(0)
                produce(0, True)
                finish(0, part_refs[1])
                to_mate(1)
                leave(stores[0])
                run(1.0)
                to_peer(1)
                if second:
                    for b in range(N_SEQ):
                        to_peer2(b)
                run(budget[0] - 3.0)
        g_peer, g_mate, g_fwd = [], [], []
        for b in range(N_SEQ) if local_fn else ():
            if rs and b:
                run(budget[1])
            val = local_fn(b, total(b) if rs else None, in_refs, out_refs)
            if ag:
                full[b, t] = val
                g_peer.append(remote(full.at[b, t], full.at[b, t], 3 * N_SEQ + b, peer))
                g_mate.append(remote(full.at[b, t], full.at[b, t], 4 * N_SEQ + b, mate))
                g_peer[b].start()
                g_mate[b].start()
        if second:
            for b in range(N_SEQ):
                local2(b, total2(b), [r_in[k] for k in i_ins2], [r_out[k] for k in o_local2])
        if sums is not None:
            sum_src, sum_dst = [r_s[k] for k in s_sum]
            at = 0
            for k in i_sums:
                n_rows = args[k].shape[0]
                sum_src[0, at:at + n_rows, :] = r_in[k][...]
                at += n_rows
            for k, (line, dev) in enumerate([(here, mate), (here, peer), (there, t)]):
                cp = remote(sum_src.at[k], sum_dst.at[k], k_sum + k, dev, line)
                cp.start()
                if k:
                    run(budget[2])
                cp.wait_recv()
                started.append(cp)
                total = sum_src[k] + sum_dst[k]
                if k < 2:
                    sum_src[k + 1] = total
                else:
                    r_out[o_sums][...] = total
        if extra:
            x_peer.wait_recv()
            x_fwd = remote(ex.at[0, peer], ex.at[0, peer], k_extra + 2, mate)
            x_fwd.start()
            started.append(x_fwd)
            landed.append(x_fwd)
        if ag:
            def forward(b):
                g_peer[b].wait_recv()
                g_fwd.append(remote(full.at[b, peer], full.at[b, peer], 5 * N_SEQ + b, mate))
                g_fwd[b].start()

            run(budget[2])
            forward(0)
            run(1.0)
            if nxt:
                w = int(bool(pro))
                g_mate[0].wait_recv()
                g_fwd[0].wait_recv()
                begin(w, full, 0)
                produce(w, False)
                forward(1)
                produce(w, True)
                finish(w, r_out[o_part])
                leave(stores[w])
            else:
                run(budget[3])
                forward(1)
            started += g_peer + g_mate + g_fwd
            landed += (g_mate + g_fwd) if not nxt else (g_mate[1:] + g_fwd[1:])
        for k in range(len(swap)):
            dst = r_out[o_swap[k]]
            for j in range(2):
                s_y[2 * k + j].wait_recv()
                cp = remote(dst.at[:, core + 2 * j], dst.at[:, core + 2 * j], k_swap + 4 * k + 2 + j, mate)
                cp.start()
                started.append(cp)
                landed.append(cp)
        run(None)
        for cp in landed:
            cp.wait_recv()
        for cp in started:
            cp.wait_send()
        for cp in leaving:
            cp.wait()

    return pl.pallas_call(
        kernel,
        out_shape=outs,
        in_specs=in_specs,
        out_specs=out_specs,
        scratch_shapes=scratch,
        compiler_params=pltpu.CompilerParams(collective_id=cid, has_side_effects=True, vmem_limit_bytes=40 * MIB),
        cost_estimate=pl.CostEstimate(flops=40_000_000, bytes_accessed=4_000_000, transcendentals=0),
        name=f'stage{cid}',
    )(*args)


def row(ref, layer):
    return ref[layer:layer + 1, :]


def row_sum(x):
    return jnp.sum(x, axis=-1, keepdims=True)


def row_mean(x):
    return row_sum(x) / x.shape[-1]


def col_sum(x):
    return jnp.sum(x, axis=0, keepdims=True)


def ln_stats(x):
    x_f32 = x.astype(F32)
    centered = x_f32 - row_mean(x_f32)
    inv_std = lax.rsqrt(row_mean(centered * centered) + NORM_EPS)
    return centered * inv_std, inv_std


def ln_bwd(grad_out, x, gain):
    x_hat, inv_std = ln_stats(x)
    grad_hat = grad_out * gain
    mean_one = row_mean(grad_hat)
    mean_two = row_mean(grad_hat * x_hat)
    return inv_std * (grad_hat - mean_one - x_hat * mean_two), x_hat


def add_rows(rows_ref, b, rows):
    for k, val in enumerate(rows):
        s = col_sum(val)
        rows_ref[k:k + 1, :] = s if b == 0 else rows_ref[k:k + 1, :] + s


def key_valid(seq_len):
    col = lax.broadcasted_iota(jnp.int32, (SEQ, SEQ), 1)
    shard = jnp.zeros_like(col)
    for k in range(1, N_TP):
        shard = shard + (col >= k * PAD).astype(jnp.int32)
    return jnp.logical_and(col - PAD * shard < TOK, col - (PAD - TOK) * shard < seq_len)


def head_probs(q_half, k_pair, valid):
    scores = mm(q_half, k_pair, NT) * 0.125
    scores = jnp.where(valid, scores, NEG_BIG)
    e = jnp.exp(scores - jnp.max(scores, axis=-1, keepdims=True))
    return e / row_sum(e)


def seq_rows(b):
    return pl.ds(b * SEQ if isinstance(b, int) else pl.multiple_of(b * SEQ, SEQ), SEQ)


def pair_cols(pair):
    return pl.ds(pl.multiple_of(pair * LANES, LANES), LANES)


def flat(x):
    return x.reshape(-1, x.shape[-1])


def attn_fwd_unit(rows, pair, x, w_ref, bias, seq_len, qkv_ref, o_ref):
    cols = pair_cols(pair)
    pieces = []
    for c in range(3):
        val = (mm(x, w_ref[c, cols, :], NT) + bias[c:c + 1, cols]).astype(BF16)
        qkv_ref[c, rows, cols] = val
        pieces.append(val)
    q, k, v = pieces
    valid = key_valid(seq_len)
    half = lax.broadcasted_iota(jnp.int32, (SEQ, LANES), 1) // 64
    res = []
    for h in range(2):
        probs = head_probs(jnp.where(half == h, q, jnp.zeros_like(q)), k, valid)
        res.append(mm(probs.astype(BF16), v))
    o_ref[rows, cols] = jnp.where(half == 0, res[0], res[1]).astype(BF16)


def attn_bwd_unit(rows, pair, g, qkv_ref, w_ref, seq_len, dqkv_ref, db_ref):
    cols = pair_cols(pair)
    do = mm(g, w_ref[cols, :], NT).astype(BF16)
    q, k, v = (qkv_ref[c, rows, cols] for c in range(3))
    valid = key_valid(seq_len)
    half = lax.broadcasted_iota(jnp.int32, (SEQ, LANES), 1) // 64
    dq, dk, dv = [], [], []
    for h in range(2):
        probs = head_probs(jnp.where(half == h, q, jnp.zeros_like(q)), k, valid)
        grad_p = mm(jnp.where(half == h, do, jnp.zeros_like(do)), v, NT)
        grad_s = (probs * (grad_p - row_sum(grad_p * probs)) * 0.125).astype(BF16)
        dv.append(mm(probs.astype(BF16), do, TN))
        dq.append(mm(grad_s, k))
        dk.append(mm(grad_s, q, TN))
    for c, pieces in enumerate((dq, dk, dv)):
        val = jnp.where(half == 0, pieces[0], pieces[1])
        dqkv_ref[c, rows, cols] = val.astype(BF16)
        db_ref[c:c + 1, cols] = col_sum(val)


def mlp_up_unit(x, u_ref, bias, cols):
    gate = mm(x, u_ref[0, :, cols]) + bias[0:1, cols]
    lin = mm(x, u_ref[1, :, cols]) + bias[1:2, cols]
    return gate, lin


def mlp_bwd_unit(rows, u, x, g, u_ref, bias, d_ref, hid_ref, gp_ref, gb_ref):
    cols = pl.ds(pl.multiple_of(u * HEADS, HEADS), HEADS)
    gate, lin = mlp_up_unit(x, u_ref, bias, cols)
    grad_hid = mm(g, d_ref[cols, :], NT)
    sig = jax.nn.sigmoid(gate)
    if hid_ref is not None:
        hid_ref[rows, cols] = (gate * sig * lin).astype(BF16)
    grad_gate = grad_hid * lin * sig * (1.0 + gate * (1.0 - sig))
    grad_lin = grad_hid * gate * sig
    for c, val in enumerate((grad_gate, grad_lin)):
        gp_ref[c, rows, cols] = val.astype(BF16)
        gb_ref[c:c + 1, cols] = col_sum(val)


def qkv_shape(rows):
    return sds((3, rows, HEADS), BF16)


def heads_shape(rows):
    return sds((rows, HEADS), BF16)


def hidden_shape(rows):
    return sds((rows, WIDTH), BF16)


def grad_pre_shape(rows):
    return sds((2, rows, WIDTH), BF16)


ALL = pl.ds(0, SEQ)
GRAD_BQ = sds((3, HEADS), F32)
GRAD_BU = sds((2, WIDTH), F32)
BOTH_BQ = sds((N_SEQ, 3, HEADS), F32)


def fill_attn_fwd(layer, normed, wq, bq, lens):
    def body(i, ins, outs):
        n_ref, w_ref, b_ref, vl_ref = ins
        b = i // 2
        attn_fwd_unit(seq_rows(b), i % 2, sequence(n_ref, b), w_ref, b_ref.at[layer], first(vl_ref[b]), *outs)
    return Work([held(normed), load(wq, layer), held(bq), held(lens)], [qkv_shape(ROWS), heads_shape(ROWS)], 4, body, 1.8)


def fill_attn_bwd(layer, qkv, grad, wp, lens):
    def body(i, ins, outs):
        qkv_ref, g_ref, w_ref, vl_ref = ins
        b = i // 2
        attn_bwd_unit(seq_rows(b), i % 2, sequence(g_ref, b), qkv_ref, w_ref, first(vl_ref[b]), outs[0], outs[1].at[b])
    return Work([load(qkv), held(grad), load(wp, layer), held(lens)], [qkv_shape(ROWS), BOTH_BQ], 4, body, 2.0)


def fill_mlp(layer, normed, grads, w_up, b_up, w_down):
    def body(i, ins, outs):
        n_ref, u_ref, b_ref, d_ref = ins[:4]
        n, g = (jnp.concatenate([sequence(ref, b) for ref in refs for b in range(ref.shape[0])], axis=0)
                for refs in ([n_ref], ins[4:]))
        mlp_bwd_unit(pl.ds(0, ROWS), i, n, g, u_ref, b_ref.at[layer], d_ref, *outs[:2], outs[2].at[0])
    return Work([normed, load(w_up, layer), held(b_up), load(w_down, layer)] + [held(g) for g in grads],
                [hidden_shape(ROWS), grad_pre_shape(ROWS), sds((1, 2, WIDTH), F32)], 4, body, 1.6)


def pro_attn_fwd(b, layer, normed, wq, bq, wp, lens):
    early = not (layer or b)

    def body(u, x, ins, outs):
        w_ref, b_ref, _, vl_ref = ins
        attn_fwd_unit(ALL, u, x[...], w_ref, b_ref.at[layer], first(vl_ref[b]), *outs)

    def fin(ins, outs):
        return mm(outs[1][...], ins[2][...])
    return Work([load(wq, layer, early), held(bq), load(wp, layer, early), held(lens)], [qkv_shape(SEQ), heads_shape(SEQ)], 2, body,
                fin=fin, x=normed)


def pro_mlp_fwd(layer, normed, w_up, b_up, w_down):
    def body(u, x, ins, outs):
        u_ref, b_ref, _ = ins
        cols = pl.ds(pl.multiple_of(u * HEADS, HEADS), HEADS)
        gate, lin = mlp_up_unit(x[...], u_ref, b_ref.at[layer], cols)
        outs[0][:, cols] = (jax.nn.silu(gate) * lin).astype(BF16)

    def fin(ins, outs):
        return mm(outs[0][...], ins[2][...])
    return Work([load(w_up, layer), held(b_up), load(w_down, layer)], [hidden_shape(SEQ)], 4, body, fin=fin, x=normed)


def pro_mlp_bwd(b, layer, normed, grad, w_up, b_up, w_down, forward):
    extra = grad if forward else normed

    def body(u, x, ins, outs):
        u_ref, b_ref, d_ref, e_ref = ins
        pair = (x[...], sequence(e_ref, b if e_ref.shape[0] > 1 else 0))
        n, g = pair if forward else pair[::-1]
        mlp_bwd_unit(ALL, u, n, g, u_ref, b_ref.at[layer], d_ref, outs[2] if forward else None, *outs[:2])

    def fin(ins, outs):
        if forward:
            val = mm(outs[2][...], ins[2][...]).astype(BF16)
            for k in range(N_TP):
                outs[3][k] = val[k * PAD:(k + 1) * PAD]
        return sum(mm(outs[0][c], ins[0][c], NT) for c in range(2))
    return Work([load(w_up, layer), held(b_up), load(w_down, layer), extra],
                [grad_pre_shape(SEQ), GRAD_BU] + ([hidden_shape(SEQ), sds((N_TP, PAD, WIDTH), BF16)] if forward else []),
                4, body, fin=fin, x=normed if forward else grad)


def pro_attn_bwd(b, layer, qkv, grad, wp, wq, lens):
    def body(u, x, ins, outs):
        qkv_ref, w_ref, _, vl_ref = ins
        attn_bwd_unit(ALL, u, x[...], qkv_ref, w_ref, first(vl_ref[b]), *outs)

    def fin(ins, outs):
        return sum(mm(outs[0][c], ins[2][c]) for c in range(3))
    return Work([load(qkv), load(wp, layer), load(wq, layer), held(lens)], [qkv_shape(SEQ), GRAD_BQ], 2, body, fin=fin,
                x=grad)


def gather_norm(cid, layer, x, gain, bias, **side):
    def local(b, acc, ins, outs):
        x_ref, g_ref, b_ref = ins
        x_hat, _ = ln_stats(x_ref[b])
        return (x_hat * row(g_ref, layer) + row(b_ref, layer)).astype(BF16)
    return stage_call(cid, local, (x, gain, bias), [], **side)


def residual_norm(cid, layer, x, bias, scale, norm_layer, gain, shift, **side):
    def local(b, acc, ins, outs):
        x_ref, b_ref, s_ref, g_ref, h_ref = ins
        total = acc + row(b_ref, layer)
        outs[1][b] = total
        x_new = (x_ref[b].astype(F32) + row(s_ref, layer) * total).astype(BF16)
        outs[0][b] = x_new
        x_hat, _ = ln_stats(x_new)
        return (x_hat * row(g_ref, norm_layer) + row(h_ref, norm_layer)).astype(BF16)
    return stage_call(cid, local, (x, bias, scale, gain, shift), [sds(x.shape, BF16), sds(x.shape, F32)], **side)


def residual_last(layer, parts, x, bias, scale, grad_y):
    def local(b, acc, ins, outs):
        x_ref, b_ref, s_ref, g_ref = ins
        total = acc + row(b_ref, layer)
        outs[0][b] = (x_ref[b].astype(F32) + row(s_ref, layer) * total).astype(BF16)
        grad = g_ref[b].astype(F32)
        add_rows(outs[1], b, [grad * total, row(s_ref, layer) * grad])
    return parts, local, (x, bias, scale, grad_y), [sds(x.shape, BF16), sds((2, x.shape[-1]), F32)]


def back_mid(cid, layer, x_mid, gain, grad_res, attn_sum, scale, **side):
    def local(b, acc, ins, outs):
        x_ref, g_ref, r_ref, a_ref, s_ref = ins
        grad_in, x_hat = ln_bwd(acc, x_ref[b], row(g_ref, layer))
        grad_mid = r_ref[b].astype(F32) + grad_in
        outs[0][b] = grad_mid
        grad_attn = row(s_ref, layer) * grad_mid
        add_rows(outs[1], b, [acc * x_hat, acc, grad_mid * a_ref[b], grad_attn])
        return grad_attn.astype(BF16)
    return stage_call(cid, local, (x_mid, gain, grad_res, attn_sum, scale),
                      [sds(x_mid.shape, F32), sds((4, x_mid.shape[-1]), F32)], **side)


def back_in(cid, layer, x_in, gain, grad_mid, mlp_sum, scale, **side):
    more = layer > 0

    def local(b, acc, ins, outs):
        x_ref, g_ref, m_ref = ins[:3]
        grad_in, x_hat = ln_bwd(acc, x_ref[b], row(g_ref, layer))
        grad = (m_ref[b] + grad_in).astype(BF16)
        outs[0][b] = grad
        if not more:
            add_rows(outs[1], b, [acc * x_hat, acc])
            return None
        grad = grad.astype(F32)
        grad_mlp = row(ins[4], layer - 1) * grad
        add_rows(outs[1], b, [acc * x_hat, acc])
        add_rows(outs[2], b, [grad * ins[3][b], grad_mlp])
        return grad_mlp.astype(BF16)
    shapes = [sds(x_in.shape, BF16)] + [sds((2, x_in.shape[-1]), F32)] * (2 if more else 1)
    return stage_call(cid, local, (x_in, gain, grad_mid) + ((mlp_sum, scale) if more else ()), shapes, ag=more, **side)


def grads_call(jobs, biases, sums):
    args, bufs, loads = [], [], []
    for job in jobs:
        for arrs in job[2:]:
            at = 0
            for arr in arrs:
                loads.append((len(args), len(bufs), at))
                args.append(arr)
                at += arr.shape[-2]
            wide = arrs[0].shape[0] if job[0] == 2 and arrs[0].ndim > 2 else 1
            lead = arrs[0].shape[:-2] if wide == 1 else ()
            bufs.append(pltpu.VMEM((*lead, at, wide * arrs[0].shape[-1]), BF16))
    n_op = len(args)
    small = [x for group in biases for trio in group for x in trio] + [sums]
    args = [pltpu.with_memory_space_constraint(a, pltpu.HBM) for a in args] + small
    specs = [HBM_SPEC] * n_op + [VMEM_SPEC] * len(small)
    width = sums.shape[-1]
    shapes = [(groups, total, width) for groups, total in ((2, WIDTH), (1, WIDTH), (3, HEADS), (1, HEADS))]
    shapes += [biases[0][0][0].shape, (3, N_TP, HEADS // N_TP)] + [(width,)] * 8
    outs = [sds((2, *shape), F32) for shape in shapes]
    stage_rows = WIDTH

    def kernel(*refs):
        ops, smalls = refs[:n_op], refs[n_op:len(args)]
        out = refs[len(args):len(args) + len(outs)]
        buf = refs[len(args) + len(outs):]
        stage, lsem, osem = buf[len(bufs):]
        copies = []
        for k, k_buf, at in loads:
            n_rows, n_cols = ops[k].shape[-2:]
            rows, dst = pl.ds(at, n_rows), buf[k_buf]
            if len(ops[k].shape) == len(dst.shape):
                pairs = [(ops[k], dst.at[:, rows] if len(dst.shape) == 3 else dst.at[rows])]
            else:
                pairs = [(ops[k].at[c], dst.at[rows, pl.ds(c * n_cols, n_cols)]) for c in range(ops[k].shape[0])]
            for src, to in pairs:
                copies.append((pltpu.make_async_copy(src, to, lsem.at[len(copies)]), k_buf // 2))

        def fetch(j, act):
            for cp, owner in copies:
                if owner == j:
                    act(cp)

        for j in range(2):
            fetch(j, lambda cp: cp.start())
        for l in range(2):
            for k in range(2):
                own_a, own_b, oth = smalls[6 * k + 3 * l:][:3]
                val = sum((oth[b] for b in range(oth.shape[0])), own_a[...] + own_b[...])
                if k:
                    n = out[5].shape[-1]
                    for h in range(N_TP):
                        out[5][l, :, h, :] = val[:, h * n:(h + 1) * n]
                else:
                    out[4][l] = val
        rows = smalls[-1]
        for k in range(8):
            for l, at in enumerate((8 + k, 2 + k if k < 6 else k - 6)):
                out[6 + k][l:l + 1, :] = rows[at:at + 1, :]
        pending = [[]] * 2
        step = 0
        for j, (slot, layer, *_) in enumerate(jobs):
            a_ref, b_ref = buf[2 * j:2 * j + 2]
            fetch(j, lambda cp: cp.wait())
            fetch(j + 2, lambda cp: cp.start())
            total = outs[slot].shape[2]
            split_b = len(b_ref.shape) > 2
            for g in range(b_ref.shape[0] if split_b else 1):
                s = step % 2
                val = mm(a_ref[...], b_ref[g] if split_b else b_ref[...], TN)
                for cp in pending[s]:
                    cp.wait()
                stage[s, :val.shape[0]] = val
                pending[s] = [pltpu.make_async_copy(stage.at[s, pl.ds(k * total, total)], out[slot].at[layer, g + k], osem.at[s, k])
                              for k in range(val.shape[0] // total)]
                for cp in pending[s]:
                    cp.start()
                step += 1
        for cp in pending[0] + pending[1]:
            cp.wait()

    return pl.pallas_call(
        kernel,
        out_shape=outs,
        in_specs=specs,
        out_specs=[HBM_SPEC] * 4 + [VMEM_SPEC] * 10,
        scratch_shapes=bufs + [pltpu.VMEM((2, stage_rows, width), F32), pltpu.SemaphoreType.DMA((2 * n_op,)),
                               pltpu.SemaphoreType.DMA((2, 3))],
        compiler_params=pltpu.CompilerParams(vmem_limit_bytes=60 * MIB),
        cost_estimate=pl.CostEstimate(flops=40_000_000_000, bytes_accessed=80_000_000, transcendentals=0),
        name='grads')(*args)


def device_fn(tokens, grad_y, valid_len, norm1_gain, norm1_bias, w_qkv, b_qkv, w_proj, b_proj, layer_scale1,
              norm2_gain, norm2_bias, w_up, b_up, w_down, b_down, layer_scale2):
    pad = ((0, 0), (0, PAD - TOK), (0, 0))
    x0 = jnp.pad(tokens, pad)
    g_y = jnp.pad(grad_y, pad)
    lens = jnp.broadcast_to(valid_len[:, None, None], (N_SEQ, 8, LANES))
    wq = jnp.moveaxis(w_qkv, 2, 4).reshape(2, 3, HEADS, WIDTH)
    bq = b_qkv.reshape(2, 3, HEADS)
    wp = w_proj.reshape(2, HEADS, WIDTH)

    mlp = w_up, b_up, w_down
    ids = itertools.count()
    n1_0, lens_x, part, qkv_0a, o_0a = gather_norm(
        next(ids), 0, x0, norm1_gain, norm1_bias, trade=[lens], nxt=pro_attn_fwd(0, 0, None, wq, bq, wp, lens))
    mid_0, asum_0, n2_0, n1_0x, n1_0h, gm_1a, part, qkv_0b, o_0b, hid_0a = residual_norm(
        next(ids), 0, x0, b_proj, layer_scale1, 0, norm2_gain, norm2_bias, parts=[part],
        pro=pro_attn_fwd(1, 0, n1_0, wq, bq, wp, lens), nxt=pro_mlp_fwd(0, None, *mlp),
        swap=[n1_0], save=[n1_0], extra=(1, 0, g_y, layer_scale2))
    x1, msum_0, n1_1, n2_0x, gm_1ax, n2_0h, n1_0xh, gm_1ah, gm_1b, part, hid_0b, qkv_1a, o_1a, qkv_0x, o_0x = residual_norm(
        next(ids), 0, mid_0, b_down, layer_scale2, 1, norm1_gain, norm1_bias, parts=[part],
        pro=pro_mlp_fwd(0, n2_0, *mlp), nxt=pro_attn_fwd(0, 1, None, wq, bq, wp, lens),
        swap=[n2_0, gm_1a], save=[n2_0, n1_0x, gm_1a], extra=(1, 1, g_y, layer_scale2),
        fills=[fill_attn_fwd(0, n1_0x, wq, bq, lens_x)])
    (mid_1, asum_1, n2_1, n1_1x, n1_1h, gm_1bh, gm_1axh, n2_0xh, part, qkv_1b, o_1b, gp_1a, gb_1a, hid_1a,
     part_ya) = residual_norm(
        next(ids), 1, x1, b_proj, layer_scale1, 1, norm2_gain, norm2_bias, parts=[part],
        pro=pro_attn_fwd(1, 1, n1_1, wq, bq, wp, lens), nxt=pro_mlp_bwd(0, 1, None, held(gm_1a), *mlp, True),
        swap=[n1_1], save=[n1_1, gm_1b, gm_1ax, n2_0x])

    (gmid_1, rows_mid_1, ga_1, n2_1x, gm_1bx, n2_1h, n1_1xh, part, gp_1b, gb_1b, hid_1b, part_yb, gq_1a, gbq_1a, qkv_1x,
     o_1x) = back_mid(
        next(ids), 1, mid_1, norm2_gain, g_y, asum_1, layer_scale1, parts=[part],
        pro=pro_mlp_bwd(1, 1, n2_1, held(gm_1b), *mlp, True), nxt=pro_attn_bwd(0, 1, qkv_1a, None, wp, wq, lens),
        swap=[n2_1, gm_1b], save=[n2_1, n1_1x], fills=[fill_attn_fwd(1, n1_1x, wq, bq, lens_x)])
    (grad_1, rows_in_1, rows_mlp_0, gm_0, ga_1x, ga_1h, n2_1xh, gm_1bxh, part, gq_1b, gbq_1b, gp_0a, gb_0a, hid_1x, gp_1x,
     gb_1x) = back_in(
        next(ids), 1, x1, norm1_gain, gmid_1, msum_0, layer_scale2, parts=[part],
        pro=pro_attn_bwd(1, 1, qkv_1b, ga_1, wp, wq, lens), nxt=pro_mlp_bwd(0, 0, load(n2_0h), None, *mlp, False),
        swap=[ga_1], save=[ga_1, n2_1x, gm_1bx], fills=[fill_mlp(1, held(n2_1x), [gm_1ax, gm_1bx], *mlp)])

    gmid_0, rows_mid_0, ga_0, gm_0x, gm_0h, ga_1xh, part, gp_0b, gb_0b, gq_0a, gbq_0a, gq_1x, gbq_1x = back_mid(
        next(ids), 0, mid_0, norm2_gain, grad_1, asum_0, layer_scale1, parts=[part],
        pro=pro_mlp_bwd(1, 0, load(n2_0h), gm_0, *mlp, False), nxt=pro_attn_bwd(0, 0, qkv_0a, None, wp, wq, lens),
        swap=[gm_0], save=[gm_0, ga_1x], fills=[fill_attn_bwd(1, qkv_1x, ga_1x, wp, lens_x)])
    grad_0, rows_in_0, y_out, rows_mlp_1, ga_0x, ga_0h, gm_0xh, gq_0b, gbq_0b, hid_0x, gp_0x, gb_0x = back_in(
        next(ids), 0, x0, norm1_gain, gmid_0, None, None, parts=[part], pro=pro_attn_bwd(1, 0, qkv_0b, ga_0, wp, wq, lens),
        second=residual_last(1, (part_ya, part_yb), mid_1, b_down, layer_scale2, g_y),
        swap=[ga_0], save=[ga_0, gm_0x], fills=[fill_mlp(0, load(n2_0xh), [gm_0x], *mlp)])
    ga_0xh, sums, gq_0x, gbq_0x = stage_call(
        next(ids), None, [rows_mlp_1], [], ag=False, save=[ga_0x], fills=[fill_attn_bwd(0, qkv_0x, ga_0x, wp, lens_x)],
        sums=(rows_mlp_1, rows_in_1, rows_mid_1, rows_in_0, rows_mid_0, rows_mlp_0))

    operands = (
        ((n2_1h, n2_1xh), (gp_1a, gp_1b, gp_1x), (hid_1a, hid_1b, hid_1x), (gm_1ah, gm_1bh, gm_1axh, gm_1bxh),
         (gq_1a, gq_1b, gq_1x), (n1_1h, n1_1xh), (o_1a, o_1b, o_1x), (ga_1h, ga_1xh)),
        ((n2_0h, n2_0xh), (gp_0a, gp_0b, gp_0x), (hid_0a, hid_0b, hid_0x), (gm_0h, gm_0xh),
         (gq_0a, gq_0b, gq_0x), (n1_0h, n1_0xh), (o_0a, o_0b, o_0x), (ga_0h, ga_0xh)))
    jobs = []
    for k, ops in enumerate(operands):
        ops = [[a if a.ndim < 4 else flat(a) for a in arrs] for arrs in ops]
        jobs += [(slot, 1 - k, *ops[2 * slot:2 * slot + 2]) for slot in (range(4) if k else reversed(range(4)))]
    g_up, g_down, g_qkv, g_proj, g_b_up, g_b_qkv, n1g, n1b, n2g, n2b, ls1, bp, ls2, bd = grads_call(
        jobs, [[(gb_0a, gb_0b, gb_0x), (gb_1a, gb_1b, gb_1x)], [(gbq_0a, gbq_0b, gbq_0x), (gbq_1a, gbq_1b, gbq_1x)]], sums)
    return (y_out[:, :TOK], grad_0[:, :TOK], n1g, n1b,
            jnp.moveaxis(g_qkv.reshape(2, 3, 4, 64, WIDTH), 4, 2), g_b_qkv,
            g_proj.reshape(2, 4, 64, WIDTH), bp, ls1, n2g, n2b, g_up, g_b_up,
            g_down.reshape(2, WIDTH, WIDTH), bd, ls2)


def split(axis, ndim):
    return P(*('tp' if k == axis else None for k in range(ndim)))


def solution(mesh):
    rep = P()
    act = P('dp', 'tp', None)
    param_specs = (rep, rep, split(3, 5), split(2, 4), split(1, 4), rep, rep, rep, rep, split(3, 4), split(2, 3), split(1, 3),
                   rep, rep)
    return jax.shard_map(device_fn, mesh=mesh, in_specs=(act, act, P('dp')) + param_specs,
                         out_specs=(act, act) + param_specs, check_vma=False)
```

```python
import itertools

import jax
import jax.numpy as jnp
from jax import lax
from jax.experimental import pallas as pl
from jax.experimental.pallas import tpu as pltpu
from jax.sharding import PartitionSpec as P

NORM_EPS = 1e-6
NEG_BIG = -1e9
F32 = jnp.float32
BF16 = jnp.bfloat16
TOK = 66
PAD = 72
N_TP = 4
N_SEQ = 2
SEQ = N_TP * PAD
ROWS = N_SEQ * SEQ
WIDTH = 1024
HEADS = 256
LANES = 128
MIB = 2 ** 20
MESH_ID = pl.DeviceIdType.MESH
VMEM_SPEC = pl.BlockSpec(memory_space=pltpu.VMEM)
HBM_SPEC = pl.BlockSpec(memory_space=pltpu.HBM)


def sds(shape, dtype):
    return jax.ShapeDtypeStruct(shape, dtype)


def mm(a, b, dims=((1,), (0,))):
    return lax.dot_general(a, b, (dims, ((), ())), preferred_element_type=F32)


NT = ((1,), (1,))
TN = ((0,), (0,))


def load(arr, index=None, pin=False):
    return arr, True, index, pin or index is None


def held(arr):
    return arr, False, None, None


def first(x):
    return x[:1, :1]


class Work:
    def __init__(self, ins, outs, count, body, cost=1.0, fin=None, x=None):
        self.ins, self.outs, self.count, self.body, self.cost, self.fin, self.x = ins, outs, count, body, cost, fin, x


def sequence(ref, b=0):
    return jnp.concatenate([ref[b, k] for k in range(N_TP)], axis=0)


def stage_call(cid, local_fn, ins, out_shapes, ag=True, parts=(), pro=None, nxt=None, swap=(), save=(), extra=None, trade=(),
               fills=(), sums=None, second=None, budget=(4.5, 2.0, 2.5, 3.0)):
    width = ins[0].shape[-1]
    rs = bool(parts)
    args, in_specs, place = [], [], {}

    def add(arr, spec=VMEM_SPEC, pin=False):
        key = (id(arr), spec is HBM_SPEC)
        if key not in place:
            place[key] = len(args)
            args.append(pltpu.with_memory_space_constraint(arr, pltpu.HBM) if pin else arr)
            in_specs.append(spec)
        return place[key]

    outs, out_specs = [], []

    def add_out(shape, spec=VMEM_SPEC):
        outs.append(pltpu.HBM(shape.shape, shape.dtype) if spec is HBM_SPEC else shape)
        out_specs.append(spec)
        return len(outs) - 1

    scratch = []

    def add_scratch(item):
        scratch.append(item)
        return len(scratch) - 1

    i_parts = [add(a) for a in parts]
    i_x = add(pro.x) if pro else None
    parts2, local2, ins2, shapes2 = second or ((), None, (), ())
    i_parts2 = [add(a) for a in parts2]
    i_ins2 = [add(a) for a in ins2]
    i_ins = [add(a) for a in ins]
    i_swap = [add(a) for a in swap]
    i_save = [add(a) for a in save]
    i_trade = [add(a) for a in trade]
    i_extra = [add(a) for a in extra[2:]] if extra else []
    i_sums = [add(a) for a in sums] if sums is not None else []
    o_local = [add_out(s) for s in out_shapes]
    o_local2 = [add_out(s) for s in shapes2]
    full_shape = sds((N_SEQ, N_TP, PAD, width), BF16)
    o_full = add_out(full_shape) if ag else None
    o_swap = [add_out(sds(a.shape, BF16)) for a in swap]
    o_save = [add_out(sds(a.shape, BF16), HBM_SPEC) for a in save]
    o_trade = [add_out(sds(a.shape, a.dtype)) for a in trade]
    o_extra = add_out(sds((1, N_TP, PAD, width), BF16)) if extra else None
    o_sums = add_out(sds((16, width), F32)) if sums is not None else None
    works = ([pro] if pro else []) + ([nxt] if nxt else []) + list(fills)
    o_part = add_out(sds((N_TP, PAD, width), BF16)) if nxt else None
    s_x = [add_scratch(pltpu.VMEM((SEQ, width), BF16)) for _ in range(2)]
    w_ins, w_outs = [], []
    n_load = n_store = 0
    for work in works:
        got = []
        for arr, copied, index, pin in work.ins:
            if copied:
                k = add_scratch(pltpu.VMEM(arr.shape if index is None else arr.shape[1:], arr.dtype))
                got.append((add(arr, HBM_SPEC, pin), index, k, n_load))
                n_load += 1
            else:
                got.append((add(arr), None, None, None))
        w_ins.append(got)
        kept = []
        for shape in work.outs:
            if shape.dtype == BF16:
                kept.append((add_out(shape, HBM_SPEC), add_scratch(pltpu.VMEM(shape.shape, shape.dtype)), n_store))
                n_store += 1
            else:
                kept.append((add_out(shape), None, None))
        w_outs.append(kept)
    shard = pltpu.VMEM((N_SEQ, PAD, width), BF16)
    s_bufs2 = [add_scratch(shard) for _ in range(4)] if second else []
    if rs:
        s_bufs = [add_scratch(shard) for _ in range(4)]
        s_part = add_scratch(pltpu.VMEM((N_TP, PAD, width), BF16)) if pro else None
    k_swap = 6 * N_SEQ
    k_extra = k_swap + 4 * len(swap)
    k_sum = k_extra + 3
    k_trade = k_sum + 3
    k_second = k_trade + len(trade)
    n_sem = k_second + 3 * N_SEQ * bool(second)
    s_send, s_recv = [add_scratch(pltpu.SemaphoreType.DMA((n_sem,))) for _ in range(2)]
    s_load = add_scratch(pltpu.SemaphoreType.DMA((n_load + n_store + len(save) + 1,)))
    if sums is not None:
        s_sum = [add_scratch(pltpu.VMEM((3, 16, width), F32)) for _ in range(2)]
    n_in, n_out = len(args), len(outs)

    def kernel(*refs):
        r_in, r_out, r_s = refs[:n_in], refs[n_in:n_in + n_out], refs[n_in + n_out:]
        in_refs = [r_in[k] for k in i_ins]
        out_refs = [r_out[k] for k in o_local]
        full = r_out[o_full] if ag else None
        ssem, rsem, lsem = r_s[s_send], r_s[s_recv], r_s[s_load]
        loads, use_in, use_out, stores, leaving = [], [], [], [], []
        for got, kept in zip(w_ins, w_outs):
            cps, use = [], []
            for k_in, index, k_buf, k_sem in got:
                if k_buf is None:
                    use.append(r_in[k_in])
                    continue
                src = r_in[k_in] if index is None else r_in[k_in].at[index]
                cps.append(pltpu.make_async_copy(src, r_s[k_buf], lsem.at[k_sem]))
                cps[-1].start()
                use.append(r_s[k_buf])
            loads.append(cps)
            use_in.append(use)
            use_out.append([r_out[k] if k_buf is None else r_s[k_buf] for k, k_buf, _ in kept])
            stores.append([pltpu.make_async_copy(r_s[k_buf], r_out[k], lsem.at[n_load + k_sem])
                           for k, k_buf, k_sem in kept if k_buf is not None])
        dp = lax.axis_index('dp')
        t = lax.axis_index('tp')
        core = lax.rem(t, 2)
        mate = t + 1 - 2 * core
        peer = lax.rem(t + 2, N_TP)
        far = lax.rem(mate + 2, N_TP)
        here, there = dp, 1 - dp

        def remote(src, dst, k, dev, line=None):
            return pltpu.make_async_remote_copy(src_ref=src, dst_ref=dst, send_sem=ssem.at[k], recv_sem=rsem.at[k],
                                                device_id=(here if line is None else line, dev), device_id_type=MESH_ID)

        def leave(cps):
            for cp in cps:
                cp.start()
            leaving.extend(cps)

        leave([pltpu.make_async_copy(r_in[a], r_out[b], lsem.at[n_load + n_store + k])
               for k, (a, b) in enumerate(zip(i_save, o_save))])
        barrier = pltpu.get_barrier_semaphore()
        peers = [(here, mate), (here, peer)]
        if swap or trade or sums is not None:
            peers.append((there, t))
        for dev in peers:
            pl.semaphore_signal(barrier, inc=1, device_id=dev, device_id_type=MESH_ID)
        pl.semaphore_wait(barrier, len(peers))

        first = bool(pro) + bool(nxt)
        done = [0] * len(works)

        def run(time):
            for f in range(first, len(works)):
                work = works[f]
                left = work.count - done[f]
                n = left if time is None else min(left, int(time / work.cost + 0.5))
                if n <= 0:
                    continue
                if done[f] == 0:
                    for cp in loads[f]:
                        cp.wait()
                lo = done[f]
                done[f] = hi = lo + n
                if n == 1:
                    work.body(lo, use_in[f], use_out[f])
                else:
                    @pl.loop(lo, hi)
                    def _(i, work=work, f=f):
                        work.body(i, use_in[f], use_out[f])
                if hi == work.count:
                    leave(stores[f])
                if time is not None:
                    time -= n * work.cost

        def channel(part_refs, bufs, k0):
            far_buf, mate_buf, peer_buf, send_buf = [r_s[k] for k in bufs]
            c_far = [remote(part_refs[b].at[far], far_buf.at[b], k0 + b, mate) for b in range(N_SEQ)]
            c_mate = [remote(part_refs[b].at[mate], mate_buf.at[b], k0 + N_SEQ + b, mate) for b in range(N_SEQ)]
            c_peer = [remote(send_buf.at[b], peer_buf.at[b], k0 + 2 * N_SEQ + b, peer) for b in range(N_SEQ)]
            started.extend(c_far + c_mate + c_peer)

            def to_mate(b):
                c_far[b].start()
                c_mate[b].start()

            def to_peer(b):
                c_far[b].wait_recv()
                send_buf[b] = (part_refs[b][peer].astype(F32) + far_buf[b].astype(F32)).astype(BF16)
                c_peer[b].start()

            def total(b):
                c_mate[b].wait_recv()
                acc = part_refs[b][t].astype(F32) + mate_buf[b].astype(F32)
                c_peer[b].wait_recv()
                return acc + peer_buf[b].astype(F32)
            return to_mate, to_peer, total

        def begin(w, ref, b):
            for cp in loads[w]:
                cp.wait()
            r_s[s_x[w]][...] = sequence(ref, b)

        def produce(w, last):
            half = works[w].count // 2

            @pl.loop(half if last else 0, works[w].count if last else half)
            def _(u):
                works[w].body(u, r_s[s_x[w]], use_in[w], use_out[w])

        def finish(w, dst):
            val = works[w].fin(use_in[w], use_out[w]).astype(BF16)
            for k in range(N_TP):
                dst[k] = val[k * PAD:(k + 1) * PAD]

        started, landed = [], []
        for k, (a, b) in enumerate(zip(i_trade, o_trade)):
            cp = remote(r_in[a], r_out[b], k_trade + k, t, there)
            cp.start()
            started.append(cp)
            landed.append(cp)
        if extra:
            ex = r_out[o_extra]
            ex[0, t] = (row(r_in[i_extra[1]], extra[0]) * r_in[i_extra[0]][extra[1]].astype(F32)).astype(BF16)
            x_peer = remote(ex.at[0, t], ex.at[0, t], k_extra, peer)
            x_mate = remote(ex.at[0, t], ex.at[0, t], k_extra + 1, mate)
            x_peer.start()
            x_mate.start()
            started += [x_peer, x_mate]
            landed.append(x_mate)
        s_y = []
        for k in range(len(swap)):
            src, dst = r_in[i_swap[k]], r_out[o_swap[k]]
            for j in range(2):
                s_y.append(remote(src.at[:, core + 2 * j], dst.at[:, core + 2 * j], k_swap + 4 * k + j, t, there))
                s_y[-1].start()
        started += s_y
        if rs:
            part_refs = [r_in[k] for k in i_parts] + ([r_s[s_part]] if pro else [])
            to_mate, to_peer, total = channel(part_refs, s_bufs, 0)
            to_mate(0)
            if second:
                to_mate2, to_peer2, total2 = channel([r_in[k] for k in i_parts2], s_bufs2, k_second)
                for b in range(N_SEQ):
                    to_mate2(b)
            if pro:
                begin(0, r_in[i_x], 1)
                produce(0, False)
                to_peer(0)
                produce(0, True)
                finish(0, part_refs[1])
                to_mate(1)
                leave(stores[0])
                run(1.0)
                to_peer(1)
                if second:
                    for b in range(N_SEQ):
                        to_peer2(b)
                run(budget[0] - 3.0)
        g_peer, g_mate, g_fwd = [], [], []
        for b in range(N_SEQ) if local_fn else ():
            if rs and b:
                run(budget[1])
            val = local_fn(b, total(b) if rs else None, in_refs, out_refs)
            if ag:
                full[b, t] = val
                g_peer.append(remote(full.at[b, t], full.at[b, t], 3 * N_SEQ + b, peer))
                g_mate.append(remote(full.at[b, t], full.at[b, t], 4 * N_SEQ + b, mate))
                g_peer[b].start()
                g_mate[b].start()
        if second:
            for b in range(N_SEQ):
                local2(b, total2(b), [r_in[k] for k in i_ins2], [r_out[k] for k in o_local2])
        if sums is not None:
            sum_src, sum_dst = [r_s[k] for k in s_sum]
            at = 0
            for k in i_sums:
                n_rows = args[k].shape[0]
                sum_src[0, at:at + n_rows, :] = r_in[k][...]
                at += n_rows
            for k, (line, dev) in enumerate([(here, mate), (here, peer), (there, t)]):
                cp = remote(sum_src.at[k], sum_dst.at[k], k_sum + k, dev, line)
                cp.start()
                if k:
                    run(budget[2])
                cp.wait_recv()
                started.append(cp)
                total = sum_src[k] + sum_dst[k]
                if k < 2:
                    sum_src[k + 1] = total
                else:
                    r_out[o_sums][...] = total
        if extra:
            x_peer.wait_recv()
            x_fwd = remote(ex.at[0, peer], ex.at[0, peer], k_extra + 2, mate)
            x_fwd.start()
            started.append(x_fwd)
            landed.append(x_fwd)
        def forward_swaps():
            for k in range(len(swap)):
                dst = r_out[o_swap[k]]
                for j in range(2):
                    s_y[2 * k + j].wait_recv()
                    cp = remote(dst.at[:, core + 2 * j], dst.at[:, core + 2 * j], k_swap + 4 * k + 2 + j, mate)
                    cp.start()
                    started.append(cp)
                    landed.append(cp)

        if ag:
            def forward(b):
                g_peer[b].wait_recv()
                g_fwd.append(remote(full.at[b, peer], full.at[b, peer], 5 * N_SEQ + b, mate))
                g_fwd[b].start()

            run(budget[2])
            forward(0)
            run(1.0)
            if nxt:
                w = int(bool(pro))
                g_mate[0].wait_recv()
                g_fwd[0].wait_recv()
                begin(w, full, 0)
                produce(w, False)
                forward(1)
                produce(w, True)
                forward_swaps()
                finish(w, r_out[o_part])
                leave(stores[w])
            else:
                run(budget[3])
                forward(1)
            started += g_peer + g_mate + g_fwd
            landed += (g_mate + g_fwd) if not nxt else (g_mate[1:] + g_fwd[1:])
        if not nxt:
            forward_swaps()
        run(None)
        for cp in landed:
            cp.wait_recv()
        for cp in started:
            cp.wait_send()
        for cp in leaving:
            cp.wait()

    return pl.pallas_call(
        kernel,
        out_shape=outs,
        in_specs=in_specs,
        out_specs=out_specs,
        scratch_shapes=scratch,
        compiler_params=pltpu.CompilerParams(collective_id=cid, has_side_effects=True, vmem_limit_bytes=40 * MIB),
        cost_estimate=pl.CostEstimate(flops=40_000_000, bytes_accessed=4_000_000, transcendentals=0),
        name=f'stage{cid}',
    )(*args)


def row(ref, layer):
    return ref[layer:layer + 1, :]


def row_sum(x):
    return jnp.sum(x, axis=-1, keepdims=True)


def row_mean(x):
    return row_sum(x) / x.shape[-1]


def col_sum(x):
    return jnp.sum(x, axis=0, keepdims=True)


def ln_stats(x):
    x_f32 = x.astype(F32)
    centered = x_f32 - row_mean(x_f32)
    inv_std = lax.rsqrt(row_mean(centered * centered) + NORM_EPS)
    return centered * inv_std, inv_std


def ln_bwd(grad_out, x, gain):
    x_hat, inv_std = ln_stats(x)
    grad_hat = grad_out * gain
    mean_one = row_mean(grad_hat)
    mean_two = row_mean(grad_hat * x_hat)
    return inv_std * (grad_hat - mean_one - x_hat * mean_two), x_hat


def add_rows(rows_ref, b, rows):
    for k, val in enumerate(rows):
        s = col_sum(val)
        rows_ref[k:k + 1, :] = s if b == 0 else rows_ref[k:k + 1, :] + s


def key_valid(seq_len):
    col = lax.broadcasted_iota(jnp.int32, (SEQ, SEQ), 1)
    shard = jnp.zeros_like(col)
    for k in range(1, N_TP):
        shard = shard + (col >= k * PAD).astype(jnp.int32)
    return jnp.logical_and(col - PAD * shard < TOK, col - (PAD - TOK) * shard < seq_len)


def head_probs(q_half, k_pair, valid):
    scores = mm(q_half, k_pair, NT) * 0.125
    scores = jnp.where(valid, scores, NEG_BIG)
    e = jnp.exp(scores - jnp.max(scores, axis=-1, keepdims=True))
    return e / row_sum(e)


def seq_rows(b):
    return pl.ds(b * SEQ if isinstance(b, int) else pl.multiple_of(b * SEQ, SEQ), SEQ)


def pair_cols(pair):
    return pl.ds(pl.multiple_of(pair * LANES, LANES), LANES)


def flat(x):
    return x.reshape(-1, x.shape[-1])


def attn_fwd_unit(rows, pair, x, w_ref, bias, seq_len, qkv_ref, o_ref):
    cols = pair_cols(pair)
    pieces = []
    for c in range(3):
        val = (mm(x, w_ref[c, cols, :], NT) + bias[c:c + 1, cols]).astype(BF16)
        qkv_ref[c, rows, cols] = val
        pieces.append(val)
    q, k, v = pieces
    valid = key_valid(seq_len)
    half = lax.broadcasted_iota(jnp.int32, (SEQ, LANES), 1) // 64
    res = []
    for h in range(2):
        probs = head_probs(jnp.where(half == h, q, jnp.zeros_like(q)), k, valid)
        res.append(mm(probs.astype(BF16), v))
    o_ref[rows, cols] = jnp.where(half == 0, res[0], res[1]).astype(BF16)


def attn_bwd_unit(rows, pair, g, qkv_ref, w_ref, seq_len, dqkv_ref, db_ref):
    cols = pair_cols(pair)
    do = mm(g, w_ref[cols, :], NT).astype(BF16)
    q, k, v = (qkv_ref[c, rows, cols] for c in range(3))
    valid = key_valid(seq_len)
    half = lax.broadcasted_iota(jnp.int32, (SEQ, LANES), 1) // 64
    dq, dk, dv = [], [], []
    for h in range(2):
        probs = head_probs(jnp.where(half == h, q, jnp.zeros_like(q)), k, valid)
        grad_p = mm(jnp.where(half == h, do, jnp.zeros_like(do)), v, NT)
        grad_s = (probs * (grad_p - row_sum(grad_p * probs)) * 0.125).astype(BF16)
        dv.append(mm(probs.astype(BF16), do, TN))
        dq.append(mm(grad_s, k))
        dk.append(mm(grad_s, q, TN))
    for c, pieces in enumerate((dq, dk, dv)):
        val = jnp.where(half == 0, pieces[0], pieces[1])
        dqkv_ref[c, rows, cols] = val.astype(BF16)
        db_ref[c:c + 1, cols] = col_sum(val)


def mlp_up_unit(x, u_ref, bias, cols):
    gate = mm(x, u_ref[0, :, cols]) + bias[0:1, cols]
    lin = mm(x, u_ref[1, :, cols]) + bias[1:2, cols]
    return gate, lin


def mlp_bwd_unit(rows, u, x, g, u_ref, bias, d_ref, hid_ref, gp_ref, gb_ref):
    cols = pl.ds(pl.multiple_of(u * HEADS, HEADS), HEADS)
    gate, lin = mlp_up_unit(x, u_ref, bias, cols)
    grad_hid = mm(g, d_ref[cols, :], NT)
    sig = jax.nn.sigmoid(gate)
    if hid_ref is not None:
        hid_ref[rows, cols] = (gate * sig * lin).astype(BF16)
    grad_gate = grad_hid * lin * sig * (1.0 + gate * (1.0 - sig))
    grad_lin = grad_hid * gate * sig
    for c, val in enumerate((grad_gate, grad_lin)):
        gp_ref[c, rows, cols] = val.astype(BF16)
        gb_ref[c:c + 1, cols] = col_sum(val)


def qkv_shape(rows):
    return sds((3, rows, HEADS), BF16)


def heads_shape(rows):
    return sds((rows, HEADS), BF16)


def hidden_shape(rows):
    return sds((rows, WIDTH), BF16)


def grad_pre_shape(rows):
    return sds((2, rows, WIDTH), BF16)


ALL = pl.ds(0, SEQ)
GRAD_BQ = sds((3, HEADS), F32)
GRAD_BU = sds((2, WIDTH), F32)
BOTH_BQ = sds((N_SEQ, 3, HEADS), F32)


def fill_attn_fwd(layer, normed, wq, bq, lens):
    def body(i, ins, outs):
        n_ref, w_ref, b_ref, vl_ref = ins
        b = i // 2
        attn_fwd_unit(seq_rows(b), i % 2, sequence(n_ref, b), w_ref, b_ref.at[layer], first(vl_ref[b]), *outs)
    return Work([held(normed), load(wq, layer), held(bq), held(lens)], [qkv_shape(ROWS), heads_shape(ROWS)], 4, body, 1.8)


def fill_attn_bwd(layer, qkv, grad, wp, lens):
    def body(i, ins, outs):
        qkv_ref, g_ref, w_ref, vl_ref = ins
        b = i // 2
        attn_bwd_unit(seq_rows(b), i % 2, sequence(g_ref, b), qkv_ref, w_ref, first(vl_ref[b]), outs[0], outs[1].at[b])
    return Work([load(qkv), held(grad), load(wp, layer), held(lens)], [qkv_shape(ROWS), BOTH_BQ], 4, body, 2.0)


def fill_mlp(layer, normed, grads, w_up, b_up, w_down):
    def body(i, ins, outs):
        n_ref, u_ref, b_ref, d_ref = ins[:4]
        n, g = (jnp.concatenate([sequence(ref, b) for ref in refs for b in range(ref.shape[0])], axis=0)
                for refs in ([n_ref], ins[4:]))
        mlp_bwd_unit(pl.ds(0, ROWS), i, n, g, u_ref, b_ref.at[layer], d_ref, *outs[:2], outs[2].at[0])
    return Work([normed, load(w_up, layer), held(b_up), load(w_down, layer)] + [held(g) for g in grads],
                [hidden_shape(ROWS), grad_pre_shape(ROWS), sds((1, 2, WIDTH), F32)], 4, body, 1.6)


def pro_attn_fwd(b, layer, normed, wq, bq, wp, lens):
    early = not (layer or b)

    def body(u, x, ins, outs):
        w_ref, b_ref, _, vl_ref = ins
        attn_fwd_unit(ALL, u, x[...], w_ref, b_ref.at[layer], first(vl_ref[b]), *outs)

    def fin(ins, outs):
        return mm(outs[1][...], ins[2][...])
    return Work([load(wq, layer, early), held(bq), load(wp, layer, early), held(lens)], [qkv_shape(SEQ), heads_shape(SEQ)], 2, body,
                fin=fin, x=normed)


def pro_mlp_fwd(layer, normed, w_up, b_up, w_down):
    def body(u, x, ins, outs):
        u_ref, b_ref, _ = ins
        cols = pl.ds(pl.multiple_of(u * HEADS, HEADS), HEADS)
        gate, lin = mlp_up_unit(x[...], u_ref, b_ref.at[layer], cols)
        outs[0][:, cols] = (jax.nn.silu(gate) * lin).astype(BF16)

    def fin(ins, outs):
        return mm(outs[0][...], ins[2][...])
    return Work([load(w_up, layer), held(b_up), load(w_down, layer)], [hidden_shape(SEQ)], 4, body, fin=fin, x=normed)


def pro_mlp_bwd(b, layer, normed, grad, w_up, b_up, w_down, forward):
    extra = grad if forward else normed

    def body(u, x, ins, outs):
        u_ref, b_ref, d_ref, e_ref = ins
        pair = (x[...], sequence(e_ref, b if e_ref.shape[0] > 1 else 0))
        n, g = pair if forward else pair[::-1]
        mlp_bwd_unit(ALL, u, n, g, u_ref, b_ref.at[layer], d_ref, outs[2] if forward else None, *outs[:2])

    def fin(ins, outs):
        if forward:
            val = mm(outs[2][...], ins[2][...]).astype(BF16)
            for k in range(N_TP):
                outs[3][k] = val[k * PAD:(k + 1) * PAD]
        return sum(mm(outs[0][c], ins[0][c], NT) for c in range(2))
    return Work([load(w_up, layer), held(b_up), load(w_down, layer), extra],
                [grad_pre_shape(SEQ), GRAD_BU] + ([hidden_shape(SEQ), sds((N_TP, PAD, WIDTH), BF16)] if forward else []),
                4, body, fin=fin, x=normed if forward else grad)


def pro_attn_bwd(b, layer, qkv, grad, wp, wq, lens):
    def body(u, x, ins, outs):
        qkv_ref, w_ref, _, vl_ref = ins
        attn_bwd_unit(ALL, u, x[...], qkv_ref, w_ref, first(vl_ref[b]), *outs)

    def fin(ins, outs):
        return sum(mm(outs[0][c], ins[2][c]) for c in range(3))
    return Work([load(qkv), load(wp, layer), load(wq, layer), held(lens)], [qkv_shape(SEQ), GRAD_BQ], 2, body, fin=fin,
                x=grad)


def gather_norm(cid, layer, x, gain, bias, **side):
    def local(b, acc, ins, outs):
        x_ref, g_ref, b_ref = ins
        x_hat, _ = ln_stats(x_ref[b])
        return (x_hat * row(g_ref, layer) + row(b_ref, layer)).astype(BF16)
    return stage_call(cid, local, (x, gain, bias), [], **side)


def residual_norm(cid, layer, x, bias, scale, norm_layer, gain, shift, **side):
    def local(b, acc, ins, outs):
        x_ref, b_ref, s_ref, g_ref, h_ref = ins
        total = acc + row(b_ref, layer)
        outs[1][b] = total
        x_new = (x_ref[b].astype(F32) + row(s_ref, layer) * total).astype(BF16)
        outs[0][b] = x_new
        x_hat, _ = ln_stats(x_new)
        return (x_hat * row(g_ref, norm_layer) + row(h_ref, norm_layer)).astype(BF16)
    return stage_call(cid, local, (x, bias, scale, gain, shift), [sds(x.shape, BF16), sds(x.shape, F32)], **side)


def residual_last(layer, parts, x, bias, scale, grad_y):
    def local(b, acc, ins, outs):
        x_ref, b_ref, s_ref, g_ref = ins
        total = acc + row(b_ref, layer)
        outs[0][b] = (x_ref[b].astype(F32) + row(s_ref, layer) * total).astype(BF16)
        grad = g_ref[b].astype(F32)
        add_rows(outs[1], b, [grad * total, row(s_ref, layer) * grad])
    return parts, local, (x, bias, scale, grad_y), [sds(x.shape, BF16), sds((2, x.shape[-1]), F32)]


def back_mid(cid, layer, x_mid, gain, grad_res, attn_sum, scale, **side):
    def local(b, acc, ins, outs):
        x_ref, g_ref, r_ref, a_ref, s_ref = ins
        grad_in, x_hat = ln_bwd(acc, x_ref[b], row(g_ref, layer))
        grad_mid = r_ref[b].astype(F32) + grad_in
        outs[0][b] = grad_mid
        grad_attn = row(s_ref, layer) * grad_mid
        add_rows(outs[1], b, [acc * x_hat, acc, grad_mid * a_ref[b], grad_attn])
        return grad_attn.astype(BF16)
    return stage_call(cid, local, (x_mid, gain, grad_res, attn_sum, scale),
                      [sds(x_mid.shape, F32), sds((4, x_mid.shape[-1]), F32)], **side)


def back_in(cid, layer, x_in, gain, grad_mid, mlp_sum, scale, **side):
    more = layer > 0

    def local(b, acc, ins, outs):
        x_ref, g_ref, m_ref = ins[:3]
        grad_in, x_hat = ln_bwd(acc, x_ref[b], row(g_ref, layer))
        grad = (m_ref[b] + grad_in).astype(BF16)
        outs[0][b] = grad
        if not more:
            add_rows(outs[1], b, [acc * x_hat, acc])
            return None
        grad = grad.astype(F32)
        grad_mlp = row(ins[4], layer - 1) * grad
        add_rows(outs[1], b, [acc * x_hat, acc])
        add_rows(outs[2], b, [grad * ins[3][b], grad_mlp])
        return grad_mlp.astype(BF16)
    shapes = [sds(x_in.shape, BF16)] + [sds((2, x_in.shape[-1]), F32)] * (2 if more else 1)
    return stage_call(cid, local, (x_in, gain, grad_mid) + ((mlp_sum, scale) if more else ()), shapes, ag=more, **side)


def grads_call(jobs, biases, sums):
    args, bufs, loads = [], [], []
    for job in jobs:
        for arrs in job[2:]:
            at = 0
            for arr in arrs:
                loads.append((len(args), len(bufs), at))
                args.append(arr)
                at += arr.shape[-2]
            wide = arrs[0].shape[0] if job[0] == 2 and arrs[0].ndim > 2 else 1
            lead = arrs[0].shape[:-2] if wide == 1 else ()
            bufs.append(pltpu.VMEM((*lead, at, wide * arrs[0].shape[-1]), BF16))
    n_op = len(args)
    small = [x for group in biases for trio in group for x in trio] + [sums]
    args = [pltpu.with_memory_space_constraint(a, pltpu.HBM) for a in args] + small
    specs = [HBM_SPEC] * n_op + [VMEM_SPEC] * len(small)
    width = sums.shape[-1]
    shapes = [(groups, total, width) for groups, total in ((2, WIDTH), (1, WIDTH), (3, HEADS), (1, HEADS))]
    shapes += [biases[0][0][0].shape, (3, N_TP, HEADS // N_TP)] + [(width,)] * 8
    outs = [sds((2, *shape), F32) for shape in shapes]
    stage_rows = WIDTH

    def kernel(*refs):
        ops, smalls = refs[:n_op], refs[n_op:len(args)]
        out = refs[len(args):len(args) + len(outs)]
        buf = refs[len(args) + len(outs):]
        stage, lsem, osem = buf[len(bufs):]
        copies = []
        for k, k_buf, at in loads:
            n_rows, n_cols = ops[k].shape[-2:]
            rows, dst = pl.ds(at, n_rows), buf[k_buf]
            if len(ops[k].shape) == len(dst.shape):
                pairs = [(ops[k], dst.at[:, rows] if len(dst.shape) == 3 else dst.at[rows])]
            else:
                pairs = [(ops[k].at[c], dst.at[rows, pl.ds(c * n_cols, n_cols)]) for c in range(ops[k].shape[0])]
            for src, to in pairs:
                copies.append((pltpu.make_async_copy(src, to, lsem.at[len(copies)]), k_buf // 2))

        def fetch(j, act):
            for cp, owner in copies:
                if owner == j:
                    act(cp)

        for j in range(2):
            fetch(j, lambda cp: cp.start())
        for l in range(2):
            for k in range(2):
                own_a, own_b, oth = smalls[6 * k + 3 * l:][:3]
                val = sum((oth[b] for b in range(oth.shape[0])), own_a[...] + own_b[...])
                if k:
                    n = out[5].shape[-1]
                    for h in range(N_TP):
                        out[5][l, :, h, :] = val[:, h * n:(h + 1) * n]
                else:
                    out[4][l] = val
        rows = smalls[-1]
        for k in range(8):
            for l, at in enumerate((8 + k, 2 + k if k < 6 else k - 6)):
                out[6 + k][l:l + 1, :] = rows[at:at + 1, :]
        pending = [[]] * 2
        step = 0
        for j, (slot, layer, *_) in enumerate(jobs):
            a_ref, b_ref = buf[2 * j:2 * j + 2]
            fetch(j, lambda cp: cp.wait())
            fetch(j + 2, lambda cp: cp.start())
            total = outs[slot].shape[2]
            split_b = len(b_ref.shape) > 2
            for g in range(b_ref.shape[0] if split_b else 1):
                s = step % 2
                val = mm(a_ref[...], b_ref[g] if split_b else b_ref[...], TN)
                for cp in pending[s]:
                    cp.wait()
                stage[s, :val.shape[0]] = val
                pending[s] = [pltpu.make_async_copy(stage.at[s, pl.ds(k * total, total)], out[slot].at[layer, g + k], osem.at[s, k])
                              for k in range(val.shape[0] // total)]
                for cp in pending[s]:
                    cp.start()
                step += 1
        for cp in pending[0] + pending[1]:
            cp.wait()

    return pl.pallas_call(
        kernel,
        out_shape=outs,
        in_specs=specs,
        out_specs=[HBM_SPEC] * 4 + [VMEM_SPEC] * 10,
        scratch_shapes=bufs + [pltpu.VMEM((2, stage_rows, width), F32), pltpu.SemaphoreType.DMA((2 * n_op,)),
                               pltpu.SemaphoreType.DMA((2, 3))],
        compiler_params=pltpu.CompilerParams(vmem_limit_bytes=60 * MIB),
        cost_estimate=pl.CostEstimate(flops=40_000_000_000, bytes_accessed=80_000_000, transcendentals=0),
        name='grads')(*args)


def device_fn(tokens, grad_y, valid_len, norm1_gain, norm1_bias, w_qkv, b_qkv, w_proj, b_proj, layer_scale1,
              norm2_gain, norm2_bias, w_up, b_up, w_down, b_down, layer_scale2):
    pad = ((0, 0), (0, PAD - TOK), (0, 0))
    x0 = jnp.pad(tokens, pad)
    g_y = jnp.pad(grad_y, pad)
    lens = jnp.broadcast_to(valid_len[:, None, None], (N_SEQ, 8, LANES))
    wq = jnp.moveaxis(w_qkv, 2, 4).reshape(2, 3, HEADS, WIDTH)
    bq = b_qkv.reshape(2, 3, HEADS)
    wp = w_proj.reshape(2, HEADS, WIDTH)

    mlp = w_up, b_up, w_down
    ids = itertools.count()
    n1_0, lens_x, part, qkv_0a, o_0a = gather_norm(
        next(ids), 0, x0, norm1_gain, norm1_bias, trade=[lens], nxt=pro_attn_fwd(0, 0, None, wq, bq, wp, lens))
    mid_0, asum_0, n2_0, n1_0x, n1_0h, gm_1a, part, qkv_0b, o_0b, hid_0a = residual_norm(
        next(ids), 0, x0, b_proj, layer_scale1, 0, norm2_gain, norm2_bias, parts=[part],
        pro=pro_attn_fwd(1, 0, n1_0, wq, bq, wp, lens), nxt=pro_mlp_fwd(0, None, *mlp),
        swap=[n1_0], save=[n1_0], extra=(1, 0, g_y, layer_scale2))
    x1, msum_0, n1_1, n2_0x, gm_1ax, n2_0h, n1_0xh, gm_1ah, gm_1b, part, hid_0b, qkv_1a, o_1a, qkv_0x, o_0x = residual_norm(
        next(ids), 0, mid_0, b_down, layer_scale2, 1, norm1_gain, norm1_bias, parts=[part],
        pro=pro_mlp_fwd(0, n2_0, *mlp), nxt=pro_attn_fwd(0, 1, None, wq, bq, wp, lens),
        swap=[n2_0, gm_1a], save=[n2_0, n1_0x, gm_1a], extra=(1, 1, g_y, layer_scale2),
        fills=[fill_attn_fwd(0, n1_0x, wq, bq, lens_x)])
    (mid_1, asum_1, n2_1, n1_1x, n1_1h, gm_1bh, gm_1axh, n2_0xh, part, qkv_1b, o_1b, gp_1a, gb_1a, hid_1a,
     part_ya) = residual_norm(
        next(ids), 1, x1, b_proj, layer_scale1, 1, norm2_gain, norm2_bias, parts=[part],
        pro=pro_attn_fwd(1, 1, n1_1, wq, bq, wp, lens), nxt=pro_mlp_bwd(0, 1, None, held(gm_1a), *mlp, True),
        swap=[n1_1], save=[n1_1, gm_1b, gm_1ax, n2_0x])

    (gmid_1, rows_mid_1, ga_1, n2_1x, gm_1bx, n2_1h, n1_1xh, part, gp_1b, gb_1b, hid_1b, part_yb, gq_1a, gbq_1a, qkv_1x,
     o_1x) = back_mid(
        next(ids), 1, mid_1, norm2_gain, g_y, asum_1, layer_scale1, parts=[part],
        pro=pro_mlp_bwd(1, 1, n2_1, held(gm_1b), *mlp, True), nxt=pro_attn_bwd(0, 1, qkv_1a, None, wp, wq, lens),
        swap=[n2_1, gm_1b], save=[n2_1, n1_1x], fills=[fill_attn_fwd(1, n1_1x, wq, bq, lens_x)])
    (grad_1, rows_in_1, rows_mlp_0, gm_0, ga_1x, ga_1h, n2_1xh, gm_1bxh, part, gq_1b, gbq_1b, gp_0a, gb_0a, hid_1x, gp_1x,
     gb_1x) = back_in(
        next(ids), 1, x1, norm1_gain, gmid_1, msum_0, layer_scale2, parts=[part],
        pro=pro_attn_bwd(1, 1, qkv_1b, ga_1, wp, wq, lens), nxt=pro_mlp_bwd(0, 0, load(n2_0h), None, *mlp, False),
        swap=[ga_1], save=[ga_1, n2_1x, gm_1bx], fills=[fill_mlp(1, held(n2_1x), [gm_1ax, gm_1bx], *mlp)])

    gmid_0, rows_mid_0, ga_0, gm_0x, gm_0h, ga_1xh, part, gp_0b, gb_0b, gq_0a, gbq_0a, gq_1x, gbq_1x = back_mid(
        next(ids), 0, mid_0, norm2_gain, grad_1, asum_0, layer_scale1, parts=[part],
        pro=pro_mlp_bwd(1, 0, load(n2_0h), gm_0, *mlp, False), nxt=pro_attn_bwd(0, 0, qkv_0a, None, wp, wq, lens),
        swap=[gm_0], save=[gm_0, ga_1x], fills=[fill_attn_bwd(1, qkv_1x, ga_1x, wp, lens_x)])
    grad_0, rows_in_0, y_out, rows_mlp_1, ga_0x, ga_0h, gm_0xh, gq_0b, gbq_0b, hid_0x, gp_0x, gb_0x = back_in(
        next(ids), 0, x0, norm1_gain, gmid_0, None, None, parts=[part], pro=pro_attn_bwd(1, 0, qkv_0b, ga_0, wp, wq, lens),
        second=residual_last(1, (part_ya, part_yb), mid_1, b_down, layer_scale2, g_y),
        swap=[ga_0], save=[ga_0, gm_0x], fills=[fill_mlp(0, load(n2_0xh), [gm_0x], *mlp)])
    ga_0xh, sums, gq_0x, gbq_0x = stage_call(
        next(ids), None, [rows_mlp_1], [], ag=False, save=[ga_0x], fills=[fill_attn_bwd(0, qkv_0x, ga_0x, wp, lens_x)],
        sums=(rows_mlp_1, rows_in_1, rows_mid_1, rows_in_0, rows_mid_0, rows_mlp_0))

    operands = (
        ((n2_1h, n2_1xh), (gp_1a, gp_1b, gp_1x), (hid_1a, hid_1b, hid_1x), (gm_1ah, gm_1bh, gm_1axh, gm_1bxh),
         (gq_1a, gq_1b, gq_1x), (n1_1h, n1_1xh), (o_1a, o_1b, o_1x), (ga_1h, ga_1xh)),
        ((n2_0h, n2_0xh), (gp_0a, gp_0b, gp_0x), (hid_0a, hid_0b, hid_0x), (gm_0h, gm_0xh),
         (gq_0a, gq_0b, gq_0x), (n1_0h, n1_0xh), (o_0a, o_0b, o_0x), (ga_0h, ga_0xh)))
    jobs = []
    for k, ops in enumerate(operands):
        ops = [[a if a.ndim < 4 else flat(a) for a in arrs] for arrs in ops]
        jobs += [(slot, 1 - k, *ops[2 * slot:2 * slot + 2]) for slot in (range(4) if k else reversed(range(4)))]
    g_up, g_down, g_qkv, g_proj, g_b_up, g_b_qkv, n1g, n1b, n2g, n2b, ls1, bp, ls2, bd = grads_call(
        jobs, [[(gb_0a, gb_0b, gb_0x), (gb_1a, gb_1b, gb_1x)], [(gbq_0a, gbq_0b, gbq_0x), (gbq_1a, gbq_1b, gbq_1x)]], sums)
    return (y_out[:, :TOK], grad_0[:, :TOK], n1g, n1b,
            jnp.moveaxis(g_qkv.reshape(2, 3, 4, 64, WIDTH), 4, 2), g_b_qkv,
            g_proj.reshape(2, 4, 64, WIDTH), bp, ls1, n2g, n2b, g_up, g_b_up,
            g_down.reshape(2, WIDTH, WIDTH), bd, ls2)


def split(axis, ndim):
    return P(*('tp' if k == axis else None for k in range(ndim)))


def solution(mesh):
    rep = P()
    act = P('dp', 'tp', None)
    param_specs = (rep, rep, split(3, 5), split(2, 4), split(1, 4), rep, rep, rep, rep, split(3, 4), split(2, 3), split(1, 3),
                   rep, rep)
    return jax.shard_map(device_fn, mesh=mesh, in_specs=(act, act, P('dp')) + param_specs,
                         out_specs=(act, act) + param_specs, check_vma=False)
```
